32 devices in a mesh: data: 32 (over z, y, x, core).
Axes of the slice: x: 2, y: 2, z: 4, core: 2. Of those that a mesh axis runs over, the one named last changes fastest.
Arguments:
- x_now: bfloat16 [64, 784, 128], P('data')
- labels_now: int32 [64], P('data')
- x_next: bfloat16 [64, 784, 128], P('data')
- up_one: float32 [4, 128, 512], replicated
- down_one: float32 [4, 512, 128], replicated
- merge_proj: float32 [512, 512], replicated
- up_two: float32 [3, 512, 2048], replicated
- down_two: float32 [3, 2048, 512], replicated
- head_proj: float32 [512, 1000], replicated
- vel_up_one: float32 [4, 128, 512], replicated
- vel_down_one: float32 [4, 512, 128], replicated
- vel_merge_proj: float32 [512, 512], replicated
- vel_up_two: float32 [3, 512, 2048], replicated
- vel_down_two: float32 [3, 2048, 512], replicated
- vel_head_proj: float32 [512, 1000], replicated
Outputs:
- output 1: float32 [64, 1000], P('data')
- output 2: float32 [4, 128, 512], replicated
- output 3: float32 [4, 512, 128], replicated
- output 4: float32 [512, 512], replicated
- output 5: float32 [3, 512, 2048], replicated
- output 6: float32 [3, 2048, 512], replicated
- output 7: float32 [512, 1000], replicated
- output 8: float32 [4, 128, 512], replicated
- output 9: float32 [4, 512, 128], replicated
- output 10: float32 [512, 512], replicated
- output 11: float32 [3, 512, 2048], replicated
- output 12: float32 [3, 2048, 512], replicated
- output 13: float32 [512, 1000], replicated
All inputs are finite; a program needn't handle non-finite values.
Results may differ from the reference program's by a relative error of at most 0.0131016.
Values are sent between devices in bfloat16 or wider.
A program may use at most 1 GiB of HBM per device.

```python
import jax
import jax.numpy as jnp
from jax import lax

DATA_DEVS = 32
IMAGES_DEV = 2
TOKENS = 784
WIDTH = 128
DEPTH_ONE = 4
DEPTH_TWO = 3
CLASSES = 1000
BATCH = DATA_DEVS * IMAGES_DEV
MERGED = TOKENS // 4
WIDTH_TWO = 4 * WIDTH
HIDDEN_ONE = 4 * WIDTH
HIDDEN_TWO = 4 * WIDTH_TWO
MOMENTUM = 0.9
TRUST = 0.1
LN_EPS = 1e-6
SHIFT_SCALE = 1.5


def draw_weight(key_w, shape_w, fan_in, scale):
    return jax.random.normal(key_w, shape_w, jnp.float32) * (scale * fan_in ** -0.5)


def draw_images(key_img, key_shift):
    img_shift = jax.random.normal(key_shift, (BATCH, 1, WIDTH), jnp.float32) * SHIFT_SCALE
    raw_vals = jax.random.normal(key_img, (BATCH, TOKENS, WIDTH), jnp.float32)
    return (raw_vals + img_shift).astype(jnp.bfloat16)


def setup_inputs(seed: int = 0) -> dict:
    key_list = jax.random.split(jax.random.key(seed), 17)
    draw_specs = [
        ('up_one', (DEPTH_ONE, WIDTH, HIDDEN_ONE), WIDTH),
        ('down_one', (DEPTH_ONE, HIDDEN_ONE, WIDTH), HIDDEN_ONE),
        ('merge_proj', (4 * WIDTH, WIDTH_TWO), 4 * WIDTH),
        ('up_two', (DEPTH_TWO, WIDTH_TWO, HIDDEN_TWO), WIDTH_TWO),
        ('down_two', (DEPTH_TWO, HIDDEN_TWO, WIDTH_TWO), HIDDEN_TWO),
        ('head_proj', (WIDTH_TWO, CLASSES), WIDTH_TWO),
    ]
    drawn = {}
    drawn['x_now'] = draw_images(key_list[0], key_list[15])
    drawn['labels_now'] = jax.random.randint(key_list[1], (BATCH,), 0, CLASSES, jnp.int32)
    drawn['x_next'] = draw_images(key_list[2], key_list[16])
    for slot_num, spec_w in enumerate(draw_specs):
        drawn[spec_w[0]] = draw_weight(key_list[3 + slot_num], spec_w[1], spec_w[2], 1.0)
    for slot_num, spec_w in enumerate(draw_specs):
        drawn['vel_' + spec_w[0]] = draw_weight(key_list[9 + slot_num], spec_w[1], spec_w[2], TRUST)
    return drawn


def layer_norm(values):
    row_mean = jnp.mean(values, axis=-1, keepdims=True)
    centered = values - row_mean
    variance = jnp.mean(centered * centered, axis=-1, keepdims=True)
    return centered * lax.rsqrt(variance + LN_EPS)


def stage_block(residual, layer_weights):
    w_up, w_down = layer_weights
    normed = layer_norm(residual.astype(jnp.float32)).astype(jnp.bfloat16)
    pre_act = jnp.dot(normed, w_up.astype(jnp.bfloat16), preferred_element_type=jnp.float32)
    activated = jax.nn.gelu(pre_act, approximate=True).astype(jnp.bfloat16)
    block_out = jnp.dot(activated, w_down.astype(jnp.bfloat16), preferred_element_type=jnp.float32)
    return (residual.astype(jnp.float32) + block_out).astype(jnp.bfloat16), None


def model_logits(params, images):
    up_one, down_one, merge_proj, up_two, down_two, head_proj = params
    img_count = images.shape[0]
    residual = images.reshape(img_count * TOKENS, WIDTH)
    residual = lax.scan(stage_block, residual, (up_one, down_one))[0]
    merged = residual.reshape(img_count * MERGED, 4 * WIDTH)
    residual = jnp.dot(merged, merge_proj.astype(jnp.bfloat16), preferred_element_type=jnp.float32).astype(jnp.bfloat16)
    residual = lax.scan(stage_block, residual, (up_two, down_two))[0]
    pooled = jnp.mean(residual.reshape(img_count, MERGED, WIDTH_TWO).astype(jnp.float32), axis=1)
    normed = layer_norm(pooled).astype(jnp.bfloat16)
    return jnp.dot(normed, head_proj.astype(jnp.bfloat16), preferred_element_type=jnp.float32)


def shard_loss(params, images, labels):
    logits = model_logits(params, images)
    log_norm = jax.nn.logsumexp(logits, axis=-1)
    picked = jnp.sum(logits * jax.nn.one_hot(labels, CLASSES, dtype=jnp.float32), axis=-1)
    return jnp.sum(log_norm - picked) / BATCH


def lars_step(weight, velocity, grad_sum):
    red_axes = (weight.ndim - 2, weight.ndim - 1)
    w_norm = jnp.sqrt(jnp.sum(weight * weight, axis=red_axes, keepdims=True))
    g_norm = jnp.sqrt(jnp.sum(grad_sum * grad_sum, axis=red_axes, keepdims=True))
    new_vel = MOMENTUM * velocity + TRUST * (w_norm / g_norm) * grad_sum
    return weight - new_vel, new_vel


def reference(x_now, labels_now, x_next, up_one, down_one, merge_proj, up_two, down_two, head_proj, vel_up_one, vel_down_one, vel_merge_proj, vel_up_two, vel_down_two, vel_head_proj):
    params = (up_one, down_one, merge_proj, up_two, down_two, head_proj)
    grad_fn = jax.grad(shard_loss)

    def add_shard(running, shard_pair):
        grads = grad_fn(params, shard_pair[0], shard_pair[1])
        summed = jax.tree.map(lambda run_sum, shard_grad: run_sum + shard_grad.astype(jnp.bfloat16).astype(jnp.float32), running, grads)
        return summed, None

    zero_sums = jax.tree.map(jnp.zeros_like, params)
    img_shards = x_now.reshape(DATA_DEVS, IMAGES_DEV, TOKENS, WIDTH)
    label_shards = labels_now.reshape(DATA_DEVS, IMAGES_DEV)
    grad_sums = lax.scan(add_shard, zero_sums, (img_shards, label_shards))[0]
    new_up_one, new_vel_up_one = lars_step(up_one, vel_up_one, grad_sums[0])
    new_down_one, new_vel_down_one = lars_step(down_one, vel_down_one, grad_sums[1])
    new_merge_proj, new_vel_merge_proj = lars_step(merge_proj, vel_merge_proj, grad_sums[2])
    new_up_two, new_vel_up_two = lars_step(up_two, vel_up_two, grad_sums[3])
    new_down_two, new_vel_down_two = lars_step(down_two, vel_down_two, grad_sums[4])
    new_head_proj, new_vel_head_proj = lars_step(head_proj, vel_head_proj, grad_sums[5])
    new_params = (new_up_one, new_down_one, new_merge_proj, new_up_two, new_down_two, new_head_proj)
    next_shards = x_next.reshape(DATA_DEVS, IMAGES_DEV, TOKENS, WIDTH)
    logits_next = lax.map(lambda images: model_logits(new_params, images), next_shards).reshape(BATCH, CLASSES)
    return (logits_next, new_up_one, new_down_one, new_merge_proj, new_up_two, new_down_two, new_head_proj, new_vel_up_one, new_vel_down_one, new_vel_merge_proj, new_vel_up_two, new_vel_down_two, new_vel_head_proj)
```

```python
import functools

import jax
import jax.numpy as jnp
from jax import lax
from jax.experimental import pallas as pl
from jax.experimental.pallas import tpu as pltpu
from jax.sharding import PartitionSpec as P

MOMENTUM = 0.9
TRUST = 0.1
LN_EPS = 1e-6


def layer_norm(values):
    row_mean = jnp.mean(values, axis=-1, keepdims=True)
    centered = values - row_mean
    variance = jnp.mean(centered * centered, axis=-1, keepdims=True)
    return centered * lax.rsqrt(variance + LN_EPS)


def gelu_tanh(values):
    return jax.nn.gelu(values, approximate=True)


def contract_rows(lhs_mat, rhs_mat):
    return lax.dot_general(lhs_mat, rhs_mat, (((0,), (0,)), ((), ())), preferred_element_type=jnp.float32)


def contract_cols(lhs_mat, rhs_mat):
    return lax.dot_general(lhs_mat, rhs_mat, (((1,), (1,)), ((), ())), preferred_element_type=jnp.float32)


def to_bf16_layers(stacked):
    return [stacked[layer_num].astype(jnp.bfloat16) for layer_num in range(stacked.shape[0])]


def cast_weights(params):
    up_one, down_one, merge_proj, up_two, down_two, head_proj = params
    return (to_bf16_layers(up_one), to_bf16_layers(down_one), merge_proj.astype(jnp.bfloat16), to_bf16_layers(up_two), to_bf16_layers(down_two), head_proj.astype(jnp.bfloat16))


def block_forward(residual, w_up, w_down):
    normed, norm_back = jax.vjp(layer_norm, residual.astype(jnp.float32))
    normed_b = normed.astype(jnp.bfloat16)
    pre_act = jnp.dot(normed_b, w_up, preferred_element_type=jnp.float32)
    activated, gelu_back = jax.vjp(gelu_tanh, pre_act)
    activated_b = activated.astype(jnp.bfloat16)
    block_out = jnp.dot(activated_b, w_down, preferred_element_type=jnp.float32)
    new_residual = (residual.astype(jnp.float32) + block_out).astype(jnp.bfloat16)
    return new_residual, (normed_b, activated_b, norm_back, gelu_back)


def block_backward(grad_out, saved, w_up, w_down):
    normed_b, activated_b, norm_back, gelu_back = saved
    grad_down = contract_rows(activated_b, grad_out)
    grad_act = contract_cols(grad_out, w_down)
    grad_pre = gelu_back(grad_act)[0].astype(jnp.bfloat16)
    grad_up = contract_rows(normed_b, grad_pre)
    grad_normed = contract_cols(grad_pre, w_up)
    grad_in = norm_back(grad_normed)[0] + grad_out.astype(jnp.float32)
    return grad_in.astype(jnp.bfloat16), grad_up, grad_down


def model_forward(images, weights):
    ups_one, downs_one, merge_w, ups_two, downs_two, head_w = weights
    img_count, tokens, width = images.shape
    residual = images.reshape(img_count * tokens, width)
    saved_one = []
    for w_up, w_down in zip(ups_one, downs_one):
        residual, saved = block_forward(residual, w_up, w_down)
        saved_one.append(saved)
    merged = residual.reshape(img_count * tokens // 4, 4 * width)
    residual = jnp.dot(merged, merge_w, preferred_element_type=jnp.float32).astype(jnp.bfloat16)
    saved_two = []
    for w_up, w_down in zip(ups_two, downs_two):
        residual, saved = block_forward(residual, w_up, w_down)
        saved_two.append(saved)
    pooled = jnp.mean(residual.reshape(img_count, tokens // 4, -1), axis=1, dtype=jnp.float32)
    head_in, head_back = jax.vjp(layer_norm, pooled)
    head_in_b = head_in.astype(jnp.bfloat16)
    logits = jnp.dot(head_in_b, head_w, preferred_element_type=jnp.float32)
    return logits, (saved_one, merged, saved_two, head_in_b, head_back)


def loss_grad(logits, labels, global_batch):
    soft_probs = jax.nn.softmax(logits, axis=-1)
    class_ids = jnp.arange(logits.shape[1], dtype=jnp.int32)
    onehot = (labels[:, None] == class_ids[None, :]).astype(jnp.float32)
    return ((soft_probs - onehot) / global_batch).astype(jnp.bfloat16)


def head_input_grad(grad_logits, head_w, head_back, merged_tokens):
    grad_pooled = head_back(contract_cols(grad_logits, head_w))[0] / merged_tokens
    img_count, width_two = grad_pooled.shape
    spread = jnp.broadcast_to(grad_pooled.astype(jnp.bfloat16)[:, None, :], (img_count, merged_tokens, width_two))
    return spread.reshape(img_count * merged_tokens, width_two)


def lars_step(weight, velocity, grad_sum):
    grad_f = grad_sum.astype(jnp.float32)
    red_axes = (weight.ndim - 2, weight.ndim - 1)
    w_norm = jnp.sqrt(jnp.sum(weight * weight, axis=red_axes, keepdims=True))
    g_norm = jnp.sqrt(jnp.sum(grad_f * grad_f, axis=red_axes, keepdims=True))
    new_vel = MOMENTUM * velocity + TRUST * (w_norm / g_norm) * grad_f
    return weight - new_vel, new_vel


def finish_step(params, velocities, grad_sums, x_next):
    updated = [lars_step(weight, velocity, grad_sum) for weight, velocity, grad_sum in zip(params, velocities, grad_sums)]
    new_params = tuple(pair_new[0] for pair_new in updated)
    new_vels = tuple(pair_new[1] for pair_new in updated)
    logits_next = model_forward(x_next, cast_weights(new_params))[0]
    return (logits_next,) + new_params + new_vels


MESH = pl.DeviceIdType.MESH
ROWS = 512
LAG = 2
STAGES = 12


def all_reduce_body(chunks, grad_buf, full_buf, recv_core, recv_one, recv_z, recv_mid, recv_two, send_sem, recv_sem, before, after):
    me = lax.axis_index('data')
    core = me % 2
    x_pos = (me // 2) % 2
    y_pos = (me // 4) % 2
    z_pos = me // 8
    one = x_pos * (1 - core) + y_pos * core
    two = y_pos * (1 - core) + x_pos * core
    one_step = 2 * (1 - core) + 4 * core
    two_step = 4 * (1 - core) + 2 * core
    dev_core = me + 1 - 2 * core
    dev_one = me + one_step * (1 - 2 * one)
    dev_two = me + two_step * (1 - 2 * two)
    upper = z_pos // 2
    is_end = (z_pos % 3) == 0
    is_mid = (z_pos % 3) != 0
    dev_inner = me + 8 * (1 - 2 * upper)
    dev_outer = me - 8 * (1 - 2 * upper)
    half = core * 256
    quarter = half + one * 128
    near = quarter + upper * 64
    far = quarter + (1 - upper) * 64
    mine = near + two * 32

    def rows(chunk, start, size):
        return grad_buf.at[chunk, pl.ds(pl.multiple_of(start, 32), size)]

    def full(chunk, start, size):
        return full_buf.at[chunk, pl.ds(pl.multiple_of(start, 32), size)]

    def remote(src, dst, which, chunk, dev):
        return pltpu.make_async_remote_copy(src_ref=src, dst_ref=dst, send_sem=send_sem.at[which, chunk], recv_sem=recv_sem.at[which, chunk], device_id=(dev,), device_id_type=MESH)

    def add_in(chunk, start, size, recv):
        def step(num, carry):
            spot = pl.ds(pl.multiple_of(start + num * 32, 32), 32)
            grad_buf[chunk, spot, :] = grad_buf[chunk, spot, :] + recv[chunk, pl.ds(pl.multiple_of(num * 32, 32), 32), :]
            return carry
        lax.fori_loop(0, size // 32, step, 0)

    def c_core(k):
        return remote(rows(k, 256 - half, 256), recv_core.at[k], 0, k, dev_core)

    def c_one(k):
        return remote(rows(k, half + (1 - one) * 128, 128), recv_one.at[k], 1, k, dev_one)

    def c_in(k):
        return remote(rows(k, far, 64), recv_z.at[k], 2, k, dev_inner)

    def c_mid(k):
        return remote(rows(k, far, 64), recv_mid.at[k], 3, k, dev_inner)

    def c_out(k):
        return remote(rows(k, near, 64), recv_z.at[k], 2, k, dev_outer)

    def c_two(k):
        return remote(rows(k, near + (1 - two) * 32, 32), recv_two.at[k], 4, k, dev_two)

    def g_two(k):
        return remote(full(k, mine, 32), full(k, mine, 32), 5, k, dev_two)

    def g_in(k):
        return remote(full(k, near, 64), full(k, near, 64), 6, k, dev_inner)

    def g_mid(k):
        return remote(full(k, near, 64), full(k, near, 64), 7, k, dev_inner)

    def g_out(k):
        return remote(full(k, far, 64), full(k, far, 64), 6, k, dev_outer)

    def g_one(k):
        return remote(full(k, quarter, 128), full(k, quarter, 128), 8, k, dev_one)

    def g_core(k):
        return remote(full(k, half, 256), full(k, half, 256), 9, k, dev_core)

    def stage_0(k):
        before(k)
        c_core(k).start()

    def stage_1(k):
        c_core(k).wait()
        add_in(k, half, 256, recv_core)
        c_one(k).start()

    def stage_2(k):
        c_one(k).wait()
        add_in(k, quarter, 128, recv_one)
        @pl.when(is_end)
        def _():
            c_in(k).start()

    def stage_3(k):
        @pl.when(is_end)
        def _():
            c_in(k).wait_send()
        @pl.when(is_mid)
        def _():
            c_out(k).wait_recv()
            add_in(k, far, 64, recv_z)
            c_mid(k).start()

    def stage_4(k):
        @pl.when(is_mid)
        def _():
            c_mid(k).wait()
            add_in(k, near, 64, recv_mid)
            c_out(k).start()

    def stage_5(k):
        @pl.when(is_mid)
        def _():
            c_out(k).wait_send()
        @pl.when(is_end)
        def _():
            c_in(k).wait_recv()
            add_in(k, near, 64, recv_z)
            c_two(k).start()

    def stage_6(k):
        @pl.when(is_end)
        def _():
            c_two(k).wait()
            spot = pl.ds(pl.multiple_of(mine, 32), 32)
            full_buf[k, spot, :] = grad_buf[k, spot, :] + recv_two[k]
            g_two(k).start()

    def stage_7(k):
        @pl.when(is_end)
        def _():
            g_two(k).wait()
            g_in(k).start()

    def stage_8(k):
        @pl.when(is_end)
        def _():
            g_in(k).wait_send()
        @pl.when(is_mid)
        def _():
            g_out(k).wait_recv()
            g_mid(k).start()

    def stage_9(k):
        @pl.when(is_mid)
        def _():
            g_mid(k).wait()
            g_out(k).start()

    def stage_10(k):
        @pl.when(is_mid)
        def _():
            g_out(k).wait_send()
        @pl.when(is_end)
        def _():
            g_in(k).wait_recv()
        g_one(k).start()

    def stage_11(k):
        g_one(k).wait()
        g_core(k).start()

    def stage_12(k):
        g_core(k).wait()
        after(k)

    stages = (stage_0, stage_1, stage_2, stage_3, stage_4, stage_5, stage_6, stage_7, stage_8, stage_9, stage_10, stage_11, stage_12)

    def tick(t, carry):
        for num, stage in enumerate(stages):
            k = t - num * LAG
            pl.when((k >= 0) & (k < chunks))(functools.partial(stage, k))
        return carry

    lax.fori_loop(0, chunks + STAGES * LAG, tick, 0)


def scratch(chunks, cols):
    return [
        pltpu.VMEM((chunks, 512, cols), jnp.bfloat16),
        pltpu.VMEM((chunks, 512, cols), jnp.bfloat16),
        pltpu.VMEM((chunks, 256, cols), jnp.bfloat16),
        pltpu.VMEM((chunks, 128, cols), jnp.bfloat16),
        pltpu.VMEM((chunks, 64, cols), jnp.bfloat16),
        pltpu.VMEM((chunks, 64, cols), jnp.bfloat16),
        pltpu.VMEM((chunks, 32, cols), jnp.bfloat16),
        pltpu.SemaphoreType.DMA((10, chunks)),
        pltpu.SemaphoreType.DMA((10, chunks)),
    ]


def windows(up_one, down_one, merge, up_two, down_two, head):
    table = []
    for layer in reversed(range(3)):
        for part in range(4):
            table.append([(down_two, (layer, pl.ds(part * 512, 512)), (pl.ds(0, 512),))])
        for part in range(4):
            table.append([(up_two, (layer, pl.ds(0, 512), pl.ds(part * 512, 512)), (pl.ds(0, 512),))])
    for part in range(2):
        table.append([(head, (pl.ds(0, 512), pl.ds(part * 512, 512)), (pl.ds(0, 512),))])
    table.append([(merge, (pl.ds(0, 512),), (pl.ds(0, 512),))])
    table.append([(down_one, (layer,), (pl.ds(0, 512), pl.ds(layer * 128, 128))) for layer in range(4)])
    table.append([(up_one, (layer,), (pl.ds(layer * 128, 128),)) for layer in range(4)])
    return table


CHUNKS = 29


def reduce_kernel(*refs):
    ups_one, downs_one, merge, ups_two, downs_two, head = refs[0:4], refs[4:8], refs[8], refs[9:12], refs[12:15], refs[15]
    outs = refs[16:22]
    load_sem, out_sem = refs[22:24]
    bufs = refs[24:]
    grad_buf, full_buf = bufs[0:2]
    loads = windows(ups_one, downs_one, merge, ups_two, downs_two, head)
    stores = windows(*outs)

    def place(array, spot):
        if isinstance(array, tuple):
            return array[spot[0]].at[spot[1:]] if len(spot) > 1 else array[spot[0]]
        return array.at[spot]

    for k, pieces in enumerate(loads):
        for array, spot, inside in pieces:
            pltpu.make_async_copy(place(array, spot), grad_buf.at[(k,) + inside], load_sem.at[k]).start()

    def before(k):
        pltpu.make_async_copy(grad_buf.at[k], grad_buf.at[k], load_sem.at[k]).wait()

    def after(k):
        for num, pieces in enumerate(stores):
            @pl.when(k == num)
            def _():
                for array, spot, inside in pieces:
                    pltpu.make_async_copy(full_buf.at[(num,) + inside], place(array, spot), out_sem.at[num]).start()

    all_reduce_body(CHUNKS, *bufs, before, after)
    for k in range(CHUNKS):
        pltpu.make_async_copy(full_buf.at[k], full_buf.at[k], out_sem.at[k]).wait()


def reduce_grads(ups_one, downs_one, merge, ups_two, downs_two, head):
    any_hbm = pl.BlockSpec(memory_space=pltpu.HBM)
    shapes = ((4, 128, 512), (4, 512, 128), (512, 512), (3, 512, 2048), (3, 2048, 512), (512, 1024))
    return pl.pallas_call(
        reduce_kernel,
        out_shape=[jax.ShapeDtypeStruct(shape, jnp.bfloat16) for shape in shapes],
        in_specs=[any_hbm] * 16,
        out_specs=[any_hbm] * 6,
        scratch_shapes=[pltpu.SemaphoreType.DMA((CHUNKS,)), pltpu.SemaphoreType.DMA((CHUNKS,))] + scratch(CHUNKS, 512),
        compiler_params=pltpu.CompilerParams(has_side_effects=True, vmem_limit_bytes=52 * 2**20),
        cost_estimate=pl.CostEstimate(flops=10**9, bytes_accessed=3 * 10**7, transcendentals=0),
    )(*ups_one, *downs_one, merge, *ups_two, *downs_two, head)


def solution(mesh):
    data_devs = mesh.shape['data']

    def local_step(x_now, labels_now, x_next, up_one, down_one, merge_proj, up_two, down_two, head_proj, vel_up_one, vel_down_one, vel_merge_proj, vel_up_two, vel_down_two, vel_head_proj):
        params = (up_one, down_one, merge_proj, up_two, down_two, head_proj)
        velocities = (vel_up_one, vel_down_one, vel_merge_proj, vel_up_two, vel_down_two, vel_head_proj)
        weights = cast_weights(params)
        ups_one, downs_one, merge_w, ups_two, downs_two, head_w = weights
        img_count, tokens, width = x_now.shape
        depth_one = len(ups_one)
        depth_two = len(ups_two)
        logits, saved = model_forward(x_now, weights)
        saved_one, merged, saved_two, head_in_b, head_back = saved
        grad_logits = loss_grad(logits, labels_now, img_count * data_devs)
        sum_head = contract_rows(head_in_b, jnp.pad(grad_logits, ((0, 0), (0, 24)))).astype(jnp.bfloat16)
        grad_resid = head_input_grad(grad_logits, head_w, head_back, tokens // 4)
        sums_up_two = [None] * depth_two
        sums_down_two = [None] * depth_two
        for layer_num in reversed(range(depth_two)):
            grad_resid, grad_up, grad_down = block_backward(grad_resid, saved_two[layer_num], ups_two[layer_num], downs_two[layer_num])
            sums_down_two[layer_num] = grad_down.astype(jnp.bfloat16)
            sums_up_two[layer_num] = grad_up.astype(jnp.bfloat16)
        sum_merge = contract_rows(merged, grad_resid).astype(jnp.bfloat16)
        grad_resid = contract_cols(grad_resid, merge_w).astype(jnp.bfloat16).reshape(img_count * tokens, width)
        sums_up_one = [None] * depth_one
        sums_down_one = [None] * depth_one
        for layer_num in reversed(range(depth_one)):
            grad_resid, grad_up, grad_down = block_backward(grad_resid, saved_one[layer_num], ups_one[layer_num], downs_one[layer_num])
            sums_down_one[layer_num] = grad_down.astype(jnp.bfloat16)
            sums_up_one[layer_num] = grad_up.astype(jnp.bfloat16)
        grad_sums = reduce_grads(sums_up_one, sums_down_one, sum_merge, sums_up_two, sums_down_two, sum_head)
        grad_sums = tuple(grad_sums[:5]) + (grad_sums[5][:, :1000],)
        return finish_step(params, velocities, grad_sums, x_next)

    replicated = P()
    batch_split = P('data')
    in_specs = (batch_split, batch_split, batch_split) + (replicated,) * 12
    out_specs = (batch_split,) + (replicated,) * 12
    return jax.shard_map(local_step, mesh=mesh, in_specs=in_specs, out_specs=out_specs, check_vma=False)
```

```python
import functools

import jax
import jax.numpy as jnp
from jax import lax
from jax.experimental import pallas as pl
from jax.experimental.pallas import tpu as pltpu
from jax.sharding import PartitionSpec as P

MOMENTUM = 0.9
TRUST = 0.1
LN_EPS = 1e-6


def layer_norm(values):
    row_mean = jnp.mean(values, axis=-1, keepdims=True)
    centered = values - row_mean
    variance = jnp.mean(centered * centered, axis=-1, keepdims=True)
    return centered * lax.rsqrt(variance + LN_EPS)


def gelu_tanh(values):
    return jax.nn.gelu(values, approximate=True)


def contract_rows(lhs_mat, rhs_mat):
    return lax.dot_general(lhs_mat, rhs_mat, (((0,), (0,)), ((), ())), preferred_element_type=jnp.float32)


def contract_cols(lhs_mat, rhs_mat):
    return lax.dot_general(lhs_mat, rhs_mat, (((1,), (1,)), ((), ())), preferred_element_type=jnp.float32)


def to_bf16_layers(stacked):
    return [stacked[layer_num].astype(jnp.bfloat16) for layer_num in range(stacked.shape[0])]


def cast_weights(params):
    up_one, down_one, merge_proj, up_two, down_two, head_proj = params
    return (to_bf16_layers(up_one), to_bf16_layers(down_one), merge_proj.astype(jnp.bfloat16), to_bf16_layers(up_two), to_bf16_layers(down_two), head_proj.astype(jnp.bfloat16))


def block_forward(residual, w_up, w_down):
    normed, norm_back = jax.vjp(layer_norm, residual.astype(jnp.float32))
    normed_b = normed.astype(jnp.bfloat16)
    pre_act = jnp.dot(normed_b, w_up, preferred_element_type=jnp.float32)
    activated, gelu_back = jax.vjp(gelu_tanh, pre_act)
    activated_b = activated.astype(jnp.bfloat16)
    block_out = jnp.dot(activated_b, w_down, preferred_element_type=jnp.float32)
    new_residual = (residual.astype(jnp.float32) + block_out).astype(jnp.bfloat16)
    return new_residual, (normed_b, activated_b, norm_back, gelu_back)


def block_backward(grad_out, saved, w_up, w_down):
    normed_b, activated_b, norm_back, gelu_back = saved
    grad_down = contract_rows(activated_b, grad_out)
    grad_act = contract_cols(grad_out, w_down)
    grad_pre = gelu_back(grad_act)[0].astype(jnp.bfloat16)
    grad_up = contract_rows(normed_b, grad_pre)
    grad_normed = contract_cols(grad_pre, w_up)
    grad_in = norm_back(grad_normed)[0] + grad_out.astype(jnp.float32)
    return grad_in.astype(jnp.bfloat16), grad_up, grad_down


def model_forward(images, weights):
    ups_one, downs_one, merge_w, ups_two, downs_two, head_w = weights
    img_count, tokens, width = images.shape
    residual = images.reshape(img_count * tokens, width)
    saved_one = []
    for w_up, w_down in zip(ups_one, downs_one):
        residual, saved = block_forward(residual, w_up, w_down)
        saved_one.append(saved)
    merged = residual.reshape(img_count * tokens // 4, 4 * width)
    residual = jnp.dot(merged, merge_w, preferred_element_type=jnp.float32).astype(jnp.bfloat16)
    saved_two = []
    for w_up, w_down in zip(ups_two, downs_two):
        residual, saved = block_forward(residual, w_up, w_down)
        saved_two.append(saved)
    pooled = jnp.mean(residual.reshape(img_count, tokens // 4, -1), axis=1, dtype=jnp.float32)
    head_in, head_back = jax.vjp(layer_norm, pooled)
    head_in_b = head_in.astype(jnp.bfloat16)
    logits = jnp.dot(head_in_b, head_w, preferred_element_type=jnp.float32)
    return logits, (saved_one, merged, saved_two, head_in_b, head_back)


def loss_grad(logits, labels, global_batch):
    soft_probs = jax.nn.softmax(logits, axis=-1)
    class_ids = jnp.arange(logits.shape[1], dtype=jnp.int32)
    onehot = (labels[:, None] == class_ids[None, :]).astype(jnp.float32)
    return ((soft_probs - onehot) / global_batch).astype(jnp.bfloat16)


def head_input_grad(grad_logits, head_w, head_back, merged_tokens):
    grad_pooled = head_back(contract_cols(grad_logits, head_w))[0] / merged_tokens
    img_count, width_two = grad_pooled.shape
    spread = jnp.broadcast_to(grad_pooled.astype(jnp.bfloat16)[:, None, :], (img_count, merged_tokens, width_two))
    return spread.reshape(img_count * merged_tokens, width_two)


MESH = pl.DeviceIdType.MESH
ROWS = 512
LAG = 3
STAGES = 12


def all_reduce_body(chunks, grad_buf, full_buf, recv_core, recv_one, recv_z, recv_mid, recv_two, send_sem, recv_sem, before, after, extra):
    me = lax.axis_index('data')
    core = me % 2
    x_pos = (me // 2) % 2
    y_pos = (me // 4) % 2
    z_pos = me // 8
    one = x_pos * (1 - core) + y_pos * core
    two = y_pos * (1 - core) + x_pos * core
    one_step = 2 * (1 - core) + 4 * core
    two_step = 4 * (1 - core) + 2 * core
    dev_core = me + 1 - 2 * core
    dev_one = me + one_step * (1 - 2 * one)
    dev_two = me + two_step * (1 - 2 * two)
    upper = z_pos // 2
    is_end = (z_pos % 3) == 0
    is_mid = (z_pos % 3) != 0
    dev_inner = me + 8 * (1 - 2 * upper)
    dev_outer = me - 8 * (1 - 2 * upper)
    half = core * 256
    quarter = half + one * 128
    near = quarter + upper * 64
    far = quarter + (1 - upper) * 64
    mine = near + two * 32

    def rows(chunk, start, size):
        return grad_buf.at[chunk, pl.ds(pl.multiple_of(start, 32), size)]

    def full(chunk, start, size):
        return full_buf.at[chunk, pl.ds(pl.multiple_of(start, 32), size)]

    def remote(src, dst, which, chunk, dev):
        return pltpu.make_async_remote_copy(src_ref=src, dst_ref=dst, send_sem=send_sem.at[which, chunk], recv_sem=recv_sem.at[which, chunk], device_id=(dev,), device_id_type=MESH)

    def add_in(chunk, start, size, recv):
        def step(num, carry):
            spot = pl.ds(pl.multiple_of(start + num * 32, 32), 32)
            grad_buf[chunk, spot, :] = grad_buf[chunk, spot, :] + recv[chunk, pl.ds(pl.multiple_of(num * 32, 32), 32), :]
            return carry
        lax.fori_loop(0, size // 32, step, 0)

    def c_core(k):
        return remote(rows(k, 256 - half, 256), recv_core.at[k], 0, k, dev_core)

    def c_one(k):
        return remote(rows(k, half + (1 - one) * 128, 128), recv_one.at[k], 1, k, dev_one)

    def c_in(k):
        return remote(rows(k, far, 64), recv_z.at[k], 2, k, dev_inner)

    def c_mid(k):
        return remote(rows(k, far, 64), recv_mid.at[k], 3, k, dev_inner)

    def c_out(k):
        return remote(rows(k, near, 64), recv_z.at[k], 2, k, dev_outer)

    def c_two(k):
        return remote(rows(k, near + (1 - two) * 32, 32), recv_two.at[k], 4, k, dev_two)

    def g_two(k):
        return remote(full(k, mine, 32), full(k, mine, 32), 5, k, dev_two)

    def g_in(k):
        return remote(full(k, near, 64), full(k, near, 64), 6, k, dev_inner)

    def g_mid(k):
        return remote(full(k, near, 64), full(k, near, 64), 7, k, dev_inner)

    def g_out(k):
        return remote(full(k, far, 64), full(k, far, 64), 6, k, dev_outer)

    def g_one(k):
        return remote(full(k, quarter, 128), full(k, quarter, 128), 8, k, dev_one)

    def g_core(k):
        return remote(full(k, half, 256), full(k, half, 256), 9, k, dev_core)

    def stage_0(k):
        before(k)
        c_core(k).start()

    def stage_1(k):
        c_core(k).wait()
        add_in(k, half, 256, recv_core)
        c_one(k).start()

    def stage_2(k):
        c_one(k).wait()
        add_in(k, quarter, 128, recv_one)
        @pl.when(is_end)
        def _():
            c_in(k).start()

    def stage_3(k):
        @pl.when(is_end)
        def _():
            c_in(k).wait_send()
        @pl.when(is_mid)
        def _():
            c_out(k).wait_recv()
            add_in(k, far, 64, recv_z)
            c_mid(k).start()

    def stage_4(k):
        @pl.when(is_mid)
        def _():
            c_mid(k).wait()
            add_in(k, near, 64, recv_mid)
            c_out(k).start()

    def stage_5(k):
        @pl.when(is_mid)
        def _():
            c_out(k).wait_send()
        @pl.when(is_end)
        def _():
            c_in(k).wait_recv()
            add_in(k, near, 64, recv_z)
            c_two(k).start()

    def stage_6(k):
        @pl.when(is_end)
        def _():
            c_two(k).wait()
            spot = pl.ds(pl.multiple_of(mine, 32), 32)
            full_buf[k, spot, :] = grad_buf[k, spot, :] + recv_two[k]
            g_two(k).start()

    def stage_7(k):
        @pl.when(is_end)
        def _():
            g_two(k).wait()
            g_in(k).start()

    def stage_8(k):
        @pl.when(is_end)
        def _():
            g_in(k).wait_send()
        @pl.when(is_mid)
        def _():
            g_out(k).wait_recv()
            g_mid(k).start()

    def stage_9(k):
        @pl.when(is_mid)
        def _():
            g_mid(k).wait()
            g_out(k).start()

    def stage_10(k):
        @pl.when(is_mid)
        def _():
            g_out(k).wait_send()
        @pl.when(is_end)
        def _():
            g_in(k).wait_recv()
        g_one(k).start()

    def stage_11(k):
        g_one(k).wait()
        g_core(k).start()

    def stage_12(k):
        g_core(k).wait()
        after(k)

    stages = (stage_0, stage_1, stage_2, stage_3, stage_4, stage_5, stage_6, stage_7, stage_8, stage_9, stage_10, stage_11, stage_12)

    def tick(t, carry):
        for num, stage in enumerate(stages):
            k = t - num * LAG
            pl.when((k >= 0) & (k < chunks))(functools.partial(stage, k))
        extra(t)
        return carry

    lax.fori_loop(0, chunks + STAGES * LAG, tick, 0)


def scratch(chunks, cols):
    return [
        pltpu.VMEM((chunks, 512, cols), jnp.bfloat16),
        pltpu.VMEM((chunks, 512, cols), jnp.bfloat16),
        pltpu.VMEM((chunks, 256, cols), jnp.bfloat16),
        pltpu.VMEM((chunks, 128, cols), jnp.bfloat16),
        pltpu.VMEM((chunks, 64, cols), jnp.bfloat16),
        pltpu.VMEM((chunks, 64, cols), jnp.bfloat16),
        pltpu.VMEM((chunks, 32, cols), jnp.bfloat16),
        pltpu.SemaphoreType.DMA((10, chunks)),
        pltpu.SemaphoreType.DMA((10, chunks)),
    ]


CHUNKS = 29
HEAD_A, HEAD_B, MERGE, DOWN_ONE, UP_ONE = 24, 25, 26, 27, 28
LANES = 512


def two_chunk(layer, is_up, part):
    return (2 - layer) * 8 + is_up * 4 + part


def windows(up_one, down_one, merge, up_two, down_two):
    whole = (pl.ds(0, 512),)
    table = {}
    for layer in range(3):
        for part in range(4):
            table[two_chunk(layer, 0, part)] = [(down_two, (layer, pl.ds(part * 512, 512)), whole)]
            table[two_chunk(layer, 1, part)] = [(up_two, (layer, pl.ds(0, 512), pl.ds(part * 512, 512)), whole)]
    table[MERGE] = [(merge, whole, whole)]
    table[DOWN_ONE] = [(down_one, (layer,), (pl.ds(0, 512), pl.ds(layer * 128, 128))) for layer in range(4)]
    table[UP_ONE] = [(up_one, (layer,), (pl.ds(layer * 128, 128),)) for layer in range(4)]
    return table


def place(array, spot):
    if isinstance(array, tuple):
        return array[spot[0]].at[spot[1:]] if len(spot) > 1 else array[spot[0]]
    return array.at[spot]


def block_squares(read, sums, chunk, lanes):
    def step(num, carry):
        total = jnp.zeros((8, lanes), jnp.float32)
        for part in range(4):
            vals = read(pl.ds(pl.multiple_of(num * 128 + part * 32, 32), 32)).astype(jnp.float32)
            vals = vals * vals
            total = total + (vals[0:8] + vals[8:16]) + (vals[16:24] + vals[24:32])
        sums[chunk, pl.ds(num, 1), 0:lanes] = jnp.sum(total, axis=0, keepdims=True)
        return carry
    lax.fori_loop(0, 4, step, 0)


def reduce_kernel(*refs):
    ups_one, downs_one, merge, ups_two, downs_two, head = refs[0:4], refs[4:8], refs[8], refs[9:12], refs[12:15], refs[15]
    w_up_one, w_down_one, w_merge, w_up_two, w_down_two, w_head = refs[16:22]
    out, w_sums, g_sums = refs[22:25]
    load_sem, out_sem, w_sem, w_buf, w_head_buf = refs[25:30]
    bufs = refs[30:]
    grad_buf, full_buf = bufs[0:2]
    loads = windows(ups_one, downs_one, merge, ups_two, downs_two)
    whole = (pl.ds(0, 512),)
    loads[HEAD_A] = [(head, (pl.ds(0, 512), pl.ds(0, 512)), whole)]
    loads[HEAD_B] = [(head, (pl.ds(0, 512), pl.ds(512, 512)), whole)]
    for k in range(CHUNKS):
        for array, spot, inside in loads[k]:
            pltpu.make_async_copy(place(array, spot), grad_buf.at[(k,) + inside], load_sem.at[k]).start()
    w_loads = windows(w_up_one, w_down_one, w_merge, w_up_two, w_down_two)

    def w_start(k):
        if k == HEAD_A:
            pltpu.make_async_copy(w_head, w_head_buf, w_sem.at[k]).start()
        elif k != HEAD_B:
            for array, spot, inside in w_loads[k]:
                pltpu.make_async_copy(place(array, spot), w_buf.at[(k % 3,) + inside], w_sem.at[k]).start()

    for k in range(3):
        w_start(k)

    def w_step(t):
        @pl.when((t < CHUNKS) & (t != HEAD_A) & (t != HEAD_B))
        def _():
            slot = t % 3
            pltpu.make_async_copy(w_buf.at[slot], w_buf.at[slot], w_sem.at[t]).wait()
            block_squares(lambda rows: w_buf[slot, rows, :], w_sums, t, LANES)

        @pl.when(t == HEAD_A)
        def _():
            pltpu.make_async_copy(w_head, w_head_buf, w_sem.at[HEAD_A]).wait()
            block_squares(lambda rows: w_head_buf[rows, 0:512], w_sums, HEAD_A, LANES)
            w_sums[HEAD_B] = jnp.zeros((4, LANES), jnp.float32)
            block_squares(lambda rows: w_head_buf[rows, 512:1000], w_sums, HEAD_B, 488)

        for num in range(CHUNKS - 3):
            @pl.when(t == num)
            def _():
                w_start(num + 3)

    def before(k):
        pltpu.make_async_copy(grad_buf.at[k], grad_buf.at[k], load_sem.at[k]).wait()

    def after(k):
        pltpu.make_async_copy(full_buf.at[k], out.at[k], out_sem.at[k]).start()
        block_squares(lambda rows: full_buf[k, rows, :], g_sums, k, LANES)

    all_reduce_body(CHUNKS, *bufs, before, after, w_step)
    for k in range(CHUNKS):
        pltpu.make_async_copy(full_buf.at[k], full_buf.at[k], out_sem.at[k]).wait()


def reduce_grads(ups_one, downs_one, merge, ups_two, downs_two, head, params):
    any_hbm = pl.BlockSpec(memory_space=pltpu.HBM)
    sums_shape = (CHUNKS, 4, LANES)
    return pl.pallas_call(
        reduce_kernel,
        out_shape=[jax.ShapeDtypeStruct((CHUNKS, 512, 512), jnp.bfloat16)] + [jax.ShapeDtypeStruct(sums_shape, jnp.float32)] * 2,
        in_specs=[any_hbm] * 22,
        out_specs=[any_hbm] + [pl.BlockSpec(memory_space=pltpu.VMEM)] * 2,
        scratch_shapes=[pltpu.SemaphoreType.DMA((CHUNKS,))] * 3 + [pltpu.VMEM((3, 512, 512), jnp.float32), pltpu.VMEM((512, 1000), jnp.float32)] + scratch(CHUNKS, 512),
        compiler_params=pltpu.CompilerParams(has_side_effects=True, vmem_limit_bytes=58 * 2**20),
        cost_estimate=pl.CostEstimate(flops=10**9, bytes_accessed=3 * 10**7, transcendentals=0),
    )(*ups_one, *downs_one, merge, *ups_two, *downs_two, head, *params)


RING = 8
AHEAD = 4
PAD_IMG = 208
PAD_ROWS = 416


def gelu_explicit(vals):
    inner = 0.7978845608028654 * (vals + 0.044715 * (vals * vals * vals))
    return vals * (0.5 * (1.0 + jnp.tanh(inner)))


def dot32(lhs, rhs):
    return jnp.dot(lhs, rhs, preferred_element_type=jnp.float32)


def next_kernel(*refs):
    grads, w_in, v_in = refs[0], refs[1:7], refs[7:13]
    w_sums, g_sums, images = refs[13:16]
    logits, w_out, v_out = refs[16], refs[17:23], refs[23:29]
    load_sem, store_sem, ring_w, ring_v, ring_g, head_w, head_v, head_g, cast, coef, resid_one, resid_two, normed_two, total_two = refs[29:43]

    whole = (pl.ds(0, 512),)
    arrays = [windows(*group[0:5]) for group in (w_in, v_in, w_out, v_out)]
    order = [UP_ONE, DOWN_ONE, MERGE, HEAD_A]
    for layer in range(3):
        order += [two_chunk(layer, 1, part) for part in range(4)] + [two_chunk(layer, 0, part) for part in range(4)]
    count = len(order)

    def start_loads(num):
        k = order[num]
        if k == HEAD_A:
            pltpu.make_async_copy(w_in[5], head_w, load_sem.at[0, k]).start()
            pltpu.make_async_copy(v_in[5], head_v, load_sem.at[1, k]).start()
            pltpu.make_async_copy(grads.at[pl.ds(HEAD_A, 2)], head_g, load_sem.at[2, k]).start()
            return
        slot = num % RING
        for which, ring in ((0, ring_w), (1, ring_v)):
            for array, spot, inside in arrays[which][k]:
                pltpu.make_async_copy(place(array, spot), ring.at[(slot,) + inside], load_sem.at[which, k]).start()
        pltpu.make_async_copy(grads.at[k], ring_g.at[slot], load_sem.at[2, k]).start()

    def wait_loads(num):
        k = order[num]
        slot = num % RING
        bufs = (head_w, head_v, head_g) if k == HEAD_A else (ring_w.at[slot], ring_v.at[slot], ring_g.at[slot])
        for which in range(3):
            pltpu.make_async_copy(bufs[which], bufs[which], load_sem.at[which, k]).wait()

    def start_stores(num):
        k = order[num]
        if k == HEAD_A:
            pltpu.make_async_copy(head_w, w_out[5], store_sem.at[0, k]).start()
            pltpu.make_async_copy(head_v, v_out[5], store_sem.at[1, k]).start()
            return
        slot = num % RING
        for which, ring in ((0, ring_w), (1, ring_v)):
            for array, spot, inside in arrays[2 + which][k]:
                pltpu.make_async_copy(ring.at[(slot,) + inside], place(array, spot), store_sem.at[which, k]).start()

    def wait_stores(num):
        k = order[num]
        slot = num % RING
        bufs = (head_w, head_v) if k == HEAD_A else (ring_w.at[slot], ring_v.at[slot])
        for which in range(2):
            pltpu.make_async_copy(bufs[which], bufs[which], store_sem.at[which, k]).wait()

    for num in range(AHEAD):
        start_loads(num)

    def ratio(w_total, g_total):
        return TRUST * (jnp.sqrt(w_total) / jnp.sqrt(g_total))

    def total(sums, first, size):
        return jnp.sum(jnp.sum(jnp.sum(sums[first:first + size], axis=0), axis=0, keepdims=True), axis=1, keepdims=True)

    for first, size in [(0, 4), (4, 4), (8, 4), (12, 4), (16, 4), (20, 4), (HEAD_A, 2), (MERGE, 1)]:
        value = ratio(total(w_sums, first, size), total(g_sums, first, size))
        for k in range(first, first + size):
            coef[k] = jnp.broadcast_to(value, (4, LANES))
    by_row = ratio(jnp.sum(w_sums[UP_ONE], axis=1, keepdims=True), jnp.sum(g_sums[UP_ONE], axis=1, keepdims=True))
    coef[UP_ONE] = jnp.broadcast_to(by_row, (4, LANES))
    for layer in range(4):
        lanes = pl.ds(layer * 128, 128)
        lane_total = [jnp.sum(jnp.sum(sums[DOWN_ONE, :, lanes], axis=0, keepdims=True), axis=1, keepdims=True) for sums in (w_sums, g_sums)]
        coef[DOWN_ONE, :, lanes] = jnp.broadcast_to(ratio(*lane_total), (4, 128))

    def apply_update(k, w_ref, v_ref, g_ref, lanes, width):
        def step(num, carry):
            rows = pl.ds(pl.multiple_of(num * 32, 32), 32)
            factor = coef[k, pl.ds(num // 4, 1), 0:width]
            new_v = MOMENTUM * v_ref[rows, lanes] + factor * g_ref[rows, 0:width].astype(jnp.float32)
            new_w = w_ref[rows, lanes] - new_v
            v_ref[rows, lanes] = new_v
            w_ref[rows, lanes] = new_w
            cast[k, rows, 0:width] = new_w.astype(jnp.bfloat16)
            return carry
        lax.fori_loop(0, 16, step, 0)

    def update(num):
        k = order[num]
        wait_loads(num)
        if k == HEAD_A:
            apply_update(HEAD_A, head_w, head_v, head_g.at[0], slice(0, 512), 512)
            cast[HEAD_B] = jnp.zeros((512, 512), jnp.bfloat16)
            apply_update(HEAD_B, head_w, head_v, head_g.at[1], slice(512, 1000), 488)
        else:
            slot = num % RING
            apply_update(k, ring_w.at[slot], ring_v.at[slot], ring_g.at[slot], slice(0, 512), 512)
        start_stores(num)
        later = num + AHEAD
        if later < count:
            if later >= RING and order[later - RING] != HEAD_A:
                wait_stores(later - RING)
                waited.add(later - RING)
            start_loads(later)

    waited = set()

    def one_body(num, carry):
        layer = num // 4
        rows = pl.ds(pl.multiple_of((num % 4) * PAD_ROWS, 32), PAD_ROWS)
        resid = resid_one[rows, :].astype(jnp.float32)
        normed = layer_norm(resid).astype(jnp.bfloat16)
        pre = dot32(normed, cast[UP_ONE, pl.ds(pl.multiple_of(layer * 128, 128), 128), :])
        act = gelu_explicit(pre).astype(jnp.bfloat16)
        out = dot32(act, cast[DOWN_ONE, :, pl.ds(pl.multiple_of(layer * 128, 128), 128)])
        resid_one[rows, :] = (resid + out).astype(jnp.bfloat16)
        return carry

    def merge_body():
        value = jnp.zeros((PAD_ROWS, 512), jnp.float32)
        for part in range(4):
            value = value + dot32(resid_one[part * PAD_ROWS:(part + 1) * PAD_ROWS, :], cast[MERGE, part * 128:(part + 1) * 128, :])
        resid_two[...] = value.astype(jnp.bfloat16)

    def two_start():
        normed_two[...] = layer_norm(resid_two[...].astype(jnp.float32)).astype(jnp.bfloat16)
        total_two[...] = jnp.zeros_like(total_two)

    def two_body(layer, part):
        pre = dot32(normed_two[...], cast[two_chunk(layer, 1, 0) + part])
        act = gelu_explicit(pre).astype(jnp.bfloat16)
        total_two[...] += dot32(act, cast[two_chunk(layer, 0, 0) + part])

    def two_end():
        resid_two[...] = (resid_two[...].astype(jnp.float32) + total_two[...]).astype(jnp.bfloat16)

    resid_one[...] = images[...]
    for num in range(4):
        update(num)
    for num in range(4, 12):
        update(num)
        lax.fori_loop((num - 4) * 2, (num - 4) * 2 + 2, one_body, 0)
    merge_body()
    for layer in range(3):
        two_start()
        if layer < 2:
            def group(part, carry, layer=layer):
                two_body(layer, part)
                return carry
            for part in range(4):
                update(12 + layer * 8 + part * 2)
                update(13 + layer * 8 + part * 2)
                lax.fori_loop(part, part + 1, group, 0)
        else:
            def group(part, carry, layer=layer):
                two_body(layer, part)
                return carry
            lax.fori_loop(0, 4, group, 0)
        two_end()
    pooled = [jnp.sum(resid_two[img * PAD_IMG:(img + 1) * PAD_IMG, :].astype(jnp.float32), axis=0, keepdims=True) / 196.0 for img in range(2)]
    head_in = layer_norm(jnp.concatenate(pooled + [jnp.zeros((6, 512), jnp.float32)], axis=0)).astype(jnp.bfloat16)
    logits[:, 0:512] = dot32(head_in, cast[HEAD_A])[0:2]
    logits[:, 512:1000] = dot32(head_in, cast[HEAD_B])[0:2, 0:488]
    for num in range(count):
        if num not in waited:
            wait_stores(num)


def arrange(images):
    count, tokens, width = images.shape
    split = images.reshape(count, tokens // 4, 4, width).transpose(2, 0, 1, 3)
    split = jnp.pad(split, ((0, 0), (0, 0), (0, PAD_IMG - tokens // 4), (0, 0)))
    return split.reshape(4 * count * PAD_IMG, width)


def update_and_forward(params, velocities, grads, w_sums, g_sums, x_next):
    any_hbm = pl.BlockSpec(memory_space=pltpu.HBM)
    in_vmem = pl.BlockSpec(memory_space=pltpu.VMEM)
    shapes = [jax.ShapeDtypeStruct(array.shape, array.dtype) for array in params]
    outs = pl.pallas_call(
        next_kernel,
        out_shape=[jax.ShapeDtypeStruct((2, 1000), jnp.float32)] + shapes + shapes,
        in_specs=[any_hbm] * 13 + [in_vmem] * 3,
        out_specs=[in_vmem] + [any_hbm] * 12,
        scratch_shapes=[
            pltpu.SemaphoreType.DMA((3, CHUNKS)),
            pltpu.SemaphoreType.DMA((2, CHUNKS)),
            pltpu.VMEM((RING, 512, 512), jnp.float32),
            pltpu.VMEM((RING, 512, 512), jnp.float32),
            pltpu.VMEM((RING, 512, 512), jnp.bfloat16),
            pltpu.VMEM((512, 1000), jnp.float32),
            pltpu.VMEM((512, 1000), jnp.float32),
            pltpu.VMEM((2, 512, 512), jnp.bfloat16),
            pltpu.VMEM((CHUNKS, 512, 512), jnp.bfloat16),
            pltpu.VMEM((CHUNKS, 4, LANES), jnp.float32),
            pltpu.VMEM((4 * PAD_ROWS, 128), jnp.bfloat16),
            pltpu.VMEM((PAD_ROWS, 512), jnp.bfloat16),
            pltpu.VMEM((PAD_ROWS, 512), jnp.bfloat16),
            pltpu.VMEM((PAD_ROWS, 512), jnp.float32),
        ],
        compiler_params=pltpu.CompilerParams(vmem_limit_bytes=58 * 2**20),
        cost_estimate=pl.CostEstimate(flops=10**10, bytes_accessed=135 * 10**6, transcendentals=0),
    )(grads, *params, *velocities, w_sums, g_sums, arrange(x_next))
    return tuple(outs)


def solution(mesh):
    data_devs = mesh.shape['data']

    def local_step(x_now, labels_now, x_next, up_one, down_one, merge_proj, up_two, down_two, head_proj, vel_up_one, vel_down_one, vel_merge_proj, vel_up_two, vel_down_two, vel_head_proj):
        params = (up_one, down_one, merge_proj, up_two, down_two, head_proj)
        velocities = (vel_up_one, vel_down_one, vel_merge_proj, vel_up_two, vel_down_two, vel_head_proj)
        weights = cast_weights(params)
        ups_one, downs_one, merge_w, ups_two, downs_two, head_w = weights
        img_count, tokens, width = x_now.shape
        depth_one = len(ups_one)
        depth_two = len(ups_two)
        logits, saved = model_forward(x_now, weights)
        saved_one, merged, saved_two, head_in_b, head_back = saved
        grad_logits = loss_grad(logits, labels_now, img_count * data_devs)
        sum_head = contract_rows(head_in_b, jnp.pad(grad_logits, ((0, 0), (0, 24)))).astype(jnp.bfloat16)
        grad_resid = head_input_grad(grad_logits, head_w, head_back, tokens // 4)
        sums_up_two = [None] * depth_two
        sums_down_two = [None] * depth_two
        for layer_num in reversed(range(depth_two)):
            grad_resid, grad_up, grad_down = block_backward(grad_resid, saved_two[layer_num], ups_two[layer_num], downs_two[layer_num])
            sums_down_two[layer_num] = grad_down.astype(jnp.bfloat16)
            sums_up_two[layer_num] = grad_up.astype(jnp.bfloat16)
        sum_merge = contract_rows(merged, grad_resid).astype(jnp.bfloat16)
        grad_resid = contract_cols(grad_resid, merge_w).astype(jnp.bfloat16).reshape(img_count * tokens, width)
        sums_up_one = [None] * depth_one
        sums_down_one = [None] * depth_one
        for layer_num in reversed(range(depth_one)):
            grad_resid, grad_up, grad_down = block_backward(grad_resid, saved_one[layer_num], ups_one[layer_num], downs_one[layer_num])
            sums_down_one[layer_num] = grad_down.astype(jnp.bfloat16)
            sums_up_one[layer_num] = grad_up.astype(jnp.bfloat16)
        grads, w_sums, g_sums = reduce_grads(sums_up_one, sums_down_one, sum_merge, sums_up_two, sums_down_two, sum_head, params)
        return update_and_forward(params, velocities, grads, w_sums, g_sums, x_next)

    replicated = P()
    batch_split = P('data')
    in_specs = (batch_split, batch_split, batch_split) + (replicated,) * 12
    out_specs = (batch_split,) + (replicated,) * 12
    return jax.shard_map(local_step, mesh=mesh, in_specs=in_specs, out_specs=out_specs, check_vma=False)
```

```python
import functools

import jax
import jax.numpy as jnp
from jax import lax
from jax.experimental import pallas as pl
from jax.experimental.pallas import tpu as pltpu
from jax.sharding import PartitionSpec as P

MOMENTUM = 0.9
TRUST = 0.1
LN_EPS = 1e-6
CHUNKS = 29
HEAD_A, HEAD_B, MERGE, DOWN_ONE, UP_ONE = 24, 25, 26, 27, 28
HEAD_REST = 488
CLASSES = 1000
LANES = 512
RING = 8
AHEAD = 4
W_RING = 3
TOKENS_TWO = 196
PAD_IMG = 208
PAD_ROWS = 416
GELU_C = 0.7978845608028654
GELU_A = 0.044715
WIDE = 512
THIN = 128
STEP = 32
QUARTER = 64
HALF = 256
TWO_CHUNKS = 24
OCT = 8
PAIR = 16

MESH = pl.DeviceIdType.MESH
ROWS = WIDE
LAG = 3
STAGES = 12


def all_reduce_body(chunks, grad_buf, full_buf, recv_core, recv_one, recv_z, recv_mid, recv_two, send_sem, recv_sem, before, after, extra):
    me = lax.axis_index('data')
    core = me % 2
    x_pos = (me // 2) % 2
    y_pos = (me // 4) % 2
    z_pos = me // OCT
    one = x_pos * (1 - core) + y_pos * core
    two = y_pos * (1 - core) + x_pos * core
    one_step = 2 * (1 - core) + 4 * core
    two_step = 4 * (1 - core) + 2 * core
    dev_core = me + 1 - 2 * core
    dev_one = me + one_step * (1 - 2 * one)
    dev_two = me + two_step * (1 - 2 * two)
    upper = z_pos // 2
    is_end = (z_pos % 3) == 0
    is_mid = (z_pos % 3) != 0
    dev_inner = me + OCT * (1 - 2 * upper)
    dev_outer = me - OCT * (1 - 2 * upper)
    half = core * HALF
    quarter = half + one * THIN
    near = quarter + upper * QUARTER
    far = quarter + (1 - upper) * QUARTER
    mine = near + two * STEP

    def rows(chunk, start, size):
        return grad_buf.at[chunk, pl.ds(pl.multiple_of(start, STEP), size)]

    def full(chunk, start, size):
        return full_buf.at[chunk, pl.ds(pl.multiple_of(start, STEP), size)]

    def remote(src, dst, which, chunk, dev):
        return pltpu.make_async_remote_copy(src_ref=src, dst_ref=dst, send_sem=send_sem.at[which, chunk], recv_sem=recv_sem.at[which, chunk], device_id=(dev,), device_id_type=MESH)

    def add_in(chunk, start, size, recv):
        def step(num, carry):
            spot = pl.ds(pl.multiple_of(start + num * STEP, STEP), STEP)
            grad_buf[chunk, spot, :] = grad_buf[chunk, spot, :] + recv[chunk, pl.ds(pl.multiple_of(num * STEP, STEP), STEP), :]
            return carry
        lax.fori_loop(0, size // STEP, step, 0)

    def c_core(k):
        return remote(rows(k, HALF - half, HALF), recv_core.at[k], 0, k, dev_core)

    def c_one(k):
        return remote(rows(k, half + (1 - one) * THIN, THIN), recv_one.at[k], 1, k, dev_one)

    def c_in(k):
        return remote(rows(k, far, QUARTER), recv_z.at[k], 2, k, dev_inner)

    def c_mid(k):
        return remote(rows(k, far, QUARTER), recv_mid.at[k], 3, k, dev_inner)

    def c_out(k):
        return remote(rows(k, near, QUARTER), recv_z.at[k], 2, k, dev_outer)

    def c_two(k):
        return remote(rows(k, near + (1 - two) * STEP, STEP), recv_two.at[k], 4, k, dev_two)

    def g_two(k):
        return remote(full(k, mine, STEP), full(k, mine, STEP), 5, k, dev_two)

    def g_in(k):
        return remote(full(k, near, QUARTER), full(k, near, QUARTER), 6, k, dev_inner)

    def g_mid(k):
        return remote(full(k, near, QUARTER), full(k, near, QUARTER), 7, k, dev_inner)

    def g_out(k):
        return remote(full(k, far, QUARTER), full(k, far, QUARTER), 6, k, dev_outer)

    def g_one(k):
        return remote(full(k, quarter, THIN), full(k, quarter, THIN), OCT, k, dev_one)

    def g_core(k):
        return remote(full(k, half, HALF), full(k, half, HALF), 9, k, dev_core)

    def stage_0(k):
        before(k)
        c_core(k).start()

    def stage_1(k):
        c_core(k).wait()
        add_in(k, half, HALF, recv_core)
        c_one(k).start()

    def stage_2(k):
        c_one(k).wait()
        add_in(k, quarter, THIN, recv_one)
        @pl.when(is_end)
        def _():
            c_in(k).start()

    def stage_3(k):
        @pl.when(is_end)
        def _():
            c_in(k).wait_send()
        @pl.when(is_mid)
        def _():
            c_out(k).wait_recv()
            add_in(k, far, QUARTER, recv_z)
            c_mid(k).start()

    def stage_4(k):
        @pl.when(is_mid)
        def _():
            c_mid(k).wait()
            add_in(k, near, QUARTER, recv_mid)
            c_out(k).start()

    def stage_5(k):
        @pl.when(is_mid)
        def _():
            c_out(k).wait_send()
        @pl.when(is_end)
        def _():
            c_in(k).wait_recv()
            add_in(k, near, QUARTER, recv_z)
            c_two(k).start()

    def stage_6(k):
        @pl.when(is_end)
        def _():
            c_two(k).wait()
            spot = pl.ds(pl.multiple_of(mine, STEP), STEP)
            full_buf[k, spot, :] = grad_buf[k, spot, :] + recv_two[k]
            g_two(k).start()

    def stage_7(k):
        @pl.when(is_end)
        def _():
            g_two(k).wait()
            g_in(k).start()

    def stage_8(k):
        @pl.when(is_end)
        def _():
            g_in(k).wait_send()
        @pl.when(is_mid)
        def _():
            g_out(k).wait_recv()
            g_mid(k).start()

    def stage_9(k):
        @pl.when(is_mid)
        def _():
            g_mid(k).wait()
            g_out(k).start()

    def stage_10(k):
        @pl.when(is_mid)
        def _():
            g_out(k).wait_send()
        @pl.when(is_end)
        def _():
            g_in(k).wait_recv()
        g_one(k).start()

    def stage_11(k):
        g_one(k).wait()
        g_core(k).start()

    def stage_12(k):
        g_core(k).wait()
        after(k)

    stages = (stage_0, stage_1, stage_2, stage_3, stage_4, stage_5, stage_6, stage_7, stage_8, stage_9, stage_10, stage_11, stage_12)

    def tick(t, carry):
        for num, stage in enumerate(stages):
            k = t - num * LAG
            pl.when((k >= 0) & (k < chunks))(functools.partial(stage, k))
        extra(t)
        return carry

    lax.fori_loop(0, chunks + STAGES * LAG, tick, 0)


def scratch(chunks, cols):
    return [
        pltpu.VMEM((chunks, WIDE, cols), jnp.bfloat16),
        pltpu.VMEM((chunks, WIDE, cols), jnp.bfloat16),
        pltpu.VMEM((chunks, HALF, cols), jnp.bfloat16),
        pltpu.VMEM((chunks, THIN, cols), jnp.bfloat16),
        pltpu.VMEM((chunks, QUARTER, cols), jnp.bfloat16),
        pltpu.VMEM((chunks, QUARTER, cols), jnp.bfloat16),
        pltpu.VMEM((chunks, STEP, cols), jnp.bfloat16),
        pltpu.SemaphoreType.DMA((10, chunks)),
        pltpu.SemaphoreType.DMA((10, chunks)),
    ]


def layer_norm(values):
    row_mean = jnp.mean(values, axis=-1, keepdims=True)
    centered = values - row_mean
    variance = jnp.mean(centered * centered, axis=-1, keepdims=True)
    return centered * lax.rsqrt(variance + LN_EPS)


def layer_norm_parts(values):
    row_mean = jnp.mean(values, axis=-1, keepdims=True)
    centered = values - row_mean
    variance = jnp.mean(centered * centered, axis=-1, keepdims=True)
    inverse = lax.rsqrt(variance + LN_EPS)
    return centered * inverse, inverse


def layer_norm_back(grad, normed, inverse):
    grad_mean = jnp.mean(grad, axis=-1, keepdims=True)
    proj = jnp.mean(grad * normed, axis=-1, keepdims=True)
    return inverse * (grad - grad_mean - normed * proj)


def gelu(vals):
    inner = GELU_C * (vals + GELU_A * (vals * vals * vals))
    return vals * (0.5 * (1.0 + jnp.tanh(inner)))


def gelu_and_slope(vals):
    square = vals * vals
    tanh_in = jnp.tanh(GELU_C * (vals + GELU_A * (square * vals)))
    cdf = 0.5 * (1.0 + tanh_in)
    slope = cdf + 0.5 * vals * (1.0 - tanh_in * tanh_in) * (GELU_C * (1.0 + (3.0 * GELU_A) * square))
    return vals * cdf, slope


def dot_plain(lhs, rhs):
    return jnp.dot(lhs, rhs, preferred_element_type=jnp.float32)


def dot_rows(lhs, rhs):
    return lax.dot_general(lhs, rhs, (((0,), (0,)), ((), ())), preferred_element_type=jnp.float32)


def dot_cols(lhs, rhs):
    return lax.dot_general(lhs, rhs, (((1,), (1,)), ((), ())), preferred_element_type=jnp.float32)


def two_copies(k, ups, downs, other, sem, to_chunk):
    layer = 2 - k // OCT
    part = pl.ds(pl.multiple_of((k % 4) * WIDE, WIDE), WIDE)
    for array, cond, spot in ((downs, (k % OCT) < 4, (layer, part)), (ups, (k % OCT) >= 4, (layer, slice(None), part))):
        @pl.when(cond)
        def _(array=array, spot=spot):
            pair = (array.at[spot], other)
            pltpu.make_async_copy(*(pair if to_chunk else pair[::-1]), sem).start()


def small_pieces(k, arrays):
    up_one, down_one, merge, head = arrays[0], arrays[1], arrays[2], arrays[5]
    if k == UP_ONE:
        return [(up_one.at[layer], (pl.ds(layer * THIN, THIN),)) for layer in range(4)]
    if k == DOWN_ONE:
        return [(down_one.at[layer], (pl.ds(0, WIDE), pl.ds(layer * THIN, THIN))) for layer in range(4)]
    if k == MERGE:
        return [(merge, (pl.ds(0, WIDE),))]
    if k == HEAD_A:
        return [(head.at[pl.ds(0, WIDE)], (pl.ds(0, WIDE),))]
    return [(head.at[pl.ds(WIDE, HEAD_REST)], (pl.ds(0, HEAD_REST),))]


def small_copies(k, arrays, other, sem, to_chunk):
    for piece, inside in small_pieces(k, arrays):
        pair = (piece, other.at[inside])
        pltpu.make_async_copy(*(pair if to_chunk else pair[::-1]), sem).start()


def wait_bytes(ref, sem):
    pltpu.make_async_copy(ref, ref, sem).wait()


def small_ref(k, ref):
    return ref.at[pl.ds(0, HEAD_REST)] if k == HEAD_B else ref


SMALL_ORDER = (UP_ONE, DOWN_ONE, MERGE, HEAD_A, HEAD_B)


def two_item(num):
    return (2 - num // OCT) * OCT + (num + 4) % OCT


def one_forward(num, resid_in, resid_out, cast):
    layer = num // 4
    rows = pl.ds(pl.multiple_of((num % 4) * PAD_ROWS, STEP), PAD_ROWS)
    lanes = pl.ds(pl.multiple_of(layer * THIN, THIN), THIN)
    resid = resid_in[rows, :].astype(jnp.float32)
    normed = layer_norm(resid).astype(jnp.bfloat16)
    act = gelu(dot_plain(normed, cast[UP_ONE, lanes, :])).astype(jnp.bfloat16)
    out = dot_plain(act, cast[DOWN_ONE, :, lanes])
    resid_out[rows, :] = (resid + out).astype(jnp.bfloat16)


def merge_forward(resid_one, cast, resid_two):
    value = jnp.zeros((PAD_ROWS, WIDE), jnp.float32)
    for part in range(4):
        value = value + dot_plain(resid_one[part * PAD_ROWS:(part + 1) * PAD_ROWS, :], cast[MERGE, part * THIN:(part + 1) * THIN, :])
    resid_two[...] = value.astype(jnp.bfloat16)


def pool_images(resid_two):
    pooled = [jnp.sum(resid_two[img * PAD_IMG:(img + 1) * PAD_IMG, :].astype(jnp.float32), axis=0, keepdims=True) / float(TOKENS_TWO) for img in range(2)]
    return jnp.concatenate(pooled + [jnp.zeros((14, WIDE), jnp.float32)], axis=0)


def grad_kernel(*refs):
    w_in, images, labels = refs[0:6], refs[6], refs[7]
    grads, resid_saved, grad_one, cast_one = refs[OCT:12]
    load_sem, store_sem, ring_w, out_ring, cast, resid_two, normed_two, act_two, slope_two, grad_two, total = refs[12:]

    def start_small(num):
        small_copies(SMALL_ORDER[num], w_in, ring_w.at[num], load_sem.at[SMALL_ORDER[num]], True)

    def start_two(num):
        k = two_item(num)
        two_copies(k, w_in[3], w_in[4], ring_w.at[(num + 5) % RING], load_sem.at[k], True)

    def cast_slot(k, slot):
        def step(num, carry):
            rows = pl.ds(pl.multiple_of(num * QUARTER, QUARTER), QUARTER)
            cast[k, rows, :] = ring_w[slot, rows, :].astype(jnp.bfloat16)
            return carry
        lax.fori_loop(0, OCT, step, 0)

    def cast_small(num):
        k = SMALL_ORDER[num]
        wait_bytes(small_ref(k, ring_w.at[num]), load_sem.at[k])
        cast_slot(k, num)
        if k == HEAD_B:
            cast[k, HEAD_REST:WIDE, :] = jnp.zeros((WIDE - HEAD_REST, WIDE), jnp.bfloat16)

    def cast_two(num):
        k = two_item(num)
        slot = (num + 5) % RING
        wait_bytes(ring_w.at[slot], load_sem.at[k])
        cast_slot(k, slot)
        @pl.when(num + RING < TWO_CHUNKS)
        def _():
            start_two(num + RING)

    for num in range(5):
        start_small(num)
    for num in range(3):
        start_two(num)
    for num in range(5):
        cast_small(num)
        start_two(num + 3)
    cast_one[0] = cast[DOWN_ONE]
    cast_one[1] = cast[UP_ONE]
    resid_saved[0] = images[...]

    def first(num, carry):
        layer = num // 4
        one_forward(num, resid_saved.at[layer], resid_saved.at[layer + 1], cast)
        cast_two(num)
        return carry

    lax.fori_loop(0, PAIR, first, 0)
    merge_forward(resid_saved.at[4], cast, resid_two.at[0])

    def second(num, carry):
        layer, part = num // 4, num % 4
        lanes = pl.ds(pl.multiple_of(part * WIDE, WIDE), WIDE)
        @pl.when(part == 0)
        def _():
            normed_two[layer] = layer_norm(resid_two[layer].astype(jnp.float32)).astype(jnp.bfloat16)
            total[...] = jnp.zeros_like(total)
        @pl.when(num < OCT)
        def _():
            cast_two(num + PAIR)
        pre = dot_plain(normed_two[layer], cast[(2 - layer) * OCT + 4 + part])
        act, slope = gelu_and_slope(pre)
        act = act.astype(jnp.bfloat16)
        act_two[layer, :, lanes] = act
        slope_two[layer, :, lanes] = slope
        total[...] += dot_plain(act, cast[(2 - layer) * OCT + part])
        @pl.when(part == 3)
        def _():
            resid_two[layer + 1] = (resid_two[layer].astype(jnp.float32) + total[...]).astype(jnp.bfloat16)
        return carry

    lax.fori_loop(0, 12, second, 0)

    pooled = pool_images(resid_two.at[3])
    head_norm, head_inv = layer_norm_parts(pooled)
    head_in = head_norm.astype(jnp.bfloat16)
    logits = jnp.concatenate([dot_cols(head_in, cast[HEAD_A]), dot_cols(head_in, cast[HEAD_B])], axis=1)
    ids = lax.broadcasted_iota(jnp.int32, (PAIR, 1024), 1)
    row = lax.broadcasted_iota(jnp.int32, (PAIR, 1024), 0)
    logits = jnp.where(ids < CLASSES, logits, -jnp.inf)
    expo = jnp.exp(logits - jnp.max(logits, axis=1, keepdims=True))
    probs = expo / jnp.sum(expo, axis=1, keepdims=True)
    target = jnp.where(row == 0, labels[0], labels[1])
    onehot = (ids == target).astype(jnp.float32)
    grad_logits = jnp.where(row < 2, (probs - onehot) / 64.0, 0.0).astype(jnp.bfloat16)

    def out_chunk(k, slot, fresh, value):
        @pl.when(jnp.logical_not(fresh))
        def _():
            wait_bytes(out_ring.at[slot], store_sem.at[slot])
        out_ring[slot] = value.astype(jnp.bfloat16)
        pltpu.make_async_copy(out_ring.at[slot], grads.at[k], store_sem.at[slot]).start()

    true = jnp.bool_(True)
    out_chunk(HEAD_A, 0, true, dot_rows(grad_logits[:, 0:WIDE], head_in))
    out_chunk(HEAD_B, 1, true, dot_rows(grad_logits[:, WIDE:1024], head_in))
    grad_head = dot_plain(grad_logits[:, 0:WIDE], cast[HEAD_A]) + dot_plain(grad_logits[:, WIDE:1024], cast[HEAD_B])
    grad_pooled = (layer_norm_back(grad_head, head_norm, head_inv) / float(TOKENS_TWO)).astype(jnp.bfloat16).astype(jnp.float32)
    spot = lax.broadcasted_iota(jnp.int32, (PAD_IMG, WIDE), 0)
    for img in range(2):
        spread = jnp.where(spot < TOKENS_TWO, jnp.broadcast_to(grad_pooled[img:img + 1], (PAD_IMG, WIDE)), 0.0)
        grad_two[img * PAD_IMG:(img + 1) * PAD_IMG, :] = spread.astype(jnp.bfloat16)

    def third(num, carry):
        layer, part = 2 - num // 4, num % 4
        lanes = pl.ds(pl.multiple_of(part * WIDE, WIDE), WIDE)
        base = (num // 4) * OCT + part
        slot = (num * 2 + 2) % RING
        fresh = num < 3
        @pl.when(part == 0)
        def _():
            total[...] = jnp.zeros_like(total)
        out_chunk(base, slot, fresh, dot_rows(act_two[layer, :, lanes], grad_two[...]))
        grad_act = dot_cols(grad_two[...], cast[base])
        grad_pre = (grad_act * slope_two[layer, :, lanes]).astype(jnp.bfloat16)
        out_chunk(base + 4, slot + 1, fresh, dot_rows(normed_two[layer], grad_pre))
        total[...] += dot_cols(grad_pre, cast[base + 4])
        @pl.when(part == 3)
        def _():
            normed, inverse = layer_norm_parts(resid_two[layer].astype(jnp.float32))
            grad_in = layer_norm_back(total[...], normed, inverse) + grad_two[...].astype(jnp.float32)
            grad_two[...] = grad_in.astype(jnp.bfloat16)
        return carry

    lax.fori_loop(0, 12, third, 0)
    wait_bytes(out_ring.at[2], store_sem.at[2])
    for part in range(4):
        rows = slice(part * PAD_ROWS, (part + 1) * PAD_ROWS)
        spots = slice(part * THIN, (part + 1) * THIN)
        out_ring[2, spots, :] = dot_rows(resid_saved[4, rows, :], grad_two[...]).astype(jnp.bfloat16)
        grad_one[rows, :] = dot_cols(grad_two[...], cast[MERGE, spots, :]).astype(jnp.bfloat16)
    pltpu.make_async_copy(out_ring.at[2], grads.at[MERGE], store_sem.at[2]).start()
    for slot in range(RING):
        wait_bytes(out_ring.at[slot], store_sem.at[slot])


def forward_and_grads(params, images, labels):
    any_hbm = pl.BlockSpec(memory_space=pltpu.HBM)
    in_vmem = pl.BlockSpec(memory_space=pltpu.VMEM)
    return pl.pallas_call(
        grad_kernel,
        out_shape=[
            jax.ShapeDtypeStruct((27, WIDE, WIDE), jnp.bfloat16),
            jax.ShapeDtypeStruct((5, 4 * PAD_ROWS, THIN), jnp.bfloat16),
            jax.ShapeDtypeStruct((4 * PAD_ROWS, THIN), jnp.bfloat16),
            jax.ShapeDtypeStruct((2, WIDE, WIDE), jnp.bfloat16),
        ],
        in_specs=[any_hbm] * 6 + [in_vmem, pl.BlockSpec(memory_space=pltpu.SMEM)],
        out_specs=[any_hbm] + [in_vmem] * 3,
        scratch_shapes=[
            pltpu.SemaphoreType.DMA((CHUNKS,)),
            pltpu.SemaphoreType.DMA((RING,)),
            pltpu.VMEM((RING, WIDE, WIDE), jnp.float32),
            pltpu.VMEM((RING, WIDE, WIDE), jnp.bfloat16),
            pltpu.VMEM((CHUNKS, WIDE, WIDE), jnp.bfloat16),
            pltpu.VMEM((4, PAD_ROWS, WIDE), jnp.bfloat16),
            pltpu.VMEM((3, PAD_ROWS, WIDE), jnp.bfloat16),
            pltpu.VMEM((3, PAD_ROWS, 2048), jnp.bfloat16),
            pltpu.VMEM((3, PAD_ROWS, 2048), jnp.float32),
            pltpu.VMEM((PAD_ROWS, WIDE), jnp.bfloat16),
            pltpu.VMEM((PAD_ROWS, WIDE), jnp.float32),
        ],
        compiler_params=pltpu.CompilerParams(vmem_limit_bytes=62 * 2**20),
        cost_estimate=pl.CostEstimate(flops=3 * 10**10, bytes_accessed=5 * 10**7, transcendentals=0),
    )(*params, images, labels)


def block_squares(read, sums, chunk):
    def step(num, carry):
        total = jnp.zeros((OCT, LANES), jnp.float32)
        for part in range(4):
            vals = read(pl.ds(pl.multiple_of(num * THIN + part * STEP, STEP), STEP)).astype(jnp.float32)
            vals = vals * vals
            total = total + (vals[0:OCT] + vals[OCT:PAIR]) + (vals[PAIR:TWO_CHUNKS] + vals[TWO_CHUNKS:STEP])
        sums[chunk, pl.ds(num, 1), :] = jnp.sum(total, axis=0, keepdims=True)
        return carry
    lax.fori_loop(0, 4, step, 0)


TILE = 208
TILES = OCT


def reduce_kernel(*refs):
    grads, w_in = refs[0], refs[1:7]
    resid_saved, grad_in, cast_one = refs[7:10]
    out, w_sums, g_sums = refs[10:13]
    load_sem, out_sem, w_sem, w_buf, grad_one, up_total, down_total = refs[13:20]
    bufs = refs[20:]
    grad_buf, full_buf = bufs[0:2]

    def load(k, carry):
        pltpu.make_async_copy(grads.at[k], grad_buf.at[k], load_sem.at[k]).start()
        return carry

    lax.fori_loop(0, 27, load, 0)

    def w_start(k):
        two_copies(k, w_in[3], w_in[4], w_buf.at[k % W_RING], w_sem.at[k], True)

    def w_sum(k):
        slot = k % W_RING
        block_squares(lambda rows: w_buf[slot, rows, :], w_sums, k)

    for k in range(W_RING):
        w_start(jnp.int32(k))
    grad_one[...] = grad_in[...]

    def one_backward(num, carry):
        layer, tile = 3 - num // TILES, num % TILES
        rows = pl.ds(pl.multiple_of(tile * TILE, PAIR), TILE)
        lanes = pl.ds(pl.multiple_of(layer * THIN, THIN), THIN)
        normed, inverse = layer_norm_parts(resid_saved[layer, rows, :].astype(jnp.float32))
        normed_b = normed.astype(jnp.bfloat16)
        up = cast_one[1, lanes, :]
        act, slope = gelu_and_slope(dot_plain(normed_b, up))
        grad = grad_one[rows, :]
        keep = jnp.where(tile == 0, 0.0, 1.0)
        down_total[...] = down_total[...] * keep + dot_rows(act.astype(jnp.bfloat16), grad)
        grad_pre = (dot_cols(grad, cast_one[0, :, lanes]) * slope).astype(jnp.bfloat16)
        up_total[...] = up_total[...] * keep + dot_rows(normed_b, grad_pre)
        back = layer_norm_back(dot_cols(grad_pre, up), normed, inverse) + grad.astype(jnp.float32)
        grad_one[rows, :] = back.astype(jnp.bfloat16)
        @pl.when(tile == TILES - 1)
        def _():
            grad_buf[DOWN_ONE, :, lanes] = down_total[...].astype(jnp.bfloat16)
            grad_buf[UP_ONE, lanes, :] = up_total[...].astype(jnp.bfloat16)
        return carry

    down_total[...] = jnp.zeros_like(down_total)
    up_total[...] = jnp.zeros_like(up_total)

    def each_tick(t):
        @pl.when(t < PAIR)
        def _():
            lax.fori_loop(t * 2, t * 2 + 2, one_backward, 0)

        @pl.when(t < TWO_CHUNKS)
        def _():
            wait_bytes(w_buf.at[t % W_RING], w_sem.at[t])
            w_sum(t)

        @pl.when(t + W_RING < TWO_CHUNKS)
        def _():
            w_start(t + W_RING)

        for k in range(TWO_CHUNKS, CHUNKS):
            @pl.when(t == k - W_RING)
            def _(k=k):
                small_copies(k, w_in, w_buf.at[k % W_RING], w_sem.at[k], True)

            @pl.when(t == k)
            def _(k=k):
                wait_bytes(small_ref(k, w_buf.at[k % W_RING]), w_sem.at[k])
                if k == HEAD_B:
                    w_buf[k % W_RING, HEAD_REST:WIDE, :] = jnp.zeros((WIDE - HEAD_REST, WIDE), jnp.float32)
                w_sum(k)

    def before(k):
        @pl.when(k < 27)
        def _():
            wait_bytes(grad_buf.at[k], load_sem.at[k])

    def after(k):
        pltpu.make_async_copy(full_buf.at[k], out.at[k], out_sem.at[k]).start()
        block_squares(lambda rows: full_buf[k, rows, :], g_sums, k)

    all_reduce_body(CHUNKS, *bufs, before, after, each_tick)

    def finish(k, carry):
        wait_bytes(full_buf.at[k], out_sem.at[k])
        return carry

    lax.fori_loop(0, CHUNKS, finish, 0)


def reduce_grads(grads, params, resid_saved, grad_one, cast_one):
    any_hbm = pl.BlockSpec(memory_space=pltpu.HBM)
    in_vmem = pl.BlockSpec(memory_space=pltpu.VMEM)
    sums_shape = (CHUNKS, 4, LANES)
    return pl.pallas_call(
        reduce_kernel,
        out_shape=[jax.ShapeDtypeStruct((CHUNKS, WIDE, WIDE), jnp.bfloat16)] + [jax.ShapeDtypeStruct(sums_shape, jnp.float32)] * 2,
        in_specs=[any_hbm] * 7 + [in_vmem] * 3,
        out_specs=[any_hbm] + [in_vmem] * 2,
        scratch_shapes=[pltpu.SemaphoreType.DMA((CHUNKS,))] * 3 + [
            pltpu.VMEM((W_RING, WIDE, WIDE), jnp.float32),
            pltpu.VMEM((4 * PAD_ROWS, THIN), jnp.bfloat16),
            pltpu.VMEM((THIN, WIDE), jnp.float32),
            pltpu.VMEM((WIDE, THIN), jnp.float32),
        ] + scratch(CHUNKS, WIDE),
        compiler_params=pltpu.CompilerParams(has_side_effects=True, vmem_limit_bytes=62 * 2**20),
        cost_estimate=pl.CostEstimate(flops=10**10, bytes_accessed=6 * 10**7, transcendentals=0),
    )(grads, *params, resid_saved, grad_one, cast_one)


def next_kernel(*refs):
    grads, w_in, v_in = refs[0], refs[1:7], refs[7:13]
    w_sums, g_sums, images = refs[13:PAIR]
    logits, w_out, v_out = refs[PAIR], refs[17:23], refs[23:29]
    load_sem, store_sem, ring_w, ring_v, ring_g, cast, coef, resid_one, resid_two, normed_two, total_two = refs[29:]
    rings = (ring_w, ring_v)

    def start_small(num):
        k = SMALL_ORDER[num]
        for which, arrays in enumerate((w_in, v_in)):
            small_copies(k, arrays, rings[which].at[num], load_sem.at[which, k], True)
        pltpu.make_async_copy(grads.at[k], ring_g.at[num], load_sem.at[2, k]).start()

    def start_two(num):
        k = two_item(num)
        slot = (num + 5) % RING
        for which, arrays in enumerate((w_in, v_in)):
            two_copies(k, arrays[3], arrays[4], rings[which].at[slot], load_sem.at[which, k], True)
        pltpu.make_async_copy(grads.at[k], ring_g.at[slot], load_sem.at[2, k]).start()

    for num in range(5):
        start_small(num)

    def ratio(w_total, g_total):
        return TRUST * (jnp.sqrt(w_total) / jnp.sqrt(g_total))

    def total(sums, first, size):
        return jnp.sum(jnp.sum(jnp.sum(sums[first:first + size], axis=0), axis=0, keepdims=True), axis=1, keepdims=True)

    for first, size in [(0, 4), (4, 4), (OCT, 4), (12, 4), (PAIR, 4), (20, 4), (HEAD_A, 2), (MERGE, 1)]:
        value = ratio(total(w_sums, first, size), total(g_sums, first, size))
        for k in range(first, first + size):
            coef[k] = jnp.broadcast_to(value, (4, LANES))
    by_row = ratio(jnp.sum(w_sums[UP_ONE], axis=1, keepdims=True), jnp.sum(g_sums[UP_ONE], axis=1, keepdims=True))
    coef[UP_ONE] = jnp.broadcast_to(by_row, (4, LANES))
    for layer in range(4):
        lanes = pl.ds(layer * THIN, THIN)
        lane_total = [jnp.sum(jnp.sum(sums[DOWN_ONE, :, lanes], axis=0, keepdims=True), axis=1, keepdims=True) for sums in (w_sums, g_sums)]
        coef[DOWN_ONE, :, lanes] = jnp.broadcast_to(ratio(*lane_total), (4, THIN))

    def apply_update(k, slot):
        def step(num, carry):
            rows = pl.ds(pl.multiple_of(num * STEP, STEP), STEP)
            factor = coef[k, pl.ds(num // 4, 1), :]
            new_v = MOMENTUM * ring_v[slot, rows, :] + factor * ring_g[slot, rows, :].astype(jnp.float32)
            new_w = ring_w[slot, rows, :] - new_v
            ring_v[slot, rows, :] = new_v
            ring_w[slot, rows, :] = new_w
            cast[k, rows, :] = new_w.astype(jnp.bfloat16)
            return carry
        lax.fori_loop(0, PAIR, step, 0)

    def update_small(num):
        k = SMALL_ORDER[num]
        for which in range(2):
            wait_bytes(small_ref(k, rings[which].at[num]), load_sem.at[which, k])
        wait_bytes(ring_g.at[num], load_sem.at[2, k])
        apply_update(k, num)
        if k == HEAD_B:
            cast[k, HEAD_REST:WIDE, :] = jnp.zeros((WIDE - HEAD_REST, WIDE), jnp.bfloat16)
        for which, arrays in enumerate((w_out, v_out)):
            small_copies(k, arrays, rings[which].at[num], store_sem.at[which, k], False)

    def wait_small_store(num):
        k = SMALL_ORDER[num]
        for which in range(2):
            wait_bytes(small_ref(k, rings[which].at[num]), store_sem.at[which, k])

    def wait_two_store(num):
        k = two_item(num)
        slot = (num + 5) % RING
        for which in range(2):
            wait_bytes(rings[which].at[slot], store_sem.at[which, k])

    def update_two(num, carry):
        k = two_item(num)
        slot = (num + 5) % RING
        for which in range(2):
            wait_bytes(rings[which].at[slot], load_sem.at[which, k])
        wait_bytes(ring_g.at[slot], load_sem.at[2, k])
        apply_update(k, slot)
        for which, arrays in enumerate((w_out, v_out)):
            two_copies(k, arrays[3], arrays[4], rings[which].at[slot], store_sem.at[which, k], False)
        later = num + AHEAD
        @pl.when((later < TWO_CHUNKS) & (later >= RING))
        def _():
            wait_two_store(later - RING)
        @pl.when(later < TWO_CHUNKS)
        def _():
            start_two(later)
        return carry

    for num in range(3):
        start_two(num)
    for num in range(5):
        update_small(num)
    resid_one[...] = images[...]
    wait_small_store(0)
    start_two(3)

    def first(num, carry):
        for small in range(1, 5):
            @pl.when(num == small - 1)
            def _(small=small):
                wait_small_store(small)
        update_two(num, 0)

        def body(part, carry):
            one_forward(part, resid_one, resid_one, cast)
            return carry

        return lax.fori_loop(num * 2, num * 2 + 2, body, carry)

    lax.fori_loop(0, OCT, first, 0)
    merge_forward(resid_one, cast, resid_two)

    def second(num, carry):
        layer, part = num // 4, num % 4
        @pl.when(part == 0)
        def _():
            normed_two[...] = layer_norm(resid_two[...].astype(jnp.float32)).astype(jnp.bfloat16)
            total_two[...] = jnp.zeros_like(total_two)
        @pl.when(layer < 2)
        def _():
            lax.fori_loop(OCT + num * 2, 10 + num * 2, update_two, 0)
        act = gelu(dot_plain(normed_two[...], cast[(2 - layer) * OCT + 4 + part])).astype(jnp.bfloat16)
        total_two[...] += dot_plain(act, cast[(2 - layer) * OCT + part])
        @pl.when(part == 3)
        def _():
            resid_two[...] = (resid_two[...].astype(jnp.float32) + total_two[...]).astype(jnp.bfloat16)
        return carry

    lax.fori_loop(0, 12, second, 0)
    head_in = layer_norm(pool_images(resid_two)).astype(jnp.bfloat16)
    logits[:, 0:WIDE] = dot_cols(head_in, cast[HEAD_A])[0:2]
    logits[:, WIDE:1000] = dot_cols(head_in, cast[HEAD_B])[0:2, 0:HEAD_REST]
    for num in range(PAIR, TWO_CHUNKS):
        wait_two_store(num)


def arrange(images):
    count, tokens, width = images.shape
    split = images.reshape(count, tokens // 4, 4, width).transpose(2, 0, 1, 3)
    split = jnp.pad(split, ((0, 0), (0, 0), (0, PAD_IMG - tokens // 4), (0, 0)))
    return split.reshape(4 * count * PAD_IMG, width)


def update_and_forward(params, velocities, grads, w_sums, g_sums, images):
    any_hbm = pl.BlockSpec(memory_space=pltpu.HBM)
    in_vmem = pl.BlockSpec(memory_space=pltpu.VMEM)
    shapes = [jax.ShapeDtypeStruct(array.shape, array.dtype) for array in params]
    outs = pl.pallas_call(
        next_kernel,
        out_shape=[jax.ShapeDtypeStruct((2, CLASSES), jnp.float32)] + shapes + shapes,
        in_specs=[any_hbm] * 13 + [in_vmem] * 3,
        out_specs=[in_vmem] + [any_hbm] * 12,
        scratch_shapes=[
            pltpu.SemaphoreType.DMA((3, CHUNKS)),
            pltpu.SemaphoreType.DMA((2, CHUNKS)),
            pltpu.VMEM((RING, WIDE, WIDE), jnp.float32),
            pltpu.VMEM((RING, WIDE, WIDE), jnp.float32),
            pltpu.VMEM((RING, WIDE, WIDE), jnp.bfloat16),
            pltpu.VMEM((CHUNKS, WIDE, WIDE), jnp.bfloat16),
            pltpu.VMEM((CHUNKS, 4, LANES), jnp.float32),
            pltpu.VMEM((4 * PAD_ROWS, THIN), jnp.bfloat16),
            pltpu.VMEM((PAD_ROWS, WIDE), jnp.bfloat16),
            pltpu.VMEM((PAD_ROWS, WIDE), jnp.bfloat16),
            pltpu.VMEM((PAD_ROWS, WIDE), jnp.float32),
        ],
        compiler_params=pltpu.CompilerParams(vmem_limit_bytes=58 * 2**20),
        cost_estimate=pl.CostEstimate(flops=10**10, bytes_accessed=135 * 10**6, transcendentals=0),
    )(grads, *params, *velocities, w_sums, g_sums, images)
    return outs


def solution(mesh):
    def local_step(x_now, labels_now, x_next, *weights):
        params = weights[0:5] + (weights[5].T,)
        velocities = weights[6:11] + (weights[11].T,)
        grads, resid_saved, grad_one, cast_one = forward_and_grads(params, arrange(x_now), labels_now)
        sums, w_sums, g_sums = reduce_grads(grads, params, resid_saved, grad_one, cast_one)
        outs = update_and_forward(params, velocities, sums, w_sums, g_sums, arrange(x_next))
        new_w, new_v = outs[1:7], outs[7:13]
        return (outs[0],) + tuple(new_w[0:5]) + (new_w[5].T,) + tuple(new_v[0:5]) + (new_v[5].T,)

    replicated = P()
    batch_split = P('data')
    in_specs = (batch_split, batch_split, batch_split) + (replicated,) * 12
    out_specs = (batch_split,) + (replicated,) * 12
    return jax.shard_map(local_step, mesh=mesh, in_specs=in_specs, out_specs=out_specs, check_vma=False)
```

```python
import functools

import jax
import jax.numpy as jnp
from jax import lax
from jax.experimental import pallas as pl
from jax.experimental.pallas import tpu as pltpu
from jax.sharding import PartitionSpec as P

MOMENTUM = 0.9
TRUST = 0.1
LN_EPS = 1e-6
CHUNKS = 29
HEAD_A, HEAD_B, MERGE, DOWN_ONE, UP_ONE = 24, 25, 26, 27, 28
HEAD_REST = 488
CLASSES = 1000
LANES = 512
RING = 8
AHEAD = 4
W_RING = 3
TOKENS_TWO = 196
TOKENS = 784
PAD_IMG = 208
PAD_ROWS = 416
GELU_C = 0.7978845608028654
GELU_A = 0.044715
WIDE = 512
THIN = 128
STEP = 32
QUARTER = 64
HALF = 256
TWO_CHUNKS = 24
OCT = 8
PAIR = 16
DOZEN = 12

MESH = pl.DeviceIdType.MESH
ROWS = WIDE
LAG = 3
STAGES = DOZEN


def all_reduce_body(chunks, grad_buf, full_buf, recv_core, recv_one, recv_z, recv_mid, recv_two, send_sem, recv_sem, before, after, extra):
    me = lax.axis_index('data')
    core = me % 2
    x_pos = (me // 2) % 2
    y_pos = (me // 4) % 2
    z_pos = me // OCT
    one = x_pos * (1 - core) + y_pos * core
    two = y_pos * (1 - core) + x_pos * core
    one_step = 2 * (1 - core) + 4 * core
    two_step = 4 * (1 - core) + 2 * core
    dev_core = me + 1 - 2 * core
    dev_one = me + one_step * (1 - 2 * one)
    dev_two = me + two_step * (1 - 2 * two)
    upper = z_pos // 2
    is_end = (z_pos % 3) == 0
    is_mid = (z_pos % 3) != 0
    dev_inner = me + OCT * (1 - 2 * upper)
    dev_outer = me - OCT * (1 - 2 * upper)
    half = core * HALF
    quarter = half + one * THIN
    near = quarter + upper * QUARTER
    far = quarter + (1 - upper) * QUARTER
    mine = near + two * STEP

    def rows(chunk, start, size):
        return grad_buf.at[chunk, pl.ds(pl.multiple_of(start, STEP), size)]

    def full(chunk, start, size):
        return full_buf.at[chunk, pl.ds(pl.multiple_of(start, STEP), size)]

    def remote(src, dst, which, chunk, dev):
        return pltpu.make_async_remote_copy(src_ref=src, dst_ref=dst, send_sem=send_sem.at[which, chunk], recv_sem=recv_sem.at[which, chunk], device_id=(dev,), device_id_type=MESH)

    def add_in(chunk, start, size, recv):
        def step(num, carry):
            spot = pl.ds(pl.multiple_of(start + num * STEP, STEP), STEP)
            grad_buf[chunk, spot, :] = grad_buf[chunk, spot, :] + recv[chunk, pl.ds(pl.multiple_of(num * STEP, STEP), STEP), :]
            return carry
        lax.fori_loop(0, size // STEP, step, 0)

    def c_core(k):
        return remote(rows(k, HALF - half, HALF), recv_core.at[k], 0, k, dev_core)

    def c_one(k):
        return remote(rows(k, half + (1 - one) * THIN, THIN), recv_one.at[k], 1, k, dev_one)

    def c_in(k):
        return remote(rows(k, far, QUARTER), recv_z.at[k], 2, k, dev_inner)

    def c_mid(k):
        return remote(rows(k, far, QUARTER), recv_mid.at[k], 3, k, dev_inner)

    def c_out(k):
        return remote(rows(k, near, QUARTER), recv_z.at[k], 2, k, dev_outer)

    def c_two(k):
        return remote(rows(k, near + (1 - two) * STEP, STEP), recv_two.at[k], 4, k, dev_two)

    def g_two(k):
        return remote(full(k, mine, STEP), full(k, mine, STEP), 5, k, dev_two)

    def g_in(k):
        return remote(full(k, near, QUARTER), full(k, near, QUARTER), 6, k, dev_inner)

    def g_mid(k):
        return remote(full(k, near, QUARTER), full(k, near, QUARTER), 7, k, dev_inner)

    def g_out(k):
        return remote(full(k, far, QUARTER), full(k, far, QUARTER), 6, k, dev_outer)

    def g_one(k):
        return remote(full(k, quarter, THIN), full(k, quarter, THIN), OCT, k, dev_one)

    def g_core(k):
        return remote(full(k, half, HALF), full(k, half, HALF), 9, k, dev_core)

    def stage_0(k):
        before(k)
        c_core(k).start()

    def stage_1(k):
        c_core(k).wait()
        add_in(k, half, HALF, recv_core)
        c_one(k).start()

    def stage_2(k):
        c_one(k).wait()
        add_in(k, quarter, THIN, recv_one)
        @pl.when(is_end)
        def _():
            c_in(k).start()

    def stage_3(k):
        @pl.when(is_end)
        def _():
            c_in(k).wait_send()
        @pl.when(is_mid)
        def _():
            c_out(k).wait_recv()
            add_in(k, far, QUARTER, recv_z)
            c_mid(k).start()

    def stage_4(k):
        @pl.when(is_mid)
        def _():
            c_mid(k).wait()
            add_in(k, near, QUARTER, recv_mid)
            c_out(k).start()

    def stage_5(k):
        @pl.when(is_mid)
        def _():
            c_out(k).wait_send()
        @pl.when(is_end)
        def _():
            c_in(k).wait_recv()
            add_in(k, near, QUARTER, recv_z)
            c_two(k).start()

    def stage_6(k):
        @pl.when(is_end)
        def _():
            c_two(k).wait()
            spot = pl.ds(pl.multiple_of(mine, STEP), STEP)
            full_buf[k, spot, :] = grad_buf[k, spot, :] + recv_two[k]
            g_two(k).start()

    def stage_7(k):
        @pl.when(is_end)
        def _():
            g_two(k).wait()
            g_in(k).start()

    def stage_8(k):
        @pl.when(is_end)
        def _():
            g_in(k).wait_send()
        @pl.when(is_mid)
        def _():
            g_out(k).wait_recv()
            g_mid(k).start()

    def stage_9(k):
        @pl.when(is_mid)
        def _():
            g_mid(k).wait()
            g_out(k).start()

    def stage_10(k):
        @pl.when(is_mid)
        def _():
            g_out(k).wait_send()
        @pl.when(is_end)
        def _():
            g_in(k).wait_recv()
        g_one(k).start()

    def stage_11(k):
        g_one(k).wait()
        g_core(k).start()

    def stage_12(k):
        g_core(k).wait()
        after(k)

    stages = (stage_0, stage_1, stage_2, stage_3, stage_4, stage_5, stage_6, stage_7, stage_8, stage_9, stage_10, stage_11, stage_12)

    def tick(t, carry):
        for num, stage in reversed(list(enumerate(stages))):
            if num == 0:
                extra(t)
            k = t - num * LAG
            pl.when((k >= 0) & (k < chunks))(functools.partial(stage, k))
        return carry

    lax.fori_loop(0, chunks + STAGES * LAG, tick, 0)


def scratch(chunks, cols):
    return [
        pltpu.VMEM((chunks, WIDE, cols), jnp.bfloat16),
        pltpu.VMEM((chunks, WIDE, cols), jnp.bfloat16),
        pltpu.VMEM((chunks, HALF, cols), jnp.bfloat16),
        pltpu.VMEM((chunks, THIN, cols), jnp.bfloat16),
        pltpu.VMEM((chunks, QUARTER, cols), jnp.bfloat16),
        pltpu.VMEM((chunks, QUARTER, cols), jnp.bfloat16),
        pltpu.VMEM((chunks, STEP, cols), jnp.bfloat16),
        pltpu.SemaphoreType.DMA((10, chunks)),
        pltpu.SemaphoreType.DMA((10, chunks)),
    ]


def layer_norm(values):
    row_mean = jnp.mean(values, axis=-1, keepdims=True)
    centered = values - row_mean
    variance = jnp.mean(centered * centered, axis=-1, keepdims=True)
    return centered * lax.rsqrt(variance + LN_EPS)


def layer_norm_parts(values):
    row_mean = jnp.mean(values, axis=-1, keepdims=True)
    centered = values - row_mean
    variance = jnp.mean(centered * centered, axis=-1, keepdims=True)
    inverse = lax.rsqrt(variance + LN_EPS)
    return centered * inverse, inverse


def layer_norm_back(grad, normed, inverse):
    grad_mean = jnp.mean(grad, axis=-1, keepdims=True)
    proj = jnp.mean(grad * normed, axis=-1, keepdims=True)
    return inverse * (grad - grad_mean - normed * proj)


def gelu(vals):
    inner = GELU_C * (vals + GELU_A * (vals * vals * vals))
    return vals * (0.5 * (1.0 + jnp.tanh(inner)))


def gelu_and_slope(vals):
    square = vals * vals
    tanh_in = jnp.tanh(GELU_C * (vals + GELU_A * (square * vals)))
    cdf = 0.5 * (1.0 + tanh_in)
    slope = cdf + 0.5 * vals * (1.0 - tanh_in * tanh_in) * (GELU_C * (1.0 + (3.0 * GELU_A) * square))
    return vals * cdf, slope


def dot_plain(lhs, rhs):
    return jnp.dot(lhs, rhs, preferred_element_type=jnp.float32)


def dot_rows(lhs, rhs):
    return lax.dot_general(lhs, rhs, (((0,), (0,)), ((), ())), preferred_element_type=jnp.float32)


def dot_cols(lhs, rhs):
    return lax.dot_general(lhs, rhs, (((1,), (1,)), ((), ())), preferred_element_type=jnp.float32)


def two_copies(k, ups, downs, other, sem, to_chunk):
    layer = 2 - k // OCT
    part = pl.ds(pl.multiple_of((k % 4) * WIDE, WIDE), WIDE)
    for array, cond, spot in ((downs, (k % OCT) < 4, (layer, part)), (ups, (k % OCT) >= 4, (layer, slice(None), part))):
        @pl.when(cond)
        def _(array=array, spot=spot):
            pair = (array.at[spot], other)
            pltpu.make_async_copy(*(pair if to_chunk else pair[::-1]), sem).start()


def small_pieces(k, arrays):
    up_one, down_one, merge, head = arrays[0], arrays[1], arrays[2], arrays[5]
    if k == UP_ONE:
        return [(up_one.at[layer], (pl.ds(layer * THIN, THIN),)) for layer in range(4)]
    if k == DOWN_ONE:
        return [(down_one.at[layer], (pl.ds(0, WIDE), pl.ds(layer * THIN, THIN))) for layer in range(4)]
    if k == MERGE:
        return [(merge, (pl.ds(0, WIDE),))]
    if k == HEAD_A:
        return [(head.at[pl.ds(0, WIDE)], (pl.ds(0, WIDE),))]
    return [(head.at[pl.ds(WIDE, HEAD_REST)], (pl.ds(0, HEAD_REST),))]


def small_copies(k, arrays, other, sem, to_chunk):
    for piece, inside in small_pieces(k, arrays):
        pair = (piece, other.at[inside])
        pltpu.make_async_copy(*(pair if to_chunk else pair[::-1]), sem).start()


def wait_bytes(ref, sem):
    pltpu.make_async_copy(ref, ref, sem).wait()


def small_ref(k, ref):
    return ref.at[pl.ds(0, HEAD_REST)] if k == HEAD_B else ref


SMALL_ORDER = (UP_ONE, DOWN_ONE, MERGE, HEAD_A, HEAD_B)


def two_item(num):
    return (2 - num // OCT) * OCT + (num + 4) % OCT


def one_forward(num, resid_in, resid_out, cast):
    layer = num // 4
    rows = pl.ds(pl.multiple_of((num % 4) * PAD_ROWS, STEP), PAD_ROWS)
    lanes = pl.ds(pl.multiple_of(layer * THIN, THIN), THIN)
    resid = resid_in[rows, :].astype(jnp.float32)
    normed = layer_norm(resid).astype(jnp.bfloat16)
    act = gelu(dot_plain(normed, cast[UP_ONE, lanes, :])).astype(jnp.bfloat16)
    out = dot_plain(act, cast[DOWN_ONE, :, lanes])
    resid_out[rows, :] = (resid + out).astype(jnp.bfloat16)


def merge_forward(resid_one, cast, resid_two):
    value = jnp.zeros((PAD_ROWS, WIDE), jnp.float32)
    for part in range(4):
        value = value + dot_plain(resid_one[part * PAD_ROWS:(part + 1) * PAD_ROWS, :], cast[MERGE, part * THIN:(part + 1) * THIN, :])
    resid_two[...] = value.astype(jnp.bfloat16)


def pool_images(resid_two):
    pooled = [jnp.sum(resid_two[img * PAD_IMG:(img + 1) * PAD_IMG, :].astype(jnp.float32), axis=0, keepdims=True) / float(TOKENS_TWO) for img in range(2)]
    return jnp.concatenate(pooled + [jnp.zeros((14, WIDE), jnp.float32)], axis=0)


def arrange(images, wide, resid):
    for img in range(2):
        wide[img * TOKENS:(img + 1) * TOKENS, :] = images[img].astype(jnp.float32)
    resid[...] = jnp.zeros_like(resid)
    for part in range(4):
        for img in range(2):
            first = part * PAD_ROWS + img * PAD_IMG
            rows = wide[pl.ds(img * TOKENS + part, TOKENS_TWO, stride=4), :]
            resid[first:first + TOKENS_TWO, :] = rows.astype(jnp.bfloat16)


def grad_kernel(*refs):
    w_in, images, labels = refs[0:6], refs[6], refs[7]
    head_grads, cast_out, act_out, slope_out, resid_saved, resid_two, grad_two, cast_one = refs[OCT:PAIR]
    load_sem, cast_sem, act_sem, slope_sem, ring_w, cast, last_two, normed_two, act_two, slope_two, total, wide = refs[PAIR:]

    def send_cast(k, spot):
        pltpu.make_async_copy(cast.at[k], cast_out.at[spot], cast_sem.at[spot]).start()

    def start_small(num):
        small_copies(SMALL_ORDER[num], w_in, ring_w.at[num], load_sem.at[SMALL_ORDER[num]], True)

    def start_two(num):
        k = two_item(num)
        two_copies(k, w_in[3], w_in[4], ring_w.at[(num + 5) % RING], load_sem.at[k], True)

    def cast_slot(k, slot):
        def step(num, carry):
            rows = pl.ds(pl.multiple_of(num * QUARTER, QUARTER), QUARTER)
            cast[k, rows, :] = ring_w[slot, rows, :].astype(jnp.bfloat16)
            return carry
        lax.fori_loop(0, OCT, step, 0)

    def cast_small(num):
        k = SMALL_ORDER[num]
        wait_bytes(small_ref(k, ring_w.at[num]), load_sem.at[k])
        cast_slot(k, num)
        if k == HEAD_B:
            cast[k, HEAD_REST:WIDE, :] = jnp.zeros((WIDE - HEAD_REST, WIDE), jnp.bfloat16)

    def cast_two(num):
        k = two_item(num)
        slot = (num + 5) % RING
        wait_bytes(ring_w.at[slot], load_sem.at[k])
        cast_slot(k, slot)
        send_cast(k, k)
        @pl.when(num + RING < TWO_CHUNKS)
        def _():
            start_two(num + RING)

    for num in range(5):
        start_small(num)
    for num in range(3):
        start_two(num)
    for num in range(5):
        cast_small(num)
        start_two(num + 3)
    send_cast(MERGE, TWO_CHUNKS)
    cast_one[0] = cast[DOWN_ONE]
    cast_one[1] = cast[UP_ONE]
    arrange(images, wide, resid_saved.at[0])

    def first(num, carry):
        layer = num // 4
        one_forward(num, resid_saved.at[layer], resid_saved.at[layer + 1], cast)
        cast_two(num)
        return carry

    lax.fori_loop(0, PAIR, first, 0)
    merge_forward(resid_saved.at[4], cast, resid_two.at[0])

    def second(num, carry):
        layer, part = num // 4, num % 4
        lanes = pl.ds(pl.multiple_of(part * WIDE, WIDE), WIDE)
        @pl.when(part == 0)
        def _():
            normed_two[...] = layer_norm(resid_two[layer].astype(jnp.float32)).astype(jnp.bfloat16)
            total[...] = jnp.zeros_like(total)
        @pl.when(num < OCT)
        def _():
            cast_two(num + PAIR)
        pre = dot_plain(normed_two[...], cast[(2 - layer) * OCT + 4 + part])
        act, slope = gelu_and_slope(pre)
        act = act.astype(jnp.bfloat16)
        act_two[layer, :, lanes] = act
        slope_two[layer, :, lanes] = slope
        total[...] += dot_plain(act, cast[(2 - layer) * OCT + part])
        pltpu.make_async_copy(act_two.at[layer, :, lanes], act_out.at[layer, :, lanes], act_sem.at[num]).start()
        pltpu.make_async_copy(slope_two.at[layer, :, lanes], slope_out.at[layer, :, lanes], slope_sem.at[num]).start()
        @pl.when(part == 3)
        def _():
            value = (resid_two[layer].astype(jnp.float32) + total[...]).astype(jnp.bfloat16)
            @pl.when(layer < 2)
            def _():
                resid_two[jnp.minimum(layer + 1, 2)] = value
            @pl.when(layer == 2)
            def _():
                last_two[...] = value
        return carry

    lax.fori_loop(0, DOZEN, second, 0)

    pooled = pool_images(last_two)
    head_norm, head_inv = layer_norm_parts(pooled)
    head_in = head_norm.astype(jnp.bfloat16)
    logits = jnp.concatenate([dot_cols(head_in, cast[HEAD_A]), dot_cols(head_in, cast[HEAD_B])], axis=1)
    ids = lax.broadcasted_iota(jnp.int32, (PAIR, 1024), 1)
    row = lax.broadcasted_iota(jnp.int32, (PAIR, 1024), 0)
    logits = jnp.where(ids < CLASSES, logits, -jnp.inf)
    expo = jnp.exp(logits - jnp.max(logits, axis=1, keepdims=True))
    probs = expo / jnp.sum(expo, axis=1, keepdims=True)
    target = jnp.where(row == 0, labels[0], labels[1])
    onehot = (ids == target).astype(jnp.float32)
    grad_logits = jnp.where(row < 2, (probs - onehot) / 64.0, 0.0).astype(jnp.bfloat16)

    head_grads[0] = dot_rows(grad_logits[:, 0:WIDE], head_in).astype(jnp.bfloat16)
    head_grads[1] = dot_rows(grad_logits[:, WIDE:1024], head_in).astype(jnp.bfloat16)
    grad_head = dot_plain(grad_logits[:, 0:WIDE], cast[HEAD_A]) + dot_plain(grad_logits[:, WIDE:1024], cast[HEAD_B])
    grad_pooled = (layer_norm_back(grad_head, head_norm, head_inv) / float(TOKENS_TWO)).astype(jnp.bfloat16).astype(jnp.float32)
    spot = lax.broadcasted_iota(jnp.int32, (PAD_IMG, WIDE), 0)
    for img in range(2):
        spread = jnp.where(spot < TOKENS_TWO, jnp.broadcast_to(grad_pooled[img:img + 1], (PAD_IMG, WIDE)), 0.0)
        grad_two[img * PAD_IMG:(img + 1) * PAD_IMG, :] = spread.astype(jnp.bfloat16)

    def finish(num, carry):
        lanes = pl.ds(pl.multiple_of((num % 4) * WIDE, WIDE), WIDE)
        wait_bytes(act_two.at[num // 4, :, lanes], act_sem.at[num])
        wait_bytes(slope_two.at[num // 4, :, lanes], slope_sem.at[num])
        return carry

    lax.fori_loop(0, DOZEN, finish, 0)

    def finish_cast(k, carry):
        wait_bytes(cast.at[k], cast_sem.at[k])
        return carry

    lax.fori_loop(0, 25, finish_cast, 0)


def forward_and_grads(params, images, labels):
    any_hbm = pl.BlockSpec(memory_space=pltpu.HBM)
    in_vmem = pl.BlockSpec(memory_space=pltpu.VMEM)
    return pl.pallas_call(
        grad_kernel,
        out_shape=[
            jax.ShapeDtypeStruct((2, WIDE, WIDE), jnp.bfloat16),
            jax.ShapeDtypeStruct((25, WIDE, WIDE), jnp.bfloat16),
            jax.ShapeDtypeStruct((3, PAD_ROWS, 2048), jnp.bfloat16),
            jax.ShapeDtypeStruct((3, PAD_ROWS, 2048), jnp.float32),
            jax.ShapeDtypeStruct((5, 4 * PAD_ROWS, THIN), jnp.bfloat16),
            jax.ShapeDtypeStruct((3, PAD_ROWS, WIDE), jnp.bfloat16),
            jax.ShapeDtypeStruct((PAD_ROWS, WIDE), jnp.bfloat16),
            jax.ShapeDtypeStruct((2, WIDE, WIDE), jnp.bfloat16),
        ],
        in_specs=[any_hbm] * 6 + [in_vmem, pl.BlockSpec(memory_space=pltpu.SMEM)],
        out_specs=[in_vmem] + [any_hbm] * 3 + [in_vmem] * 4,
        scratch_shapes=[
            pltpu.SemaphoreType.DMA((CHUNKS,)),
            pltpu.SemaphoreType.DMA((25,)),
            pltpu.SemaphoreType.DMA((DOZEN,)),
            pltpu.SemaphoreType.DMA((DOZEN,)),
            pltpu.VMEM((RING, WIDE, WIDE), jnp.float32),
            pltpu.VMEM((CHUNKS, WIDE, WIDE), jnp.bfloat16),
            pltpu.VMEM((PAD_ROWS, WIDE), jnp.bfloat16),
            pltpu.VMEM((PAD_ROWS, WIDE), jnp.bfloat16),
            pltpu.VMEM((3, PAD_ROWS, 2048), jnp.bfloat16),
            pltpu.VMEM((3, PAD_ROWS, 2048), jnp.float32),
            pltpu.VMEM((PAD_ROWS, WIDE), jnp.float32),
            pltpu.VMEM((2 * TOKENS, THIN), jnp.float32),
        ],
        compiler_params=pltpu.CompilerParams(vmem_limit_bytes=62 * 2**20),
        cost_estimate=pl.CostEstimate(flops=3 * 10**10, bytes_accessed=5 * 10**7, transcendentals=0),
    )(*params, images, labels)


def block_squares(read, sums, chunk):
    def step(num, carry):
        total = jnp.zeros((OCT, LANES), jnp.float32)
        for part in range(4):
            vals = read(pl.ds(pl.multiple_of(num * THIN + part * STEP, STEP), STEP)).astype(jnp.float32)
            vals = vals * vals
            total = total + (vals[0:OCT] + vals[OCT:PAIR]) + (vals[PAIR:TWO_CHUNKS] + vals[TWO_CHUNKS:STEP])
        sums[chunk, pl.ds(num, 1), :] = jnp.sum(total, axis=0, keepdims=True)
        return carry
    lax.fori_loop(0, 4, step, 0)


TILE = PAD_ROWS
TILES = 4


def reduce_kernel(*refs):
    head_grads, w_cast, act_in, slope_in, w_in = refs[0], refs[1], refs[2], refs[3], refs[4:10]
    resid_saved, resid_two, grad_in, cast_one = refs[10:14]
    out, w_sums, g_sums = refs[14:17]
    load_sem, cast_sem, act_sem, slope_sem, out_sem, w_sem, w_buf, act_buf, slope_buf, normed_two, grad_two, total, grad_one, up_total, down_total = refs[17:STEP]
    bufs = refs[STEP:]
    grad_buf, full_buf = bufs[0:2]

    def load_cast(k, spot):
        pltpu.make_async_copy(w_cast.at[spot], full_buf.at[k], cast_sem.at[spot]).start()

    def load_saved(num):
        layer = 2 - num // 4
        lanes = pl.ds(pl.multiple_of((num % 4) * WIDE, WIDE), WIDE)
        pltpu.make_async_copy(act_in.at[layer, :, lanes], act_buf.at[num % 2], act_sem.at[num]).start()
        pltpu.make_async_copy(slope_in.at[layer, :, lanes], slope_buf.at[num % 2], slope_sem.at[num]).start()

    def load_pair(num, carry):
        base = (num // 4) * OCT + num % 4
        load_cast(base, base)
        load_cast(base + 4, base + 4)
        @pl.when(num < 2)
        def _():
            load_saved(num)
        return carry

    lax.fori_loop(0, DOZEN, load_pair, 0)
    load_cast(MERGE, TWO_CHUNKS)
    for k in range(2):
        pltpu.make_async_copy(head_grads.at[k], grad_buf.at[HEAD_A + k], load_sem.at[k]).start()
    grad_two[...] = grad_in[...]

    def two_backward(num):
        layer, part = 2 - num // 4, num % 4
        base = (num // 4) * OCT + part
        slot = num % 2
        for k in range(2):
            wait_bytes(full_buf.at[base + 4 * k], cast_sem.at[base + 4 * k])
        wait_bytes(act_buf.at[slot], act_sem.at[num])
        wait_bytes(slope_buf.at[slot], slope_sem.at[num])
        @pl.when(part == 0)
        def _():
            normed_two[...] = layer_norm(resid_two[layer].astype(jnp.float32)).astype(jnp.bfloat16)
            total[...] = jnp.zeros_like(total)
        grad_buf[base] = dot_rows(act_buf[slot], grad_two[...]).astype(jnp.bfloat16)
        grad_pre = (dot_cols(grad_two[...], full_buf[base]) * slope_buf[slot]).astype(jnp.bfloat16)
        grad_buf[base + 4] = dot_rows(normed_two[...], grad_pre).astype(jnp.bfloat16)
        total[...] += dot_cols(grad_pre, full_buf[base + 4])
        @pl.when(part == 3)
        def _():
            normed, inverse = layer_norm_parts(resid_two[layer].astype(jnp.float32))
            back = layer_norm_back(total[...], normed, inverse) + grad_two[...].astype(jnp.float32)
            grad_two[...] = back.astype(jnp.bfloat16)
        @pl.when(num < 10)
        def _():
            load_saved(num + 2)

    def merge_backward():
        wait_bytes(full_buf.at[MERGE], cast_sem.at[TWO_CHUNKS])
        for part in range(4):
            rows = slice(part * PAD_ROWS, (part + 1) * PAD_ROWS)
            spots = slice(part * THIN, (part + 1) * THIN)
            grad_buf[MERGE, spots, :] = dot_rows(resid_saved[4, rows, :], grad_two[...]).astype(jnp.bfloat16)
            grad_one[rows, :] = dot_cols(grad_two[...], full_buf[MERGE, spots, :]).astype(jnp.bfloat16)

    def w_start(k):
        two_copies(k, w_in[3], w_in[4], w_buf.at[k % W_RING], w_sem.at[k], True)

    def w_sum(k):
        slot = k % W_RING
        block_squares(lambda rows: w_buf[slot, rows, :], w_sums, k)

    for k in range(W_RING):
        w_start(jnp.int32(k))

    def one_backward(num, carry):
        layer, tile = 3 - num // TILES, num % TILES
        rows = pl.ds(pl.multiple_of(tile * TILE, PAIR), TILE)
        lanes = pl.ds(pl.multiple_of(layer * THIN, THIN), THIN)
        normed, inverse = layer_norm_parts(resid_saved[layer, rows, :].astype(jnp.float32))
        normed_b = normed.astype(jnp.bfloat16)
        up = cast_one[1, lanes, :]
        act, slope = gelu_and_slope(dot_plain(normed_b, up))
        grad = grad_one[rows, :]
        keep = jnp.where(tile == 0, 0.0, 1.0)
        down_total[...] = down_total[...] * keep + dot_rows(act.astype(jnp.bfloat16), grad)
        grad_pre = (dot_cols(grad, cast_one[0, :, lanes]) * slope).astype(jnp.bfloat16)
        up_total[...] = up_total[...] * keep + dot_rows(normed_b, grad_pre)
        back = layer_norm_back(dot_cols(grad_pre, up), normed, inverse) + grad.astype(jnp.float32)
        grad_one[rows, :] = back.astype(jnp.bfloat16)
        @pl.when(tile == TILES - 1)
        def _():
            grad_buf[DOWN_ONE, :, lanes] = down_total[...].astype(jnp.bfloat16)
            grad_buf[UP_ONE, lanes, :] = up_total[...].astype(jnp.bfloat16)
        return carry

    down_total[...] = jnp.zeros_like(down_total)
    up_total[...] = jnp.zeros_like(up_total)

    def each_tick(t):
        @pl.when(t < DOZEN)
        def _():
            two_backward(t)

        @pl.when(t == DOZEN)
        def _():
            merge_backward()

        @pl.when((t >= DOZEN) & (t < 28))
        def _():
            one_backward(t - DOZEN, 0)

        @pl.when(t < TWO_CHUNKS)
        def _():
            wait_bytes(w_buf.at[t % W_RING], w_sem.at[t])
            w_sum(t)

        @pl.when(t + W_RING < TWO_CHUNKS)
        def _():
            w_start(t + W_RING)

        for k in range(TWO_CHUNKS, CHUNKS):
            @pl.when(t == k - W_RING)
            def _(k=k):
                small_copies(k, w_in, w_buf.at[k % W_RING], w_sem.at[k], True)

            @pl.when(t == k)
            def _(k=k):
                wait_bytes(small_ref(k, w_buf.at[k % W_RING]), w_sem.at[k])
                if k == HEAD_B:
                    w_buf[k % W_RING, HEAD_REST:WIDE, :] = jnp.zeros((WIDE - HEAD_REST, WIDE), jnp.float32)
                w_sum(k)

    def before(k):
        for num in range(2):
            @pl.when(k == HEAD_A + num)
            def _(num=num):
                wait_bytes(grad_buf.at[HEAD_A + num], load_sem.at[num])

    def after(k):
        pltpu.make_async_copy(full_buf.at[k], out.at[k], out_sem.at[k]).start()
        block_squares(lambda rows: full_buf[k, rows, :], g_sums, k)

    all_reduce_body(CHUNKS, *bufs, before, after, each_tick)

    def finish(k, carry):
        wait_bytes(full_buf.at[k], out_sem.at[k])
        return carry

    lax.fori_loop(0, CHUNKS, finish, 0)


def reduce_grads(saved, params):
    any_hbm = pl.BlockSpec(memory_space=pltpu.HBM)
    in_vmem = pl.BlockSpec(memory_space=pltpu.VMEM)
    sums_shape = (CHUNKS, 4, LANES)
    return pl.pallas_call(
        reduce_kernel,
        out_shape=[jax.ShapeDtypeStruct((CHUNKS, WIDE, WIDE), jnp.bfloat16)] + [jax.ShapeDtypeStruct(sums_shape, jnp.float32)] * 2,
        in_specs=[any_hbm] * 10 + [in_vmem] * 4,
        out_specs=[any_hbm] + [in_vmem] * 2,
        scratch_shapes=[
            pltpu.SemaphoreType.DMA((2,)),
            pltpu.SemaphoreType.DMA((25,)),
            pltpu.SemaphoreType.DMA((DOZEN,)),
            pltpu.SemaphoreType.DMA((DOZEN,)),
            pltpu.SemaphoreType.DMA((CHUNKS,)),
            pltpu.SemaphoreType.DMA((CHUNKS,)),
            pltpu.VMEM((W_RING, WIDE, WIDE), jnp.float32),
            pltpu.VMEM((2, PAD_ROWS, WIDE), jnp.bfloat16),
            pltpu.VMEM((2, PAD_ROWS, WIDE), jnp.float32),
            pltpu.VMEM((PAD_ROWS, WIDE), jnp.bfloat16),
            pltpu.VMEM((PAD_ROWS, WIDE), jnp.bfloat16),
            pltpu.VMEM((PAD_ROWS, WIDE), jnp.float32),
            pltpu.VMEM((4 * PAD_ROWS, THIN), jnp.bfloat16),
            pltpu.VMEM((THIN, WIDE), jnp.float32),
            pltpu.VMEM((WIDE, THIN), jnp.float32),
        ] + scratch(CHUNKS, WIDE),
        compiler_params=pltpu.CompilerParams(has_side_effects=True, vmem_limit_bytes=62 * 2**20),
        cost_estimate=pl.CostEstimate(flops=10**10, bytes_accessed=6 * 10**7, transcendentals=0),
    )(*saved[0:4], *params, *saved[4:OCT])


def next_kernel(*refs):
    grads, w_in, v_in = refs[0], refs[1:7], refs[7:13]
    w_sums, g_sums, images = refs[13:PAIR]
    logits, w_out, v_out = refs[PAIR], refs[17:23], refs[23:29]
    load_sem, store_sem, ring_w, ring_v, ring_g, cast, coef, resid_one, resid_two, normed_two, total_two, wide = refs[29:]
    rings = (ring_w, ring_v)

    def start_small(num):
        k = SMALL_ORDER[num]
        for which, arrays in enumerate((w_in, v_in)):
            small_copies(k, arrays, rings[which].at[num], load_sem.at[which, k], True)
        pltpu.make_async_copy(grads.at[k], ring_g.at[num], load_sem.at[2, k]).start()

    def start_two(num):
        k = two_item(num)
        slot = (num + 5) % RING
        for which, arrays in enumerate((w_in, v_in)):
            two_copies(k, arrays[3], arrays[4], rings[which].at[slot], load_sem.at[which, k], True)
        pltpu.make_async_copy(grads.at[k], ring_g.at[slot], load_sem.at[2, k]).start()

    for num in range(5):
        start_small(num)

    def ratio(w_total, g_total):
        return TRUST * (jnp.sqrt(w_total) / jnp.sqrt(g_total))

    def total(sums, first, size):
        return jnp.sum(jnp.sum(jnp.sum(sums[first:first + size], axis=0), axis=0, keepdims=True), axis=1, keepdims=True)

    for first, size in [(0, 4), (4, 4), (OCT, 4), (DOZEN, 4), (PAIR, 4), (20, 4), (HEAD_A, 2), (MERGE, 1)]:
        value = ratio(total(w_sums, first, size), total(g_sums, first, size))
        for k in range(first, first + size):
            coef[k] = jnp.broadcast_to(value, (4, LANES))
    by_row = ratio(jnp.sum(w_sums[UP_ONE], axis=1, keepdims=True), jnp.sum(g_sums[UP_ONE], axis=1, keepdims=True))
    coef[UP_ONE] = jnp.broadcast_to(by_row, (4, LANES))
    for layer in range(4):
        lanes = pl.ds(layer * THIN, THIN)
        lane_total = [jnp.sum(jnp.sum(sums[DOWN_ONE, :, lanes], axis=0, keepdims=True), axis=1, keepdims=True) for sums in (w_sums, g_sums)]
        coef[DOWN_ONE, :, lanes] = jnp.broadcast_to(ratio(*lane_total), (4, THIN))

    def apply_update(k, slot):
        def step(num, carry):
            rows = pl.ds(pl.multiple_of(num * STEP, STEP), STEP)
            factor = coef[k, pl.ds(num // 4, 1), :]
            new_v = MOMENTUM * ring_v[slot, rows, :] + factor * ring_g[slot, rows, :].astype(jnp.float32)
            new_w = ring_w[slot, rows, :] - new_v
            ring_v[slot, rows, :] = new_v
            ring_w[slot, rows, :] = new_w
            cast[k, rows, :] = new_w.astype(jnp.bfloat16)
            return carry
        lax.fori_loop(0, PAIR, step, 0)

    def update_small(num):
        k = SMALL_ORDER[num]
        for which in range(2):
            wait_bytes(small_ref(k, rings[which].at[num]), load_sem.at[which, k])
        wait_bytes(ring_g.at[num], load_sem.at[2, k])
        apply_update(k, num)
        if k == HEAD_B:
            cast[k, HEAD_REST:WIDE, :] = jnp.zeros((WIDE - HEAD_REST, WIDE), jnp.bfloat16)
        for which, arrays in enumerate((w_out, v_out)):
            small_copies(k, arrays, rings[which].at[num], store_sem.at[which, k], False)

    def wait_small_store(num):
        k = SMALL_ORDER[num]
        for which in range(2):
            wait_bytes(small_ref(k, rings[which].at[num]), store_sem.at[which, k])

    def wait_two_store(num):
        k = two_item(num)
        slot = (num + 5) % RING
        for which in range(2):
            wait_bytes(rings[which].at[slot], store_sem.at[which, k])

    def update_two(num, carry):
        k = two_item(num)
        slot = (num + 5) % RING
        for which in range(2):
            wait_bytes(rings[which].at[slot], load_sem.at[which, k])
        wait_bytes(ring_g.at[slot], load_sem.at[2, k])
        apply_update(k, slot)
        for which, arrays in enumerate((w_out, v_out)):
            two_copies(k, arrays[3], arrays[4], rings[which].at[slot], store_sem.at[which, k], False)
        later = num + AHEAD
        @pl.when((later < TWO_CHUNKS) & (later >= RING))
        def _():
            wait_two_store(later - RING)
        @pl.when(later < TWO_CHUNKS)
        def _():
            start_two(later)
        return carry

    for num in range(3):
        start_two(num)
    for num in range(5):
        update_small(num)
    arrange(images, wide, resid_one)
    wait_small_store(0)
    start_two(3)

    def first(num, carry):
        for small in range(1, 5):
            @pl.when(num == small - 1)
            def _(small=small):
                wait_small_store(small)
        update_two(num, 0)

        def body(part, carry):
            one_forward(part, resid_one, resid_one, cast)
            return carry

        return lax.fori_loop(num * 2, num * 2 + 2, body, carry)

    lax.fori_loop(0, OCT, first, 0)
    merge_forward(resid_one, cast, resid_two)

    def second(num, carry):
        layer, part = num // 4, num % 4
        @pl.when(part == 0)
        def _():
            normed_two[...] = layer_norm(resid_two[...].astype(jnp.float32)).astype(jnp.bfloat16)
            total_two[...] = jnp.zeros_like(total_two)
        @pl.when(layer < 2)
        def _():
            lax.fori_loop(OCT + num * 2, 10 + num * 2, update_two, 0)
        act = gelu(dot_plain(normed_two[...], cast[(2 - layer) * OCT + 4 + part])).astype(jnp.bfloat16)
        total_two[...] += dot_plain(act, cast[(2 - layer) * OCT + part])
        @pl.when(part == 3)
        def _():
            resid_two[...] = (resid_two[...].astype(jnp.float32) + total_two[...]).astype(jnp.bfloat16)
        return carry

    lax.fori_loop(0, DOZEN, second, 0)
    head_in = layer_norm(pool_images(resid_two)).astype(jnp.bfloat16)
    logits[:, 0:WIDE] = dot_cols(head_in, cast[HEAD_A])[0:2]
    logits[:, WIDE:1000] = dot_cols(head_in, cast[HEAD_B])[0:2, 0:HEAD_REST]
    for num in range(PAIR, TWO_CHUNKS):
        wait_two_store(num)


def update_and_forward(params, velocities, grads, w_sums, g_sums, images):
    any_hbm = pl.BlockSpec(memory_space=pltpu.HBM)
    in_vmem = pl.BlockSpec(memory_space=pltpu.VMEM)
    shapes = [jax.ShapeDtypeStruct(array.shape, array.dtype) for array in params]
    outs = pl.pallas_call(
        next_kernel,
        out_shape=[jax.ShapeDtypeStruct((2, CLASSES), jnp.float32)] + shapes + shapes,
        in_specs=[any_hbm] * 13 + [in_vmem] * 3,
        out_specs=[in_vmem] + [any_hbm] * DOZEN,
        scratch_shapes=[
            pltpu.SemaphoreType.DMA((3, CHUNKS)),
            pltpu.SemaphoreType.DMA((2, CHUNKS)),
            pltpu.VMEM((RING, WIDE, WIDE), jnp.float32),
            pltpu.VMEM((RING, WIDE, WIDE), jnp.float32),
            pltpu.VMEM((RING, WIDE, WIDE), jnp.bfloat16),
            pltpu.VMEM((CHUNKS, WIDE, WIDE), jnp.bfloat16),
            pltpu.VMEM((CHUNKS, 4, LANES), jnp.float32),
            pltpu.VMEM((4 * PAD_ROWS, THIN), jnp.bfloat16),
            pltpu.VMEM((PAD_ROWS, WIDE), jnp.bfloat16),
            pltpu.VMEM((PAD_ROWS, WIDE), jnp.bfloat16),
            pltpu.VMEM((PAD_ROWS, WIDE), jnp.float32),
            pltpu.VMEM((2 * TOKENS, THIN), jnp.float32),
        ],
        compiler_params=pltpu.CompilerParams(vmem_limit_bytes=58 * 2**20),
        cost_estimate=pl.CostEstimate(flops=10**10, bytes_accessed=135 * 10**6, transcendentals=0),
    )(grads, *params, *velocities, w_sums, g_sums, images)
    return outs


def solution(mesh):
    def local_step(x_now, labels_now, x_next, *weights):
        params = weights[0:5] + (weights[5].T,)
        velocities = weights[6:11] + (weights[11].T,)
        saved = forward_and_grads(params, x_now, labels_now)
        sums, w_sums, g_sums = reduce_grads(saved, params)
        outs = update_and_forward(params, velocities, sums, w_sums, g_sums, x_next)
        new_w, new_v = outs[1:7], outs[7:13]
        return (outs[0],) + tuple(new_w[0:5]) + (new_w[5].T,) + tuple(new_v[0:5]) + (new_v[5].T,)

    replicated = P()
    batch_split = P('data')
    in_specs = (batch_split, batch_split, batch_split) + (replicated,) * DOZEN
    out_specs = (batch_split,) + (replicated,) * DOZEN
    return jax.shard_map(local_step, mesh=mesh, in_specs=in_specs, out_specs=out_specs, check_vma=False)
```

```python
import functools

import jax
import jax.numpy as jnp
from jax import lax
from jax.experimental import pallas as pl
from jax.experimental.pallas import tpu as pltpu
from jax.sharding import PartitionSpec as P

MOMENTUM = 0.9
TRUST = 0.1
LN_EPS = 1e-6
CHUNKS = 29
HEAD_A, HEAD_B, MERGE, DOWN_ONE, UP_ONE = 24, 25, 26, 27, 28
HEAD_REST = 488
CLASSES = 1000
LANES = 512
RING = 8
AHEAD = 4
W_RING = 3
TOKENS_TWO = 196
TOKENS = 784
PAD_IMG = 208
PAD_ROWS = 416
GELU_C = 0.7978845608028654
GELU_A = 0.044715
WIDE = 512
THIN = 128
STEP = 32
QUARTER = 64
HALF = 256
TWO_CHUNKS = 24
OCT = 8
PAIR = 16
DOZEN = 12
SMALL_COUNT = 5
CASTS = 25

MESH = pl.DeviceIdType.MESH
OFFSETS = tuple(2 * num + (num >= 2) + (num >= 11) for num in range(13))


def all_reduce_body(chunks, grad_buf, full_buf, recv_core, recv_one, recv_z, recv_mid, recv_two, send_sem, recv_sem, before, after, extra):
    me = lax.axis_index('data')
    core = me % 2
    x_pos = (me // 2) % 2
    y_pos = (me // 4) % 2
    z_pos = me // OCT
    one = x_pos * (1 - core) + y_pos * core
    two = y_pos * (1 - core) + x_pos * core
    one_step = 2 * (1 - core) + 4 * core
    two_step = 4 * (1 - core) + 2 * core
    dev_core = me + 1 - 2 * core
    dev_one = me + one_step * (1 - 2 * one)
    dev_two = me + two_step * (1 - 2 * two)
    upper = z_pos // 2
    is_end = (z_pos % 3) == 0
    is_mid = (z_pos % 3) != 0
    dev_inner = me + OCT * (1 - 2 * upper)
    dev_outer = me - OCT * (1 - 2 * upper)
    half = core * HALF
    quarter = half + one * THIN
    near = quarter + upper * QUARTER
    far = quarter + (1 - upper) * QUARTER
    mine = near + two * STEP

    def rows(chunk, start, size):
        return grad_buf.at[chunk, pl.ds(pl.multiple_of(start, STEP), size)]

    def full(chunk, start, size):
        return full_buf.at[chunk, pl.ds(pl.multiple_of(start, STEP), size)]

    def remote(src, dst, which, chunk, dev):
        return pltpu.make_async_remote_copy(src_ref=src, dst_ref=dst, send_sem=send_sem.at[which, chunk], recv_sem=recv_sem.at[which, chunk], device_id=(dev,), device_id_type=MESH)

    def add_in(chunk, start, size, recv):
        def step(num, carry):
            spot = pl.ds(pl.multiple_of(start + num * STEP, STEP), STEP)
            grad_buf[chunk, spot, :] = grad_buf[chunk, spot, :] + recv[chunk, pl.ds(pl.multiple_of(num * STEP, STEP), STEP), :]
            return carry
        lax.fori_loop(0, size // STEP, step, 0)

    def c_core(k):
        return remote(rows(k, HALF - half, HALF), recv_core.at[k], 0, k, dev_core)

    def c_one(k):
        return remote(rows(k, half + (1 - one) * THIN, THIN), recv_one.at[k], 1, k, dev_one)

    def c_in(k):
        return remote(rows(k, far, QUARTER), recv_z.at[k], 2, k, dev_inner)

    def c_mid(k):
        return remote(rows(k, far, QUARTER), recv_mid.at[k], 3, k, dev_inner)

    def c_out(k):
        return remote(rows(k, near, QUARTER), recv_z.at[k], 2, k, dev_outer)

    def c_two(k):
        return remote(rows(k, near + (1 - two) * STEP, STEP), recv_two.at[k], 4, k, dev_two)

    def g_two(k):
        return remote(full(k, mine, STEP), full(k, mine, STEP), SMALL_COUNT, k, dev_two)

    def g_in(k):
        return remote(full(k, near, QUARTER), full(k, near, QUARTER), 6, k, dev_inner)

    def g_mid(k):
        return remote(full(k, near, QUARTER), full(k, near, QUARTER), 7, k, dev_inner)

    def g_out(k):
        return remote(full(k, far, QUARTER), full(k, far, QUARTER), 6, k, dev_outer)

    def g_one(k):
        return remote(full(k, quarter, THIN), full(k, quarter, THIN), OCT, k, dev_one)

    def g_core(k):
        return remote(full(k, half, HALF), full(k, half, HALF), 9, k, dev_core)

    def stage_0(k):
        before(k)
        c_core(k).start()

    def stage_1(k):
        c_core(k).wait()
        add_in(k, half, HALF, recv_core)
        c_one(k).start()

    def stage_2(k):
        c_one(k).wait()
        add_in(k, quarter, THIN, recv_one)
        @pl.when(is_end)
        def _():
            c_in(k).start()

    def stage_3(k):
        @pl.when(is_end)
        def _():
            c_in(k).wait_send()
        @pl.when(is_mid)
        def _():
            c_out(k).wait_recv()
            add_in(k, far, QUARTER, recv_z)
            c_mid(k).start()

    def stage_4(k):
        @pl.when(is_mid)
        def _():
            c_mid(k).wait()
            add_in(k, near, QUARTER, recv_mid)
            c_out(k).start()

    def stage_5(k):
        @pl.when(is_mid)
        def _():
            c_out(k).wait_send()
        @pl.when(is_end)
        def _():
            c_in(k).wait_recv()
            add_in(k, near, QUARTER, recv_z)
            c_two(k).start()

    def stage_6(k):
        @pl.when(is_end)
        def _():
            c_two(k).wait()
            spot = pl.ds(pl.multiple_of(mine, STEP), STEP)
            full_buf[k, spot, :] = grad_buf[k, spot, :] + recv_two[k]
            g_two(k).start()

    def stage_7(k):
        @pl.when(is_end)
        def _():
            g_two(k).wait()
            g_in(k).start()

    def stage_8(k):
        @pl.when(is_end)
        def _():
            g_in(k).wait_send()
        @pl.when(is_mid)
        def _():
            g_out(k).wait_recv()
            g_mid(k).start()

    def stage_9(k):
        @pl.when(is_mid)
        def _():
            g_mid(k).wait()
            g_out(k).start()

    def stage_10(k):
        @pl.when(is_mid)
        def _():
            g_out(k).wait_send()
        @pl.when(is_end)
        def _():
            g_in(k).wait_recv()
        g_one(k).start()

    def stage_11(k):
        g_one(k).wait()
        g_core(k).start()

    def stage_12(k):
        g_core(k).wait()
        after(k)

    stages = (stage_0, stage_1, stage_2, stage_3, stage_4, stage_5, stage_6, stage_7, stage_8, stage_9, stage_10, stage_11, stage_12)

    def tick(t, carry):
        for num, stage in reversed(list(enumerate(stages))):
            if num == 0:
                extra(t)
            k = t - OFFSETS[num]
            pl.when((k >= 0) & (k < chunks))(functools.partial(stage, k))
        return carry

    lax.fori_loop(0, chunks + OFFSETS[-1], tick, 0)


def scratch(chunks, cols):
    return [
        pltpu.VMEM((chunks, WIDE, cols), jnp.bfloat16),
        pltpu.VMEM((chunks, WIDE, cols), jnp.bfloat16),
        pltpu.VMEM((chunks, HALF, cols), jnp.bfloat16),
        pltpu.VMEM((chunks, THIN, cols), jnp.bfloat16),
        pltpu.VMEM((chunks, QUARTER, cols), jnp.bfloat16),
        pltpu.VMEM((chunks, QUARTER, cols), jnp.bfloat16),
        pltpu.VMEM((chunks, STEP, cols), jnp.bfloat16),
        pltpu.SemaphoreType.DMA((10, chunks)),
        pltpu.SemaphoreType.DMA((10, chunks)),
    ]


def layer_norm(values):
    row_mean = jnp.mean(values, axis=-1, keepdims=True)
    centered = values - row_mean
    variance = jnp.mean(centered * centered, axis=-1, keepdims=True)
    return centered * lax.rsqrt(variance + LN_EPS)


def layer_norm_parts(values):
    row_mean = jnp.mean(values, axis=-1, keepdims=True)
    centered = values - row_mean
    variance = jnp.mean(centered * centered, axis=-1, keepdims=True)
    inverse = lax.rsqrt(variance + LN_EPS)
    return centered * inverse, inverse


def layer_norm_back(grad, normed, inverse):
    grad_mean = jnp.mean(grad, axis=-1, keepdims=True)
    proj = jnp.mean(grad * normed, axis=-1, keepdims=True)
    return inverse * (grad - grad_mean - normed * proj)


def gelu(vals):
    inner = GELU_C * (vals + GELU_A * (vals * vals * vals))
    return vals * (0.5 * (1.0 + jnp.tanh(inner)))


def gelu_and_slope(vals):
    square = vals * vals
    tanh_in = jnp.tanh(GELU_C * (vals + GELU_A * (square * vals)))
    cdf = 0.5 * (1.0 + tanh_in)
    slope = cdf + 0.5 * vals * (1.0 - tanh_in * tanh_in) * (GELU_C * (1.0 + (3.0 * GELU_A) * square))
    return vals * cdf, slope


def dot_plain(lhs, rhs):
    return jnp.dot(lhs, rhs, preferred_element_type=jnp.float32)


def dot_rows(lhs, rhs):
    return lax.dot_general(lhs, rhs, (((0,), (0,)), ((), ())), preferred_element_type=jnp.float32)


def dot_cols(lhs, rhs):
    return lax.dot_general(lhs, rhs, (((1,), (1,)), ((), ())), preferred_element_type=jnp.float32)


def two_copies(k, ups, downs, other, sem, to_chunk):
    layer = 2 - k // OCT
    part = pl.ds(pl.multiple_of((k % 4) * WIDE, WIDE), WIDE)
    for array, cond, spot in ((downs, (k % OCT) < 4, (layer, part)), (ups, (k % OCT) >= 4, (layer, slice(None), part))):
        @pl.when(cond)
        def _(array=array, spot=spot):
            pair = (array.at[spot], other)
            pltpu.make_async_copy(*(pair if to_chunk else pair[::-1]), sem).start()


def small_pieces(k, arrays):
    up_one, down_one, merge, head = arrays[0], arrays[1], arrays[2], arrays[SMALL_COUNT]
    if k == UP_ONE:
        return [(up_one.at[layer], (pl.ds(layer * THIN, THIN),)) for layer in range(4)]
    if k == DOWN_ONE:
        return [(down_one.at[layer], (pl.ds(0, WIDE), pl.ds(layer * THIN, THIN))) for layer in range(4)]
    if k == MERGE:
        return [(merge, (pl.ds(0, WIDE),))]
    if k == HEAD_A:
        return [(head.at[pl.ds(0, WIDE)], (pl.ds(0, WIDE),))]
    return [(head.at[pl.ds(WIDE, HEAD_REST)], (pl.ds(0, HEAD_REST),))]


def small_copies(k, arrays, other, sem, to_chunk):
    for piece, inside in small_pieces(k, arrays):
        pair = (piece, other.at[inside])
        pltpu.make_async_copy(*(pair if to_chunk else pair[::-1]), sem).start()


def wait_bytes(ref, sem):
    pltpu.make_async_copy(ref, ref, sem).wait()


def small_ref(k, ref):
    return ref.at[pl.ds(0, HEAD_REST)] if k == HEAD_B else ref


SMALL_ORDER = (UP_ONE, DOWN_ONE, MERGE, HEAD_A, HEAD_B)


def two_item(num):
    return (2 - num // OCT) * OCT + (1 - num % 2) * 4 + (num % OCT) // 2


def one_forward(num, resid_in, resid_out, cast):
    layer = num // 4
    rows = pl.ds(pl.multiple_of((num % 4) * PAD_ROWS, STEP), PAD_ROWS)
    lanes = pl.ds(pl.multiple_of(layer * THIN, THIN), THIN)
    resid = resid_in[rows, :].astype(jnp.float32)
    normed = layer_norm(resid).astype(jnp.bfloat16)
    act = gelu(dot_plain(normed, cast[UP_ONE, lanes, :])).astype(jnp.bfloat16)
    out = dot_plain(act, cast[DOWN_ONE, :, lanes])
    resid_out[rows, :] = (resid + out).astype(jnp.bfloat16)


def merge_forward(resid_one, cast, resid_two):
    value = jnp.zeros((PAD_ROWS, WIDE), jnp.float32)
    for part in range(4):
        value = value + dot_plain(resid_one[part * PAD_ROWS:(part + 1) * PAD_ROWS, :], cast[MERGE, part * THIN:(part + 1) * THIN, :])
    resid_two[...] = value.astype(jnp.bfloat16)


def pool_images(resid_two):
    pooled = [jnp.sum(resid_two[img * PAD_IMG:(img + 1) * PAD_IMG, :].astype(jnp.float32), axis=0, keepdims=True) / float(TOKENS_TWO) for img in range(2)]
    return jnp.concatenate(pooled + [jnp.zeros((14, WIDE), jnp.float32)], axis=0)


def arrange(images, wide, resid):
    for img in range(2):
        wide[img * TOKENS:(img + 1) * TOKENS, :] = images[img].astype(jnp.float32)
    resid[...] = jnp.zeros_like(resid)
    for part in range(4):
        for img in range(2):
            first = part * PAD_ROWS + img * PAD_IMG
            rows = wide[pl.ds(img * TOKENS + part, TOKENS_TWO, stride=4), :]
            resid[first:first + TOKENS_TWO, :] = rows.astype(jnp.bfloat16)


def grad_kernel(*refs):
    w_in, images, labels = refs[0:6], refs[6], refs[7]
    head_grads, cast_out, act_out, slope_out, resid_saved, resid_two, grad_two, cast_one = refs[OCT:PAIR]
    load_sem, cast_sem, act_sem, slope_sem, ring_w, cast, last_two, normed_two, act_two, slope_two, total, wide = refs[PAIR:]

    def send_cast(k, spot):
        pltpu.make_async_copy(cast.at[k], cast_out.at[spot], cast_sem.at[spot]).start()

    def start_small(num):
        small_copies(SMALL_ORDER[num], w_in, ring_w.at[num], load_sem.at[SMALL_ORDER[num]], True)

    def start_two(num):
        k = two_item(num)
        two_copies(k, w_in[3], w_in[4], ring_w.at[(num + SMALL_COUNT) % RING], load_sem.at[k], True)

    def cast_slot(k, slot):
        def step(num, carry):
            rows = pl.ds(pl.multiple_of(num * THIN, THIN), THIN)
            cast[k, rows, :] = ring_w[slot, rows, :].astype(jnp.bfloat16)
            return carry
        lax.fori_loop(0, 4, step, 0)

    def cast_small(num):
        k = SMALL_ORDER[num]
        wait_bytes(small_ref(k, ring_w.at[num]), load_sem.at[k])
        cast_slot(k, num)
        if k == HEAD_B:
            cast[k, HEAD_REST:WIDE, :] = jnp.zeros((WIDE - HEAD_REST, WIDE), jnp.bfloat16)

    def cast_two(num):
        k = two_item(num)
        slot = (num + SMALL_COUNT) % RING
        wait_bytes(ring_w.at[slot], load_sem.at[k])
        cast_slot(k, slot)
        send_cast(k, k)
        @pl.when(num + RING < TWO_CHUNKS)
        def _():
            start_two(num + RING)

    for num in range(SMALL_COUNT):
        start_small(num)
    for num in range(3):
        start_two(num)
    arrange(images, wide, resid_saved.at[0])
    for num in range(SMALL_COUNT):
        cast_small(num)
        start_two(num + 3)
    send_cast(MERGE, TWO_CHUNKS)
    cast_one[0] = cast[DOWN_ONE]
    cast_one[1] = cast[UP_ONE]

    def first(num, carry):
        layer = num // 4
        one_forward(num, resid_saved.at[layer], resid_saved.at[layer + 1], cast)
        cast_two(num)
        return carry

    lax.fori_loop(0, PAIR, first, 0)
    merge_forward(resid_saved.at[4], cast, resid_two.at[0])

    def second(num, carry):
        layer, part = num // 4, num % 4
        lanes = pl.ds(pl.multiple_of(part * WIDE, WIDE), WIDE)
        @pl.when(part == 0)
        def _():
            normed_two[...] = layer_norm(resid_two[layer].astype(jnp.float32)).astype(jnp.bfloat16)
            total[...] = jnp.zeros_like(total)
        @pl.when(num < OCT)
        def _():
            cast_two(num + PAIR)
        pre = dot_plain(normed_two[...], cast[(2 - layer) * OCT + 4 + part])
        act, slope = gelu_and_slope(pre)
        act = act.astype(jnp.bfloat16)
        act_two[layer, :, lanes] = act
        slope_two[layer, :, lanes] = slope
        total[...] += dot_plain(act, cast[(2 - layer) * OCT + part])
        pltpu.make_async_copy(act_two.at[layer, :, lanes], act_out.at[layer, :, lanes], act_sem.at[num]).start()
        pltpu.make_async_copy(slope_two.at[layer, :, lanes], slope_out.at[layer, :, lanes], slope_sem.at[num]).start()
        @pl.when(part == 3)
        def _():
            value = (resid_two[layer].astype(jnp.float32) + total[...]).astype(jnp.bfloat16)
            @pl.when(layer < 2)
            def _():
                resid_two[jnp.minimum(layer + 1, 2)] = value
            @pl.when(layer == 2)
            def _():
                last_two[...] = value
        return carry

    lax.fori_loop(0, DOZEN, second, 0)

    pooled = pool_images(last_two)
    head_norm, head_inv = layer_norm_parts(pooled)
    head_in = head_norm.astype(jnp.bfloat16)
    logits = jnp.concatenate([dot_cols(head_in, cast[HEAD_A]), dot_cols(head_in, cast[HEAD_B])], axis=1)
    ids = lax.broadcasted_iota(jnp.int32, (PAIR, 1024), 1)
    row = lax.broadcasted_iota(jnp.int32, (PAIR, 1024), 0)
    logits = jnp.where(ids < CLASSES, logits, -jnp.inf)
    expo = jnp.exp(logits - jnp.max(logits, axis=1, keepdims=True))
    probs = expo / jnp.sum(expo, axis=1, keepdims=True)
    target = jnp.where(row == 0, labels[0], labels[1])
    onehot = (ids == target).astype(jnp.float32)
    grad_logits = jnp.where(row < 2, (probs - onehot) / 64.0, 0.0).astype(jnp.bfloat16)

    head_grads[0] = dot_rows(grad_logits[:, 0:WIDE], head_in).astype(jnp.bfloat16)
    head_grads[1] = dot_rows(grad_logits[:, WIDE:1024], head_in).astype(jnp.bfloat16)
    grad_head = dot_plain(grad_logits[:, 0:WIDE], cast[HEAD_A]) + dot_plain(grad_logits[:, WIDE:1024], cast[HEAD_B])
    grad_pooled = (layer_norm_back(grad_head, head_norm, head_inv) / float(TOKENS_TWO)).astype(jnp.bfloat16).astype(jnp.float32)
    spot = lax.broadcasted_iota(jnp.int32, (PAD_IMG, WIDE), 0)
    for img in range(2):
        spread = jnp.where(spot < TOKENS_TWO, jnp.broadcast_to(grad_pooled[img:img + 1], (PAD_IMG, WIDE)), 0.0)
        grad_two[img * PAD_IMG:(img + 1) * PAD_IMG, :] = spread.astype(jnp.bfloat16)

    def finish(num, carry):
        lanes = pl.ds(pl.multiple_of((num % 4) * WIDE, WIDE), WIDE)
        wait_bytes(act_two.at[num // 4, :, lanes], act_sem.at[num])
        wait_bytes(slope_two.at[num // 4, :, lanes], slope_sem.at[num])
        return carry

    lax.fori_loop(0, DOZEN, finish, 0)

    def finish_cast(k, carry):
        wait_bytes(cast.at[k], cast_sem.at[k])
        return carry

    lax.fori_loop(0, CASTS, finish_cast, 0)


def forward_and_grads(params, images, labels):
    any_hbm = pl.BlockSpec(memory_space=pltpu.HBM)
    in_vmem = pl.BlockSpec(memory_space=pltpu.VMEM)
    return pl.pallas_call(
        grad_kernel,
        out_shape=[
            jax.ShapeDtypeStruct((2, WIDE, WIDE), jnp.bfloat16),
            jax.ShapeDtypeStruct((CASTS, WIDE, WIDE), jnp.bfloat16),
            jax.ShapeDtypeStruct((3, PAD_ROWS, 2048), jnp.bfloat16),
            jax.ShapeDtypeStruct((3, PAD_ROWS, 2048), jnp.float32),
            jax.ShapeDtypeStruct((SMALL_COUNT, 4 * PAD_ROWS, THIN), jnp.bfloat16),
            jax.ShapeDtypeStruct((3, PAD_ROWS, WIDE), jnp.bfloat16),
            jax.ShapeDtypeStruct((PAD_ROWS, WIDE), jnp.bfloat16),
            jax.ShapeDtypeStruct((2, WIDE, WIDE), jnp.bfloat16),
        ],
        in_specs=[any_hbm] * 6 + [in_vmem, pl.BlockSpec(memory_space=pltpu.SMEM)],
        out_specs=[in_vmem] + [any_hbm] * 3 + [in_vmem] * 4,
        scratch_shapes=[
            pltpu.SemaphoreType.DMA((CHUNKS,)),
            pltpu.SemaphoreType.DMA((CASTS,)),
            pltpu.SemaphoreType.DMA((DOZEN,)),
            pltpu.SemaphoreType.DMA((DOZEN,)),
            pltpu.VMEM((RING, WIDE, WIDE), jnp.float32),
            pltpu.VMEM((CHUNKS, WIDE, WIDE), jnp.bfloat16),
            pltpu.VMEM((PAD_ROWS, WIDE), jnp.bfloat16),
            pltpu.VMEM((PAD_ROWS, WIDE), jnp.bfloat16),
            pltpu.VMEM((3, PAD_ROWS, 2048), jnp.bfloat16),
            pltpu.VMEM((3, PAD_ROWS, 2048), jnp.float32),
            pltpu.VMEM((PAD_ROWS, WIDE), jnp.float32),
            pltpu.VMEM((2 * TOKENS, THIN), jnp.float32),
        ],
        compiler_params=pltpu.CompilerParams(vmem_limit_bytes=62 * 2**20),
        cost_estimate=pl.CostEstimate(flops=3 * 10**10, bytes_accessed=SMALL_COUNT * 10**7, transcendentals=0),
    )(*params, images, labels)


def block_squares(read, sums, chunk):
    def step(num, carry):
        total = jnp.zeros((OCT, LANES), jnp.float32)
        for part in range(4):
            vals = read(pl.ds(pl.multiple_of(num * THIN + part * STEP, STEP), STEP)).astype(jnp.float32)
            vals = vals * vals
            total = total + (vals[0:OCT] + vals[OCT:PAIR]) + (vals[PAIR:TWO_CHUNKS] + vals[TWO_CHUNKS:STEP])
        sums[chunk, pl.ds(num, 1), :] = jnp.sum(total, axis=0, keepdims=True)
        return carry
    lax.fori_loop(0, 4, step, 0)


TILE = PAD_ROWS
TILES = 4


def reduce_kernel(*refs):
    head_grads, w_cast, act_in, slope_in, w_in = refs[0], refs[1], refs[2], refs[3], refs[4:10]
    resid_saved, resid_two, grad_in, cast_one = refs[10:14]
    out, w_sums, g_sums = refs[14:17]
    load_sem, cast_sem, act_sem, slope_sem, out_sem, w_sem, w_buf, act_buf, slope_buf, normed_two, grad_two, total, grad_one, up_total, down_total = refs[17:STEP]
    bufs = refs[STEP:]
    grad_buf, full_buf = bufs[0:2]

    def load_cast(k, spot):
        pltpu.make_async_copy(w_cast.at[spot], full_buf.at[k], cast_sem.at[spot]).start()

    def load_saved(num):
        layer = 2 - num // 4
        lanes = pl.ds(pl.multiple_of((num % 4) * WIDE, WIDE), WIDE)
        pltpu.make_async_copy(act_in.at[layer, :, lanes], act_buf.at[num % 2], act_sem.at[num]).start()
        pltpu.make_async_copy(slope_in.at[layer, :, lanes], slope_buf.at[num % 2], slope_sem.at[num]).start()

    def load_pair(num, carry):
        base = (num // 4) * OCT + num % 4
        load_cast(base, base)
        load_cast(base + 4, base + 4)
        @pl.when(num < 2)
        def _():
            load_saved(num)
        return carry

    lax.fori_loop(0, DOZEN, load_pair, 0)
    load_cast(MERGE, TWO_CHUNKS)
    for k in range(2):
        pltpu.make_async_copy(head_grads.at[k], grad_buf.at[HEAD_A + k], load_sem.at[k]).start()
    grad_two[...] = grad_in[...]

    def two_backward(num):
        layer, part = 2 - num // 4, num % 4
        base = (num // 4) * OCT + part
        slot = num % 2
        for k in range(2):
            wait_bytes(full_buf.at[base + 4 * k], cast_sem.at[base + 4 * k])
        wait_bytes(act_buf.at[slot], act_sem.at[num])
        wait_bytes(slope_buf.at[slot], slope_sem.at[num])
        @pl.when(part == 0)
        def _():
            normed_two[...] = layer_norm(resid_two[layer].astype(jnp.float32)).astype(jnp.bfloat16)
            total[...] = jnp.zeros_like(total)
        grad_buf[base] = dot_rows(act_buf[slot], grad_two[...]).astype(jnp.bfloat16)
        grad_pre = (dot_cols(grad_two[...], full_buf[base]) * slope_buf[slot]).astype(jnp.bfloat16)
        grad_buf[base + 4] = dot_rows(normed_two[...], grad_pre).astype(jnp.bfloat16)
        total[...] += dot_cols(grad_pre, full_buf[base + 4])
        @pl.when(part == 3)
        def _():
            normed, inverse = layer_norm_parts(resid_two[layer].astype(jnp.float32))
            back = layer_norm_back(total[...], normed, inverse) + grad_two[...].astype(jnp.float32)
            grad_two[...] = back.astype(jnp.bfloat16)
        @pl.when(num < 10)
        def _():
            load_saved(num + 2)

    def merge_backward():
        wait_bytes(full_buf.at[MERGE], cast_sem.at[TWO_CHUNKS])
        for part in range(4):
            rows = slice(part * PAD_ROWS, (part + 1) * PAD_ROWS)
            spots = slice(part * THIN, (part + 1) * THIN)
            grad_buf[MERGE, spots, :] = dot_rows(resid_saved[4, rows, :], grad_two[...]).astype(jnp.bfloat16)
            grad_one[rows, :] = dot_cols(grad_two[...], full_buf[MERGE, spots, :]).astype(jnp.bfloat16)

    def w_start(k):
        two_copies(k, w_in[3], w_in[4], w_buf.at[k % W_RING], w_sem.at[k], True)

    def w_sum(k):
        slot = k % W_RING
        block_squares(lambda rows: w_buf[slot, rows, :], w_sums, k)

    for k in range(W_RING):
        w_start(jnp.int32(k))

    def one_backward(num, carry):
        layer, tile = 3 - num // TILES, num % TILES
        rows = pl.ds(pl.multiple_of(tile * TILE, PAIR), TILE)
        lanes = pl.ds(pl.multiple_of(layer * THIN, THIN), THIN)
        normed, inverse = layer_norm_parts(resid_saved[layer, rows, :].astype(jnp.float32))
        normed_b = normed.astype(jnp.bfloat16)
        up = cast_one[1, lanes, :]
        act, slope = gelu_and_slope(dot_plain(normed_b, up))
        grad = grad_one[rows, :]
        keep = jnp.where(tile == 0, 0.0, 1.0)
        down_total[...] = down_total[...] * keep + dot_rows(act.astype(jnp.bfloat16), grad)
        grad_pre = (dot_cols(grad, cast_one[0, :, lanes]) * slope).astype(jnp.bfloat16)
        up_total[...] = up_total[...] * keep + dot_rows(normed_b, grad_pre)
        back = layer_norm_back(dot_cols(grad_pre, up), normed, inverse) + grad.astype(jnp.float32)
        grad_one[rows, :] = back.astype(jnp.bfloat16)
        @pl.when(tile == TILES - 1)
        def _():
            grad_buf[DOWN_ONE, :, lanes] = down_total[...].astype(jnp.bfloat16)
            grad_buf[UP_ONE, lanes, :] = up_total[...].astype(jnp.bfloat16)
        return carry

    down_total[...] = jnp.zeros_like(down_total)
    up_total[...] = jnp.zeros_like(up_total)

    def each_tick(t):
        @pl.when(t < DOZEN)
        def _():
            two_backward(t)

        @pl.when(t == DOZEN)
        def _():
            merge_backward()

        @pl.when((t >= DOZEN) & (t < 28))
        def _():
            one_backward(t - DOZEN, 0)

        @pl.when(t < TWO_CHUNKS)
        def _():
            wait_bytes(w_buf.at[t % W_RING], w_sem.at[t])
            w_sum(t)

        @pl.when(t + W_RING < TWO_CHUNKS)
        def _():
            w_start(t + W_RING)

        for k in range(TWO_CHUNKS, CHUNKS):
            @pl.when(t == k - W_RING)
            def _(k=k):
                small_copies(k, w_in, w_buf.at[k % W_RING], w_sem.at[k], True)

            @pl.when(t == k)
            def _(k=k):
                wait_bytes(small_ref(k, w_buf.at[k % W_RING]), w_sem.at[k])
                if k == HEAD_B:
                    w_buf[k % W_RING, HEAD_REST:WIDE, :] = jnp.zeros((WIDE - HEAD_REST, WIDE), jnp.float32)
                w_sum(k)

    def before(k):
        for num in range(2):
            @pl.when(k == HEAD_A + num)
            def _(num=num):
                wait_bytes(grad_buf.at[HEAD_A + num], load_sem.at[num])

    def after(k):
        pltpu.make_async_copy(full_buf.at[k], out.at[k], out_sem.at[k]).start()
        block_squares(lambda rows: full_buf[k, rows, :], g_sums, k)

    all_reduce_body(CHUNKS, *bufs, before, after, each_tick)

    def finish(k, carry):
        wait_bytes(full_buf.at[k], out_sem.at[k])
        return carry

    lax.fori_loop(0, CHUNKS, finish, 0)


def reduce_grads(saved, params):
    any_hbm = pl.BlockSpec(memory_space=pltpu.HBM)
    in_vmem = pl.BlockSpec(memory_space=pltpu.VMEM)
    sums_shape = (CHUNKS, 4, LANES)
    return pl.pallas_call(
        reduce_kernel,
        out_shape=[jax.ShapeDtypeStruct((CHUNKS, WIDE, WIDE), jnp.bfloat16)] + [jax.ShapeDtypeStruct(sums_shape, jnp.float32)] * 2,
        in_specs=[any_hbm] * 10 + [in_vmem] * 4,
        out_specs=[any_hbm] + [in_vmem] * 2,
        scratch_shapes=[
            pltpu.SemaphoreType.DMA((2,)),
            pltpu.SemaphoreType.DMA((CASTS,)),
            pltpu.SemaphoreType.DMA((DOZEN,)),
            pltpu.SemaphoreType.DMA((DOZEN,)),
            pltpu.SemaphoreType.DMA((CHUNKS,)),
            pltpu.SemaphoreType.DMA((CHUNKS,)),
            pltpu.VMEM((W_RING, WIDE, WIDE), jnp.float32),
            pltpu.VMEM((2, PAD_ROWS, WIDE), jnp.bfloat16),
            pltpu.VMEM((2, PAD_ROWS, WIDE), jnp.float32),
            pltpu.VMEM((PAD_ROWS, WIDE), jnp.bfloat16),
            pltpu.VMEM((PAD_ROWS, WIDE), jnp.bfloat16),
            pltpu.VMEM((PAD_ROWS, WIDE), jnp.float32),
            pltpu.VMEM((4 * PAD_ROWS, THIN), jnp.bfloat16),
            pltpu.VMEM((THIN, WIDE), jnp.float32),
            pltpu.VMEM((WIDE, THIN), jnp.float32),
        ] + scratch(CHUNKS, WIDE),
        compiler_params=pltpu.CompilerParams(has_side_effects=True, vmem_limit_bytes=62 * 2**20),
        cost_estimate=pl.CostEstimate(flops=10**10, bytes_accessed=6 * 10**7, transcendentals=0),
    )(*saved[0:4], *params, *saved[4:OCT])


def next_kernel(*refs):
    grads, w_in, v_in = refs[0], refs[1:7], refs[7:13]
    w_sums, g_sums, images = refs[13:PAIR]
    logits, w_out, v_out = refs[PAIR], refs[17:23], refs[23:29]
    load_sem, store_sem, ring_w, ring_v, ring_g, cast, coef, resid_one, resid_two, normed_two, total_two, wide = refs[29:]
    rings = (ring_w, ring_v)

    def start_small(num):
        k = SMALL_ORDER[num]
        for which, arrays in enumerate((w_in, v_in)):
            small_copies(k, arrays, rings[which].at[num], load_sem.at[which, k], True)
        pltpu.make_async_copy(grads.at[k], ring_g.at[num], load_sem.at[2, k]).start()

    def start_two(num):
        k = two_item(num)
        slot = (num + SMALL_COUNT) % RING
        for which, arrays in enumerate((w_in, v_in)):
            two_copies(k, arrays[3], arrays[4], rings[which].at[slot], load_sem.at[which, k], True)
        pltpu.make_async_copy(grads.at[k], ring_g.at[slot], load_sem.at[2, k]).start()

    for num in range(SMALL_COUNT):
        start_small(num)
    for num in range(3):
        start_two(num)

    def ratio(w_total, g_total):
        return TRUST * (jnp.sqrt(w_total) / jnp.sqrt(g_total))

    def total(sums, first, size):
        return jnp.sum(jnp.sum(jnp.sum(sums[first:first + size], axis=0), axis=0, keepdims=True), axis=1, keepdims=True)

    for first, size in [(0, 4), (4, 4), (OCT, 4), (DOZEN, 4), (PAIR, 4), (20, 4), (HEAD_A, 2), (MERGE, 1)]:
        value = ratio(total(w_sums, first, size), total(g_sums, first, size))
        for k in range(first, first + size):
            coef[k] = jnp.broadcast_to(value, (4, LANES))
    by_row = ratio(jnp.sum(w_sums[UP_ONE], axis=1, keepdims=True), jnp.sum(g_sums[UP_ONE], axis=1, keepdims=True))
    coef[UP_ONE] = jnp.broadcast_to(by_row, (4, LANES))
    for layer in range(4):
        lanes = pl.ds(layer * THIN, THIN)
        lane_total = [jnp.sum(jnp.sum(sums[DOWN_ONE, :, lanes], axis=0, keepdims=True), axis=1, keepdims=True) for sums in (w_sums, g_sums)]
        coef[DOWN_ONE, :, lanes] = jnp.broadcast_to(ratio(*lane_total), (4, THIN))

    def apply_update(k, slot):
        def step(num, carry):
            rows = pl.ds(pl.multiple_of(num * QUARTER, QUARTER), QUARTER)
            factor = coef[k, pl.ds(num // 2, 1), :]
            new_v = MOMENTUM * ring_v[slot, rows, :] + factor * ring_g[slot, rows, :].astype(jnp.float32)
            new_w = ring_w[slot, rows, :] - new_v
            ring_v[slot, rows, :] = new_v
            ring_w[slot, rows, :] = new_w
            cast[k, rows, :] = new_w.astype(jnp.bfloat16)
            return carry
        lax.fori_loop(0, OCT, step, 0)

    def update_small(num):
        k = SMALL_ORDER[num]
        for which in range(2):
            wait_bytes(small_ref(k, rings[which].at[num]), load_sem.at[which, k])
        wait_bytes(ring_g.at[num], load_sem.at[2, k])
        apply_update(k, num)
        if k == HEAD_B:
            cast[k, HEAD_REST:WIDE, :] = jnp.zeros((WIDE - HEAD_REST, WIDE), jnp.bfloat16)
        for which, arrays in enumerate((w_out, v_out)):
            small_copies(k, arrays, rings[which].at[num], store_sem.at[which, k], False)

    def wait_small_store(num):
        k = SMALL_ORDER[num]
        for which in range(2):
            wait_bytes(small_ref(k, rings[which].at[num]), store_sem.at[which, k])

    def wait_two_store(num):
        k = two_item(num)
        slot = (num + SMALL_COUNT) % RING
        for which in range(2):
            wait_bytes(rings[which].at[slot], store_sem.at[which, k])

    def update_two(num, carry):
        k = two_item(num)
        slot = (num + SMALL_COUNT) % RING
        for which in range(2):
            wait_bytes(rings[which].at[slot], load_sem.at[which, k])
        wait_bytes(ring_g.at[slot], load_sem.at[2, k])
        apply_update(k, slot)
        for which, arrays in enumerate((w_out, v_out)):
            two_copies(k, arrays[3], arrays[4], rings[which].at[slot], store_sem.at[which, k], False)
        later = num + AHEAD
        @pl.when((later < TWO_CHUNKS) & (later >= RING))
        def _():
            wait_two_store(later - RING)
        @pl.when(later < TWO_CHUNKS)
        def _():
            start_two(later)
        return carry

    arrange(images, wide, resid_one)
    for num in range(SMALL_COUNT):
        update_small(num)
    wait_small_store(0)
    start_two(3)

    def first(num, carry):
        for small in range(1, SMALL_COUNT):
            @pl.when(num == small - 1)
            def _(small=small):
                wait_small_store(small)
        update_two(num, 0)

        def body(part, carry):
            one_forward(part, resid_one, resid_one, cast)
            return carry

        return lax.fori_loop(num * 2, num * 2 + 2, body, carry)

    lax.fori_loop(0, OCT, first, 0)
    merge_forward(resid_one, cast, resid_two)

    def two_forward(num):
        layer, part = num // 4, num % 4
        @pl.when(part == 0)
        def _():
            normed_two[...] = layer_norm(resid_two[...].astype(jnp.float32)).astype(jnp.bfloat16)
            total_two[...] = jnp.zeros_like(total_two)
        act = gelu(dot_plain(normed_two[...], cast[(2 - layer) * OCT + 4 + part])).astype(jnp.bfloat16)
        total_two[...] += dot_plain(act, cast[(2 - layer) * OCT + part])
        @pl.when(part == 3)
        def _():
            resid_two[...] = (resid_two[...].astype(jnp.float32) + total_two[...]).astype(jnp.bfloat16)

    def second(num, carry):
        update_two(num + OCT, 0)
        @pl.when((num < OCT) | (num % 2 == 1))
        def _():
            two_forward(jnp.minimum(num, OCT) + jnp.maximum(num - OCT, 0) // 2)
        return carry

    lax.fori_loop(0, PAIR, second, 0)
    head_in = layer_norm(pool_images(resid_two)).astype(jnp.bfloat16)
    logits[:, 0:WIDE] = dot_cols(head_in, cast[HEAD_A])[0:2]
    logits[:, WIDE:1000] = dot_cols(head_in, cast[HEAD_B])[0:2, 0:HEAD_REST]
    for num in range(PAIR, TWO_CHUNKS):
        wait_two_store(num)


def update_and_forward(params, velocities, grads, w_sums, g_sums, images):
    any_hbm = pl.BlockSpec(memory_space=pltpu.HBM)
    in_vmem = pl.BlockSpec(memory_space=pltpu.VMEM)
    shapes = [jax.ShapeDtypeStruct(array.shape, array.dtype) for array in params]
    outs = pl.pallas_call(
        next_kernel,
        out_shape=[jax.ShapeDtypeStruct((2, CLASSES), jnp.float32)] + shapes + shapes,
        in_specs=[any_hbm] * 13 + [in_vmem] * 3,
        out_specs=[in_vmem] + [any_hbm] * DOZEN,
        scratch_shapes=[
            pltpu.SemaphoreType.DMA((3, CHUNKS)),
            pltpu.SemaphoreType.DMA((2, CHUNKS)),
            pltpu.VMEM((RING, WIDE, WIDE), jnp.float32),
            pltpu.VMEM((RING, WIDE, WIDE), jnp.float32),
            pltpu.VMEM((RING, WIDE, WIDE), jnp.bfloat16),
            pltpu.VMEM((CHUNKS, WIDE, WIDE), jnp.bfloat16),
            pltpu.VMEM((CHUNKS, 4, LANES), jnp.float32),
            pltpu.VMEM((4 * PAD_ROWS, THIN), jnp.bfloat16),
            pltpu.VMEM((PAD_ROWS, WIDE), jnp.bfloat16),
            pltpu.VMEM((PAD_ROWS, WIDE), jnp.bfloat16),
            pltpu.VMEM((PAD_ROWS, WIDE), jnp.float32),
            pltpu.VMEM((2 * TOKENS, THIN), jnp.float32),
        ],
        compiler_params=pltpu.CompilerParams(vmem_limit_bytes=58 * 2**20),
        cost_estimate=pl.CostEstimate(flops=10**10, bytes_accessed=135 * 10**6, transcendentals=0),
    )(grads, *params, *velocities, w_sums, g_sums, images)
    return outs


def solution(mesh):
    def local_step(x_now, labels_now, x_next, *weights):
        params = weights[0:SMALL_COUNT] + (weights[SMALL_COUNT].T,)
        velocities = weights[6:11] + (weights[11].T,)
        saved = forward_and_grads(params, x_now, labels_now)
        sums, w_sums, g_sums = reduce_grads(saved, params)
        outs = update_and_forward(params, velocities, sums, w_sums, g_sums, x_next)
        new_w, new_v = outs[1:7], outs[7:13]
        return (outs[0],) + tuple(new_w[0:SMALL_COUNT]) + (new_w[SMALL_COUNT].T,) + tuple(new_v[0:SMALL_COUNT]) + (new_v[SMALL_COUNT].T,)

    replicated = P()
    batch_split = P('data')
    in_specs = (batch_split, batch_split, batch_split) + (replicated,) * DOZEN
    out_specs = (batch_split,) + (replicated,) * DOZEN
    return jax.shard_map(local_step, mesh=mesh, in_specs=in_specs, out_specs=out_specs, check_vma=False)
```

```python
import functools

import jax
import jax.numpy as jnp
from jax import lax
from jax.experimental import pallas as pl
from jax.experimental.pallas import tpu as pltpu
from jax.sharding import PartitionSpec as P

MOMENTUM = 0.9
TRUST = 0.1
LN_EPS = 1e-6
CHUNKS = 29
HEAD_A, HEAD_B, MERGE, DOWN_ONE, UP_ONE = 24, 25, 26, 27, 28
HEAD_REST = 488
CLASSES = 1000
LANES = 512
RING = 8
AHEAD = 4
W_RING = 3
TOKENS_TWO = 196
TOKENS = 784
PAD_IMG = 208
PAD_ROWS = 416
TALL = 1664
GELU_C = 0.7978845608028654
GELU_A = 0.044715
WIDE = 512
THIN = 128
STEP = 32
QUARTER = 64
HALF = 256
TWO_CHUNKS = 24
OCT = 8
PAIR = 16
DOZEN = 12
SMALL_COUNT = 5
CASTS = 25

MESH = pl.DeviceIdType.MESH
OFFSETS = tuple(2 * num + (num >= 2) + 2 * (num >= 11) for num in range(13))


def all_reduce_body(chunks, grad_buf, full_buf, recv_core, recv_one, recv_z, recv_mid, recv_two, send_sem, recv_sem, before, after, extra):
    me = lax.axis_index('data')
    core = me % 2
    x_pos = (me // 2) % 2
    y_pos = (me // 4) % 2
    z_pos = me // OCT
    one = x_pos * (1 - core) + y_pos * core
    two = y_pos * (1 - core) + x_pos * core
    one_step = 2 * (1 - core) + 4 * core
    two_step = 4 * (1 - core) + 2 * core
    dev_core = me + 1 - 2 * core
    dev_one = me + one_step * (1 - 2 * one)
    dev_two = me + two_step * (1 - 2 * two)
    upper = z_pos // 2
    is_end = (z_pos % 3) == 0
    is_mid = (z_pos % 3) != 0
    dev_inner = me + OCT * (1 - 2 * upper)
    dev_outer = me - OCT * (1 - 2 * upper)
    half = core * HALF
    quarter = half + one * THIN
    near = quarter + upper * QUARTER
    far = quarter + (1 - upper) * QUARTER
    mine = near + two * STEP

    def rows(chunk, start, size):
        return grad_buf.at[chunk, pl.ds(pl.multiple_of(start, STEP), size)]

    def full(chunk, start, size):
        return full_buf.at[chunk, pl.ds(pl.multiple_of(start, STEP), size)]

    def remote(src, dst, which, chunk, dev):
        return pltpu.make_async_remote_copy(src_ref=src, dst_ref=dst, send_sem=send_sem.at[which, chunk], recv_sem=recv_sem.at[which, chunk], device_id=(dev,), device_id_type=MESH)

    def add_in(chunk, start, size, recv):
        def step(num, carry):
            spot = pl.ds(pl.multiple_of(start + num * STEP, STEP), STEP)
            grad_buf[chunk, spot, :] = grad_buf[chunk, spot, :] + recv[chunk, pl.ds(pl.multiple_of(num * STEP, STEP), STEP), :]
            return carry
        lax.fori_loop(0, size // STEP, step, 0)

    def c_core(k):
        return remote(rows(k, HALF - half, HALF), recv_core.at[k], 0, k, dev_core)

    def c_one(k):
        return remote(rows(k, half + (1 - one) * THIN, THIN), recv_one.at[k], 1, k, dev_one)

    def c_in(k):
        return remote(rows(k, far, QUARTER), recv_z.at[k], 2, k, dev_inner)

    def c_mid(k):
        return remote(rows(k, far, QUARTER), recv_mid.at[k], 3, k, dev_inner)

    def c_out(k):
        return remote(rows(k, near, QUARTER), recv_z.at[k], 2, k, dev_outer)

    def c_two(k):
        return remote(rows(k, near + (1 - two) * STEP, STEP), recv_two.at[k], 4, k, dev_two)

    def g_two(k):
        return remote(full(k, mine, STEP), full(k, mine, STEP), SMALL_COUNT, k, dev_two)

    def g_in(k):
        return remote(full(k, near, QUARTER), full(k, near, QUARTER), 6, k, dev_inner)

    def g_mid(k):
        return remote(full(k, near, QUARTER), full(k, near, QUARTER), 7, k, dev_inner)

    def g_out(k):
        return remote(full(k, far, QUARTER), full(k, far, QUARTER), 6, k, dev_outer)

    def g_one(k):
        return remote(full(k, quarter, THIN), full(k, quarter, THIN), OCT, k, dev_one)

    def g_core(k):
        return remote(full(k, half, HALF), full(k, half, HALF), 9, k, dev_core)

    def stage_0(k):
        before(k)
        c_core(k).start()

    def stage_1(k):
        c_core(k).wait()
        add_in(k, half, HALF, recv_core)
        c_one(k).start()

    def stage_2(k):
        c_one(k).wait()
        add_in(k, quarter, THIN, recv_one)
        @pl.when(is_end)
        def _():
            c_in(k).start()

    def stage_3(k):
        @pl.when(is_end)
        def _():
            c_in(k).wait_send()
        @pl.when(is_mid)
        def _():
            c_out(k).wait_recv()
            add_in(k, far, QUARTER, recv_z)
            c_mid(k).start()

    def stage_4(k):
        @pl.when(is_mid)
        def _():
            c_mid(k).wait()
            add_in(k, near, QUARTER, recv_mid)
            c_out(k).start()

    def stage_5(k):
        @pl.when(is_mid)
        def _():
            c_out(k).wait_send()
        @pl.when(is_end)
        def _():
            c_in(k).wait_recv()
            add_in(k, near, QUARTER, recv_z)
            c_two(k).start()

    def stage_6(k):
        @pl.when(is_end)
        def _():
            c_two(k).wait()
            spot = pl.ds(pl.multiple_of(mine, STEP), STEP)
            full_buf[k, spot, :] = grad_buf[k, spot, :] + recv_two[k]
            g_two(k).start()

    def stage_7(k):
        @pl.when(is_end)
        def _():
            g_two(k).wait()
            g_in(k).start()

    def stage_8(k):
        @pl.when(is_end)
        def _():
            g_in(k).wait_send()
        @pl.when(is_mid)
        def _():
            g_out(k).wait_recv()
            g_mid(k).start()

    def stage_9(k):
        @pl.when(is_mid)
        def _():
            g_mid(k).wait()
            g_out(k).start()

    def stage_10(k):
        @pl.when(is_mid)
        def _():
            g_out(k).wait_send()
        @pl.when(is_end)
        def _():
            g_in(k).wait_recv()
        g_one(k).start()

    def stage_11(k):
        g_one(k).wait()
        g_core(k).start()

    def stage_12(k):
        g_core(k).wait()
        after(k)

    stages = (stage_0, stage_1, stage_2, stage_3, stage_4, stage_5, stage_6, stage_7, stage_8, stage_9, stage_10, stage_11, stage_12)

    def tick(t, carry):
        for num, stage in reversed(list(enumerate(stages))):
            if num == 0:
                extra(t)
            k = t - OFFSETS[num]
            pl.when((k >= 0) & (k < chunks))(functools.partial(stage, k))
        return carry

    lax.fori_loop(0, chunks + OFFSETS[-1], tick, 0)


def scratch(chunks, cols):
    return [
        pltpu.VMEM((chunks, WIDE, cols), jnp.bfloat16),
        pltpu.VMEM((chunks, WIDE, cols), jnp.bfloat16),
        pltpu.VMEM((chunks, HALF, cols), jnp.bfloat16),
        pltpu.VMEM((chunks, THIN, cols), jnp.bfloat16),
        pltpu.VMEM((chunks, QUARTER, cols), jnp.bfloat16),
        pltpu.VMEM((chunks, QUARTER, cols), jnp.bfloat16),
        pltpu.VMEM((chunks, STEP, cols), jnp.bfloat16),
        pltpu.SemaphoreType.DMA((10, chunks)),
        pltpu.SemaphoreType.DMA((10, chunks)),
    ]


def layer_norm(values):
    row_mean = jnp.mean(values, axis=-1, keepdims=True)
    centered = values - row_mean
    variance = jnp.mean(centered * centered, axis=-1, keepdims=True)
    return centered * lax.rsqrt(variance + LN_EPS)


def layer_norm_parts(values):
    row_mean = jnp.mean(values, axis=-1, keepdims=True)
    centered = values - row_mean
    variance = jnp.mean(centered * centered, axis=-1, keepdims=True)
    inverse = lax.rsqrt(variance + LN_EPS)
    return centered * inverse, inverse


def layer_norm_back(grad, normed, inverse):
    grad_mean = jnp.mean(grad, axis=-1, keepdims=True)
    proj = jnp.mean(grad * normed, axis=-1, keepdims=True)
    return inverse * (grad - grad_mean - normed * proj)


def gelu(vals):
    inner = GELU_C * (vals + GELU_A * (vals * vals * vals))
    return vals * (0.5 * (1.0 + jnp.tanh(inner)))


def gelu_and_slope(vals):
    square = vals * vals
    tanh_in = jnp.tanh(GELU_C * (vals + GELU_A * (square * vals)))
    cdf = 0.5 * (1.0 + tanh_in)
    slope = cdf + 0.5 * vals * (1.0 - tanh_in * tanh_in) * (GELU_C * (1.0 + (3.0 * GELU_A) * square))
    return vals * cdf, slope


def dot_plain(lhs, rhs):
    return jnp.dot(lhs, rhs, preferred_element_type=jnp.float32)


def dot_rows(lhs, rhs):
    return lax.dot_general(lhs, rhs, (((0,), (0,)), ((), ())), preferred_element_type=jnp.float32)


def dot_cols(lhs, rhs):
    return lax.dot_general(lhs, rhs, (((1,), (1,)), ((), ())), preferred_element_type=jnp.float32)


def two_copies(k, ups, downs, other, sem, to_chunk):
    layer = 2 - k // OCT
    part = pl.ds(pl.multiple_of((k % 4) * WIDE, WIDE), WIDE)
    for array, cond, spot in ((downs, (k % OCT) < 4, (layer, part)), (ups, (k % OCT) >= 4, (layer, slice(None), part))):
        @pl.when(cond)
        def _(array=array, spot=spot):
            pair = (array.at[spot], other)
            pltpu.make_async_copy(*(pair if to_chunk else pair[::-1]), sem).start()


def small_pieces(k, arrays):
    up_one, down_one, merge, head = arrays[0], arrays[1], arrays[2], arrays[SMALL_COUNT]
    if k == UP_ONE:
        return [(up_one.at[layer], (pl.ds(layer * THIN, THIN),)) for layer in range(4)]
    if k == DOWN_ONE:
        return [(down_one.at[layer], (pl.ds(0, WIDE), pl.ds(layer * THIN, THIN))) for layer in range(4)]
    if k == MERGE:
        return [(merge, (pl.ds(0, WIDE),))]
    if k == HEAD_A:
        return [(head.at[pl.ds(0, WIDE)], (pl.ds(0, WIDE),))]
    return [(head.at[pl.ds(WIDE, HEAD_REST)], (pl.ds(0, HEAD_REST),))]


def small_copies(k, arrays, other, sem, to_chunk):
    for piece, inside in small_pieces(k, arrays):
        pair = (piece, other.at[inside])
        pltpu.make_async_copy(*(pair if to_chunk else pair[::-1]), sem).start()


def wait_bytes(ref, sem):
    pltpu.make_async_copy(ref, ref, sem).wait()


def small_ref(k, ref):
    return ref.at[pl.ds(0, HEAD_REST)] if k == HEAD_B else ref


SMALL_ORDER = (UP_ONE, DOWN_ONE, MERGE, HEAD_A, HEAD_B)


def two_item(num):
    return (2 - num // OCT) * OCT + (1 - num % 2) * 4 + (num % OCT) // 2


def one_forward(num, resid_in, resid_out, cast):
    layer = num // 1
    rows = pl.ds(pl.multiple_of((num % 1) * TALL, STEP), TALL)
    lanes = pl.ds(pl.multiple_of(layer * THIN, THIN), THIN)
    resid = resid_in[rows, :].astype(jnp.float32)
    normed = layer_norm(resid).astype(jnp.bfloat16)
    act = gelu(dot_plain(normed, cast[UP_ONE, lanes, :])).astype(jnp.bfloat16)
    out = dot_plain(act, cast[DOWN_ONE, :, lanes])
    resid_out[rows, :] = (resid + out).astype(jnp.bfloat16)


def merge_forward(resid_one, cast, resid_two):
    value = jnp.zeros((PAD_ROWS, WIDE), jnp.float32)
    for part in range(4):
        value = value + dot_plain(resid_one[part * PAD_ROWS:(part + 1) * PAD_ROWS, :], cast[MERGE, part * THIN:(part + 1) * THIN, :])
    resid_two[...] = value.astype(jnp.bfloat16)


def pool_images(resid_two):
    pooled = [jnp.sum(resid_two[img * PAD_IMG:(img + 1) * PAD_IMG, :].astype(jnp.float32), axis=0, keepdims=True) / float(TOKENS_TWO) for img in range(2)]
    return jnp.concatenate(pooled + [jnp.zeros((14, WIDE), jnp.float32)], axis=0)


def arrange(images, wide, resid):
    for img in range(2):
        wide[img * TOKENS:(img + 1) * TOKENS, :] = images[img].astype(jnp.float32)
    resid[...] = jnp.zeros_like(resid)
    for part in range(4):
        for img in range(2):
            first = part * PAD_ROWS + img * PAD_IMG
            rows = wide[pl.ds(img * TOKENS + part, TOKENS_TWO, stride=4), :]
            resid[first:first + TOKENS_TWO, :] = rows.astype(jnp.bfloat16)


def grad_kernel(*refs):
    w_in, images, labels = refs[0:6], refs[6], refs[7]
    head_grads, cast_out, act_out, slope_out, resid_saved, resid_two, grad_two, cast_one = refs[OCT:PAIR]
    load_sem, cast_sem, act_sem, slope_sem, ring_w, cast, last_two, normed_two, act_two, slope_two, total, wide = refs[PAIR:]

    def send_cast(k, spot):
        pltpu.make_async_copy(cast.at[k], cast_out.at[spot], cast_sem.at[spot]).start()

    def start_small(num):
        small_copies(SMALL_ORDER[num], w_in, ring_w.at[num], load_sem.at[SMALL_ORDER[num]], True)

    def start_two(num):
        k = two_item(num)
        two_copies(k, w_in[3], w_in[4], ring_w.at[(num + SMALL_COUNT) % RING], load_sem.at[k], True)

    def cast_slot(k, slot):
        def step(num, carry):
            rows = pl.ds(pl.multiple_of(num * THIN, THIN), THIN)
            cast[k, rows, :] = ring_w[slot, rows, :].astype(jnp.bfloat16)
            return carry
        lax.fori_loop(0, 4, step, 0)

    def cast_small(num):
        k = SMALL_ORDER[num]
        wait_bytes(small_ref(k, ring_w.at[num]), load_sem.at[k])
        cast_slot(k, num)
        if k == HEAD_B:
            cast[k, HEAD_REST:WIDE, :] = jnp.zeros((WIDE - HEAD_REST, WIDE), jnp.bfloat16)

    def cast_two(num):
        k = two_item(num)
        slot = (num + SMALL_COUNT) % RING
        wait_bytes(ring_w.at[slot], load_sem.at[k])
        cast_slot(k, slot)
        send_cast(k, k)
        @pl.when(num + RING < TWO_CHUNKS)
        def _():
            start_two(num + RING)

    for num in range(SMALL_COUNT):
        start_small(num)
    for num in range(3):
        start_two(num)
    arrange(images, wide, resid_saved.at[0])
    for num in range(SMALL_COUNT):
        cast_small(num)
        start_two(num + 3)
    send_cast(MERGE, TWO_CHUNKS)
    cast_one[0] = cast[DOWN_ONE]
    cast_one[1] = cast[UP_ONE]

    def first(num, carry):
        layer = num // 1
        one_forward(num, resid_saved.at[layer], resid_saved.at[layer + 1], cast)
        for extra in range(4):
            cast_two(4 * num + extra)
        return carry

    lax.fori_loop(0, 4, first, 0)
    merge_forward(resid_saved.at[4], cast, resid_two.at[0])

    def second(num, carry):
        layer = num // 2
        @pl.when(num % 2 == 0)
        def _():
            normed_two[...] = layer_norm(resid_two[layer].astype(jnp.float32)).astype(jnp.bfloat16)
            total[...] = jnp.zeros_like(total)
        @pl.when(num < 4)
        def _():
            cast_two(2 * num + PAIR)
            cast_two(2 * num + PAIR + 1)
        value = total[...]
        for sub in range(2):
            part = 2 * (num % 2) + sub
            lanes = pl.ds(pl.multiple_of(part * WIDE, WIDE), WIDE)
            pre = dot_plain(normed_two[...], cast[(2 - layer) * OCT + 4 + part])
            act, slope = gelu_and_slope(pre)
            act = act.astype(jnp.bfloat16)
            act_two[layer, :, lanes] = act
            slope_two[layer, :, lanes] = slope
            value = value + dot_plain(act, cast[(2 - layer) * OCT + part])
        total[...] = value
        for sub in range(2):
            part = 2 * (num % 2) + sub
            lanes = pl.ds(pl.multiple_of(part * WIDE, WIDE), WIDE)
            pltpu.make_async_copy(act_two.at[layer, :, lanes], act_out.at[layer, :, lanes], act_sem.at[2 * num + sub]).start()
            pltpu.make_async_copy(slope_two.at[layer, :, lanes], slope_out.at[layer, :, lanes], slope_sem.at[2 * num + sub]).start()
        @pl.when(num % 2 == 1)
        def _():
            value = (resid_two[layer].astype(jnp.float32) + total[...]).astype(jnp.bfloat16)
            @pl.when(layer < 2)
            def _():
                resid_two[jnp.minimum(layer + 1, 2)] = value
            @pl.when(layer == 2)
            def _():
                last_two[...] = value
        return carry

    lax.fori_loop(0, 6, second, 0)

    pooled = pool_images(last_two)
    head_norm, head_inv = layer_norm_parts(pooled)
    head_in = head_norm.astype(jnp.bfloat16)
    logits = jnp.concatenate([dot_cols(head_in, cast[HEAD_A]), dot_cols(head_in, cast[HEAD_B])], axis=1)
    ids = lax.broadcasted_iota(jnp.int32, (PAIR, 1024), 1)
    row = lax.broadcasted_iota(jnp.int32, (PAIR, 1024), 0)
    logits = jnp.where(ids < CLASSES, logits, -jnp.inf)
    expo = jnp.exp(logits - jnp.max(logits, axis=1, keepdims=True))
    probs = expo / jnp.sum(expo, axis=1, keepdims=True)
    target = jnp.where(row == 0, labels[0], labels[1])
    onehot = (ids == target).astype(jnp.float32)
    grad_logits = jnp.where(row < 2, (probs - onehot) / 64.0, 0.0).astype(jnp.bfloat16)

    head_grads[0] = dot_rows(grad_logits[:, 0:WIDE], head_in).astype(jnp.bfloat16)
    head_grads[1] = dot_rows(grad_logits[:, WIDE:1024], head_in).astype(jnp.bfloat16)
    grad_head = dot_plain(grad_logits[:, 0:WIDE], cast[HEAD_A]) + dot_plain(grad_logits[:, WIDE:1024], cast[HEAD_B])
    grad_pooled = (layer_norm_back(grad_head, head_norm, head_inv) / float(TOKENS_TWO)).astype(jnp.bfloat16).astype(jnp.float32)
    spot = lax.broadcasted_iota(jnp.int32, (PAD_IMG, WIDE), 0)
    for img in range(2):
        spread = jnp.where(spot < TOKENS_TWO, jnp.broadcast_to(grad_pooled[img:img + 1], (PAD_IMG, WIDE)), 0.0)
        grad_two[img * PAD_IMG:(img + 1) * PAD_IMG, :] = spread.astype(jnp.bfloat16)

    def finish(num, carry):
        lanes = pl.ds(pl.multiple_of((num % 4) * WIDE, WIDE), WIDE)
        wait_bytes(act_two.at[num // 4, :, lanes], act_sem.at[num])
        wait_bytes(slope_two.at[num // 4, :, lanes], slope_sem.at[num])
        return carry

    lax.fori_loop(0, DOZEN, finish, 0)

    def finish_cast(k, carry):
        wait_bytes(cast.at[k], cast_sem.at[k])
        return carry

    lax.fori_loop(0, CASTS, finish_cast, 0)


def forward_and_grads(params, images, labels):
    any_hbm = pl.BlockSpec(memory_space=pltpu.HBM)
    in_vmem = pl.BlockSpec(memory_space=pltpu.VMEM)
    return pl.pallas_call(
        grad_kernel,
        out_shape=[
            jax.ShapeDtypeStruct((2, WIDE, WIDE), jnp.bfloat16),
            jax.ShapeDtypeStruct((CASTS, WIDE, WIDE), jnp.bfloat16),
            jax.ShapeDtypeStruct((3, PAD_ROWS, 2048), jnp.bfloat16),
            jax.ShapeDtypeStruct((3, PAD_ROWS, 2048), jnp.float32),
            jax.ShapeDtypeStruct((SMALL_COUNT, 4 * PAD_ROWS, THIN), jnp.bfloat16),
            jax.ShapeDtypeStruct((3, PAD_ROWS, WIDE), jnp.bfloat16),
            jax.ShapeDtypeStruct((PAD_ROWS, WIDE), jnp.bfloat16),
            jax.ShapeDtypeStruct((2, WIDE, WIDE), jnp.bfloat16),
        ],
        in_specs=[any_hbm] * 6 + [in_vmem, pl.BlockSpec(memory_space=pltpu.SMEM)],
        out_specs=[in_vmem] + [any_hbm] * 3 + [in_vmem] * 4,
        scratch_shapes=[
            pltpu.SemaphoreType.DMA((CHUNKS,)),
            pltpu.SemaphoreType.DMA((CASTS,)),
            pltpu.SemaphoreType.DMA((DOZEN,)),
            pltpu.SemaphoreType.DMA((DOZEN,)),
            pltpu.VMEM((RING, WIDE, WIDE), jnp.float32),
            pltpu.VMEM((CHUNKS, WIDE, WIDE), jnp.bfloat16),
            pltpu.VMEM((PAD_ROWS, WIDE), jnp.bfloat16),
            pltpu.VMEM((PAD_ROWS, WIDE), jnp.bfloat16),
            pltpu.VMEM((3, PAD_ROWS, 2048), jnp.bfloat16),
            pltpu.VMEM((3, PAD_ROWS, 2048), jnp.float32),
            pltpu.VMEM((PAD_ROWS, WIDE), jnp.float32),
            pltpu.VMEM((2 * TOKENS, THIN), jnp.float32),
        ],
        compiler_params=pltpu.CompilerParams(vmem_limit_bytes=62 * 2**20),
        cost_estimate=pl.CostEstimate(flops=3 * 10**10, bytes_accessed=SMALL_COUNT * 10**7, transcendentals=0),
    )(*params, images, labels)


def block_squares(read, sums, chunk):
    def step(num, carry):
        total = jnp.zeros((OCT, LANES), jnp.float32)
        for part in range(4):
            vals = read(pl.ds(pl.multiple_of(num * THIN + part * STEP, STEP), STEP)).astype(jnp.float32)
            vals = vals * vals
            total = total + (vals[0:OCT] + vals[OCT:PAIR]) + (vals[PAIR:TWO_CHUNKS] + vals[TWO_CHUNKS:STEP])
        sums[chunk, pl.ds(num, 1), :] = jnp.sum(total, axis=0, keepdims=True)
        return carry
    lax.fori_loop(0, 4, step, 0)


TILE = PAD_ROWS
TILES = 4


def reduce_kernel(*refs):
    head_grads, w_cast, act_in, slope_in, w_in = refs[0], refs[1], refs[2], refs[3], refs[4:10]
    resid_saved, resid_two, grad_in, cast_one = refs[10:14]
    out, w_sums, g_sums = refs[14:17]
    load_sem, cast_sem, act_sem, slope_sem, out_sem, w_sem, w_buf, act_buf, slope_buf, normed_two, grad_two, total, grad_one, up_total, down_total = refs[17:STEP]
    bufs = refs[STEP:]
    grad_buf, full_buf = bufs[0:2]

    def load_cast(k, spot):
        pltpu.make_async_copy(w_cast.at[spot], full_buf.at[k], cast_sem.at[spot]).start()

    def load_saved(num):
        layer = 2 - num // 4
        lanes = pl.ds(pl.multiple_of((num % 4) * WIDE, WIDE), WIDE)
        pltpu.make_async_copy(act_in.at[layer, :, lanes], act_buf.at[num % 2], act_sem.at[num]).start()
        pltpu.make_async_copy(slope_in.at[layer, :, lanes], slope_buf.at[num % 2], slope_sem.at[num]).start()

    def load_pair(num, carry):
        base = (num // 4) * OCT + num % 4
        load_cast(base, base)
        load_cast(base + 4, base + 4)
        @pl.when(num < 2)
        def _():
            load_saved(num)
        return carry

    lax.fori_loop(0, DOZEN, load_pair, 0)
    load_cast(MERGE, TWO_CHUNKS)
    for k in range(2):
        pltpu.make_async_copy(head_grads.at[k], grad_buf.at[HEAD_A + k], load_sem.at[k]).start()
    grad_two[...] = grad_in[...]

    def two_backward(num):
        layer, part = 2 - num // 4, num % 4
        base = (num // 4) * OCT + part
        slot = num % 2
        for k in range(2):
            wait_bytes(full_buf.at[base + 4 * k], cast_sem.at[base + 4 * k])
        wait_bytes(act_buf.at[slot], act_sem.at[num])
        wait_bytes(slope_buf.at[slot], slope_sem.at[num])
        @pl.when(part == 0)
        def _():
            normed_two[...] = layer_norm(resid_two[layer].astype(jnp.float32)).astype(jnp.bfloat16)
            total[...] = jnp.zeros_like(total)
        grad_buf[base] = dot_rows(act_buf[slot], grad_two[...]).astype(jnp.bfloat16)
        grad_pre = (dot_cols(grad_two[...], full_buf[base]) * slope_buf[slot]).astype(jnp.bfloat16)
        grad_buf[base + 4] = dot_rows(normed_two[...], grad_pre).astype(jnp.bfloat16)
        total[...] += dot_cols(grad_pre, full_buf[base + 4])
        @pl.when(part == 3)
        def _():
            normed, inverse = layer_norm_parts(resid_two[layer].astype(jnp.float32))
            back = layer_norm_back(total[...], normed, inverse) + grad_two[...].astype(jnp.float32)
            grad_two[...] = back.astype(jnp.bfloat16)
        @pl.when(num < 10)
        def _():
            load_saved(num + 2)

    def merge_backward():
        wait_bytes(full_buf.at[MERGE], cast_sem.at[TWO_CHUNKS])
        for part in range(4):
            rows = slice(part * PAD_ROWS, (part + 1) * PAD_ROWS)
            spots = slice(part * THIN, (part + 1) * THIN)
            grad_buf[MERGE, spots, :] = dot_rows(resid_saved[4, rows, :], grad_two[...]).astype(jnp.bfloat16)
            grad_one[rows, :] = dot_cols(grad_two[...], full_buf[MERGE, spots, :]).astype(jnp.bfloat16)

    def w_start(k):
        two_copies(k, w_in[3], w_in[4], w_buf.at[k % W_RING], w_sem.at[k], True)

    def w_sum(k):
        slot = k % W_RING
        block_squares(lambda rows: w_buf[slot, rows, :], w_sums, k)

    for k in range(W_RING):
        w_start(jnp.int32(k))

    def one_backward(num, carry):
        layer, tile = 3 - num // TILES, num % TILES
        rows = pl.ds(pl.multiple_of(tile * TILE, PAIR), TILE)
        lanes = pl.ds(pl.multiple_of(layer * THIN, THIN), THIN)
        normed, inverse = layer_norm_parts(resid_saved[layer, rows, :].astype(jnp.float32))
        normed_b = normed.astype(jnp.bfloat16)
        up = cast_one[1, lanes, :]
        act, slope = gelu_and_slope(dot_plain(normed_b, up))
        grad = grad_one[rows, :]
        keep = jnp.where(tile == 0, 0.0, 1.0)
        down_total[...] = down_total[...] * keep + dot_rows(act.astype(jnp.bfloat16), grad)
        grad_pre = (dot_cols(grad, cast_one[0, :, lanes]) * slope).astype(jnp.bfloat16)
        up_total[...] = up_total[...] * keep + dot_rows(normed_b, grad_pre)
        back = layer_norm_back(dot_cols(grad_pre, up), normed, inverse) + grad.astype(jnp.float32)
        grad_one[rows, :] = back.astype(jnp.bfloat16)
        @pl.when(tile == TILES - 1)
        def _():
            grad_buf[DOWN_ONE, :, lanes] = down_total[...].astype(jnp.bfloat16)
            grad_buf[UP_ONE, lanes, :] = up_total[...].astype(jnp.bfloat16)
        return carry

    down_total[...] = jnp.zeros_like(down_total)
    up_total[...] = jnp.zeros_like(up_total)

    def each_tick(t):
        @pl.when(t < DOZEN)
        def _():
            two_backward(t)

        @pl.when(t == DOZEN)
        def _():
            merge_backward()

        @pl.when((t >= DOZEN) & (t < 28))
        def _():
            one_backward(t - DOZEN, 0)

        @pl.when(t < TWO_CHUNKS)
        def _():
            wait_bytes(w_buf.at[t % W_RING], w_sem.at[t])
            w_sum(t)

        @pl.when(t + W_RING < TWO_CHUNKS)
        def _():
            w_start(t + W_RING)

        for k in range(TWO_CHUNKS, CHUNKS):
            @pl.when(t == k - W_RING)
            def _(k=k):
                small_copies(k, w_in, w_buf.at[k % W_RING], w_sem.at[k], True)

            @pl.when(t == k)
            def _(k=k):
                wait_bytes(small_ref(k, w_buf.at[k % W_RING]), w_sem.at[k])
                if k == HEAD_B:
                    w_buf[k % W_RING, HEAD_REST:WIDE, :] = jnp.zeros((WIDE - HEAD_REST, WIDE), jnp.float32)
                w_sum(k)

    def before(k):
        for num in range(2):
            @pl.when(k == HEAD_A + num)
            def _(num=num):
                wait_bytes(grad_buf.at[HEAD_A + num], load_sem.at[num])

    def after(k):
        pltpu.make_async_copy(full_buf.at[k], out.at[k], out_sem.at[k]).start()
        block_squares(lambda rows: full_buf[k, rows, :], g_sums, k)

    all_reduce_body(CHUNKS, *bufs, before, after, each_tick)

    def finish(k, carry):
        wait_bytes(full_buf.at[k], out_sem.at[k])
        return carry

    lax.fori_loop(0, CHUNKS, finish, 0)


def reduce_grads(saved, params):
    any_hbm = pl.BlockSpec(memory_space=pltpu.HBM)
    in_vmem = pl.BlockSpec(memory_space=pltpu.VMEM)
    sums_shape = (CHUNKS, 4, LANES)
    return pl.pallas_call(
        reduce_kernel,
        out_shape=[jax.ShapeDtypeStruct((CHUNKS, WIDE, WIDE), jnp.bfloat16)] + [jax.ShapeDtypeStruct(sums_shape, jnp.float32)] * 2,
        in_specs=[any_hbm] * 10 + [in_vmem] * 4,
        out_specs=[any_hbm] + [in_vmem] * 2,
        scratch_shapes=[
            pltpu.SemaphoreType.DMA((2,)),
            pltpu.SemaphoreType.DMA((CASTS,)),
            pltpu.SemaphoreType.DMA((DOZEN,)),
            pltpu.SemaphoreType.DMA((DOZEN,)),
            pltpu.SemaphoreType.DMA((CHUNKS,)),
            pltpu.SemaphoreType.DMA((CHUNKS,)),
            pltpu.VMEM((W_RING, WIDE, WIDE), jnp.float32),
            pltpu.VMEM((2, PAD_ROWS, WIDE), jnp.bfloat16),
            pltpu.VMEM((2, PAD_ROWS, WIDE), jnp.float32),
            pltpu.VMEM((PAD_ROWS, WIDE), jnp.bfloat16),
            pltpu.VMEM((PAD_ROWS, WIDE), jnp.bfloat16),
            pltpu.VMEM((PAD_ROWS, WIDE), jnp.float32),
            pltpu.VMEM((4 * PAD_ROWS, THIN), jnp.bfloat16),
            pltpu.VMEM((THIN, WIDE), jnp.float32),
            pltpu.VMEM((WIDE, THIN), jnp.float32),
        ] + scratch(CHUNKS, WIDE),
        compiler_params=pltpu.CompilerParams(has_side_effects=True, vmem_limit_bytes=62 * 2**20),
        cost_estimate=pl.CostEstimate(flops=10**10, bytes_accessed=6 * 10**7, transcendentals=0),
    )(*saved[0:4], *params, *saved[4:OCT])


def next_kernel(*refs):
    grads, w_in, v_in = refs[0], refs[1:7], refs[7:13]
    w_sums, g_sums, images = refs[13:PAIR]
    logits, w_out, v_out = refs[PAIR], refs[17:23], refs[23:29]
    load_sem, store_sem, ring_w, ring_v, ring_g, cast, coef, resid_one, resid_two, normed_two, total_two, wide = refs[29:]
    rings = (ring_w, ring_v)

    def start_small(num):
        k = SMALL_ORDER[num]
        for which, arrays in enumerate((w_in, v_in)):
            small_copies(k, arrays, rings[which].at[num], load_sem.at[which, k], True)
        pltpu.make_async_copy(grads.at[k], ring_g.at[num], load_sem.at[2, k]).start()

    def start_two(num):
        k = two_item(num)
        slot = (num + SMALL_COUNT) % RING
        for which, arrays in enumerate((w_in, v_in)):
            two_copies(k, arrays[3], arrays[4], rings[which].at[slot], load_sem.at[which, k], True)
        pltpu.make_async_copy(grads.at[k], ring_g.at[slot], load_sem.at[2, k]).start()

    for num in range(SMALL_COUNT):
        start_small(num)
    for num in range(3):
        start_two(num)

    def ratio(w_total, g_total):
        return TRUST * (jnp.sqrt(w_total) / jnp.sqrt(g_total))

    def total(sums, first, size):
        return jnp.sum(jnp.sum(jnp.sum(sums[first:first + size], axis=0), axis=0, keepdims=True), axis=1, keepdims=True)

    for first, size in [(0, 4), (4, 4), (OCT, 4), (DOZEN, 4), (PAIR, 4), (20, 4), (HEAD_A, 2), (MERGE, 1)]:
        value = ratio(total(w_sums, first, size), total(g_sums, first, size))
        for k in range(first, first + size):
            coef[k] = jnp.broadcast_to(value, (4, LANES))
    by_row = ratio(jnp.sum(w_sums[UP_ONE], axis=1, keepdims=True), jnp.sum(g_sums[UP_ONE], axis=1, keepdims=True))
    coef[UP_ONE] = jnp.broadcast_to(by_row, (4, LANES))
    for layer in range(4):
        lanes = pl.ds(layer * THIN, THIN)
        lane_total = [jnp.sum(jnp.sum(sums[DOWN_ONE, :, lanes], axis=0, keepdims=True), axis=1, keepdims=True) for sums in (w_sums, g_sums)]
        coef[DOWN_ONE, :, lanes] = jnp.broadcast_to(ratio(*lane_total), (4, THIN))

    def apply_update(k, slot):
        def step(num, carry):
            rows = pl.ds(pl.multiple_of(num * QUARTER, QUARTER), QUARTER)
            factor = coef[k, pl.ds(num // 2, 1), :]
            new_v = MOMENTUM * ring_v[slot, rows, :] + factor * ring_g[slot, rows, :].astype(jnp.float32)
            new_w = ring_w[slot, rows, :] - new_v
            ring_v[slot, rows, :] = new_v
            ring_w[slot, rows, :] = new_w
            cast[k, rows, :] = new_w.astype(jnp.bfloat16)
            return carry
        lax.fori_loop(0, OCT, step, 0)

    def update_small(num):
        k = SMALL_ORDER[num]
        for which in range(2):
            wait_bytes(small_ref(k, rings[which].at[num]), load_sem.at[which, k])
        wait_bytes(ring_g.at[num], load_sem.at[2, k])
        apply_update(k, num)
        if k == HEAD_B:
            cast[k, HEAD_REST:WIDE, :] = jnp.zeros((WIDE - HEAD_REST, WIDE), jnp.bfloat16)
        for which, arrays in enumerate((w_out, v_out)):
            small_copies(k, arrays, rings[which].at[num], store_sem.at[which, k], False)

    def wait_small_store(num):
        k = SMALL_ORDER[num]
        for which in range(2):
            wait_bytes(small_ref(k, rings[which].at[num]), store_sem.at[which, k])

    def wait_two_store(num):
        k = two_item(num)
        slot = (num + SMALL_COUNT) % RING
        for which in range(2):
            wait_bytes(rings[which].at[slot], store_sem.at[which, k])

    def update_two(num, carry):
        k = two_item(num)
        slot = (num + SMALL_COUNT) % RING
        for which in range(2):
            wait_bytes(rings[which].at[slot], load_sem.at[which, k])
        wait_bytes(ring_g.at[slot], load_sem.at[2, k])
        apply_update(k, slot)
        for which, arrays in enumerate((w_out, v_out)):
            two_copies(k, arrays[3], arrays[4], rings[which].at[slot], store_sem.at[which, k], False)
        later = num + AHEAD
        @pl.when((later < TWO_CHUNKS) & (later >= RING))
        def _():
            wait_two_store(later - RING)
        @pl.when(later < TWO_CHUNKS)
        def _():
            start_two(later)
        return carry

    arrange(images, wide, resid_one)
    for num in range(SMALL_COUNT):
        update_small(num)
    wait_small_store(0)
    start_two(3)

    def first(num, carry):
        for small in range(1, SMALL_COUNT):
            @pl.when(num == small - 1)
            def _(small=small):
                wait_small_store(small)
        update_two(num, 0)

        @pl.when(num % 2 == 1)
        def _():
            one_forward(num // 2, resid_one, resid_one, cast)
        return carry

    lax.fori_loop(0, OCT, first, 0)
    merge_forward(resid_one, cast, resid_two)

    def two_forward(num):
        layer, part = num // 4, num % 4
        @pl.when(part == 0)
        def _():
            normed_two[...] = layer_norm(resid_two[...].astype(jnp.float32)).astype(jnp.bfloat16)
            total_two[...] = jnp.zeros_like(total_two)
        act = gelu(dot_plain(normed_two[...], cast[(2 - layer) * OCT + 4 + part])).astype(jnp.bfloat16)
        total_two[...] += dot_plain(act, cast[(2 - layer) * OCT + part])
        @pl.when(part == 3)
        def _():
            resid_two[...] = (resid_two[...].astype(jnp.float32) + total_two[...]).astype(jnp.bfloat16)

    def second(num, carry):
        update_two(num + OCT, 0)
        @pl.when((num < OCT) | (num % 2 == 1))
        def _():
            two_forward(jnp.minimum(num, OCT) + jnp.maximum(num - OCT, 0) // 2)
        return carry

    lax.fori_loop(0, PAIR, second, 0)
    head_in = layer_norm(pool_images(resid_two)).astype(jnp.bfloat16)
    logits[:, 0:WIDE] = dot_cols(head_in, cast[HEAD_A])[0:2]
    logits[:, WIDE:1000] = dot_cols(head_in, cast[HEAD_B])[0:2, 0:HEAD_REST]
    for num in range(PAIR, TWO_CHUNKS):
        wait_two_store(num)


def update_and_forward(params, velocities, grads, w_sums, g_sums, images):
    any_hbm = pl.BlockSpec(memory_space=pltpu.HBM)
    in_vmem = pl.BlockSpec(memory_space=pltpu.VMEM)
    shapes = [jax.ShapeDtypeStruct(array.shape, array.dtype) for array in params]
    outs = pl.pallas_call(
        next_kernel,
        out_shape=[jax.ShapeDtypeStruct((2, CLASSES), jnp.float32)] + shapes + shapes,
        in_specs=[any_hbm] * 13 + [in_vmem] * 3,
        out_specs=[in_vmem] + [any_hbm] * DOZEN,
        scratch_shapes=[
            pltpu.SemaphoreType.DMA((3, CHUNKS)),
            pltpu.SemaphoreType.DMA((2, CHUNKS)),
            pltpu.VMEM((RING, WIDE, WIDE), jnp.float32),
            pltpu.VMEM((RING, WIDE, WIDE), jnp.float32),
            pltpu.VMEM((RING, WIDE, WIDE), jnp.bfloat16),
            pltpu.VMEM((CHUNKS, WIDE, WIDE), jnp.bfloat16),
            pltpu.VMEM((CHUNKS, 4, LANES), jnp.float32),
            pltpu.VMEM((4 * PAD_ROWS, THIN), jnp.bfloat16),
            pltpu.VMEM((PAD_ROWS, WIDE), jnp.bfloat16),
            pltpu.VMEM((PAD_ROWS, WIDE), jnp.bfloat16),
            pltpu.VMEM((PAD_ROWS, WIDE), jnp.float32),
            pltpu.VMEM((2 * TOKENS, THIN), jnp.float32),
        ],
        compiler_params=pltpu.CompilerParams(vmem_limit_bytes=58 * 2**20),
        cost_estimate=pl.CostEstimate(flops=10**10, bytes_accessed=135 * 10**6, transcendentals=0),
    )(grads, *params, *velocities, w_sums, g_sums, images)
    return outs


def solution(mesh):
    def local_step(x_now, labels_now, x_next, *weights):
        params = weights[0:SMALL_COUNT] + (weights[SMALL_COUNT].T,)
        velocities = weights[6:11] + (weights[11].T,)
        saved = forward_and_grads(params, x_now, labels_now)
        sums, w_sums, g_sums = reduce_grads(saved, params)
        outs = update_and_forward(params, velocities, sums, w_sums, g_sums, x_next)
        new_w, new_v = outs[1:7], outs[7:13]
        return (outs[0],) + tuple(new_w[0:SMALL_COUNT]) + (new_w[SMALL_COUNT].T,) + tuple(new_v[0:SMALL_COUNT]) + (new_v[SMALL_COUNT].T,)

    replicated = P()
    batch_split = P('data')
    in_specs = (batch_split, batch_split, batch_split) + (replicated,) * DOZEN
    out_specs = (batch_split,) + (replicated,) * DOZEN
    return jax.shard_map(local_step, mesh=mesh, in_specs=in_specs, out_specs=out_specs, check_vma=False)
```
